16 devices in a mesh: dp: 2 (over y, z), sp: 8 (over x, core).
Axes of the slice: x: 4, y: 2, z: 1, core: 2. Of those that a mesh axis runs over, the one named last changes fastest.
The devices are a block of a 4x4x8 slice.
Arguments:
- dec_hidden: bfloat16 [8192, 768], P(('dp', 'sp')), parts along dimension 0
- memory: bfloat16 [4096, 768], P(('dp', 'sp')), parts along dimension 0
- mem_len: int32 [2], P('dp'), parts along dimension 0
- gain_self: bfloat16 [2, 768], replicated
- gain_cross: bfloat16 [2, 768], replicated
- gain_mlp: bfloat16 [2, 768], replicated
- self_q: bfloat16 [2, 768, 768], replicated
- self_k: bfloat16 [2, 768, 768], replicated
- self_v: bfloat16 [2, 768, 768], replicated
- self_o: bfloat16 [2, 768, 768], replicated
- cross_q: bfloat16 [2, 768, 768], replicated
- cross_k: bfloat16 [2, 768, 128], replicated
- cross_v: bfloat16 [2, 768, 128], replicated
- cross_o: bfloat16 [2, 768, 768], replicated
- mlp_gate: bfloat16 [2, 768, 2048], replicated
- mlp_up: bfloat16 [2, 768, 2048], replicated
- mlp_down: bfloat16 [2, 2048, 768], replicated
Outputs:
- output: bfloat16 [8192, 768], P(('dp', 'sp')), parts along dimension 0
There are 2 independent parts. The reference program is written for one: setup_inputs(seed, part) draws one part's arguments, and reference() takes and returns one part's arrays. A program takes and returns all parts, laid end to end along the dimension named above; an argument that names none is the same for every part.
All inputs are finite; a program needn't handle non-finite values.
Results may differ from the reference program's by a relative error of at most 0.0139901.
Values are sent between devices in bfloat16 or wider.
A program may use at most 768 MiB of HBM per device.

```python
import jax
import jax.numpy as jnp
from jax import lax

SHARDS = 8
TQ_DEV = 512
TM_DEV = 256
D_MODEL = 768
HEAD = 64
KV_HEADS = 2
FF_DIM = 2048
LAYERS = 2

TQ_LEN = TQ_DEV * SHARDS
TM_LEN = TM_DEV * SHARDS
HEADS = D_MODEL // HEAD
KV_DIM = HEAD * KV_HEADS
GROUP_SIZE = HEADS // KV_HEADS
ATT_SCALE = HEAD ** -0.5


def draw_matrix(key_mat, shape):
    return (jax.random.normal(key_mat, shape, jnp.float32) * shape[1] ** -0.5).astype(jnp.bfloat16)


def draw_gain(key_gain):
    return (1.0 + 0.3 * jax.random.normal(key_gain, (LAYERS, D_MODEL), jnp.float32)).astype(jnp.bfloat16)


def setup_inputs(seed: int = 0, part: int = 0) -> dict:
    part_key = jax.random.fold_in(jax.random.key(seed), part)
    part_keys = jax.random.split(part_key, 5)
    dec_noise = jax.random.normal(part_keys[0], (SHARDS, TQ_DEV, D_MODEL), jnp.float32)
    dec_shift = 0.8 * jax.random.normal(part_keys[1], (SHARDS, 1, D_MODEL), jnp.float32)
    mem_noise = jax.random.normal(part_keys[2], (SHARDS, TM_DEV, D_MODEL), jnp.float32)
    mem_shift = jax.random.normal(part_keys[3], (SHARDS, 1, D_MODEL), jnp.float32)
    mem_len = jax.random.randint(part_keys[4], (1,), TM_LEN // 4 + 1, 3 * TM_LEN // 4 + 1, dtype=jnp.int32)
    w_keys = jax.random.split(jax.random.key(seed + 1), 14)
    return {
        "dec_hidden": (dec_noise + dec_shift).reshape(TQ_LEN, D_MODEL).astype(jnp.bfloat16),
        "memory": (mem_noise + mem_shift).reshape(TM_LEN, D_MODEL).astype(jnp.bfloat16),
        "mem_len": mem_len,
        "gain_self": draw_gain(w_keys[0]),
        "gain_cross": draw_gain(w_keys[1]),
        "gain_mlp": draw_gain(w_keys[2]),
        "self_q": draw_matrix(w_keys[3], (LAYERS, D_MODEL, D_MODEL)),
        "self_k": draw_matrix(w_keys[4], (LAYERS, D_MODEL, D_MODEL)),
        "self_v": draw_matrix(w_keys[5], (LAYERS, D_MODEL, D_MODEL)),
        "self_o": draw_matrix(w_keys[6], (LAYERS, D_MODEL, D_MODEL)),
        "cross_q": draw_matrix(w_keys[7], (LAYERS, D_MODEL, D_MODEL)),
        "cross_k": draw_matrix(w_keys[8], (LAYERS, D_MODEL, KV_DIM)),
        "cross_v": draw_matrix(w_keys[9], (LAYERS, D_MODEL, KV_DIM)),
        "cross_o": draw_matrix(w_keys[10], (LAYERS, D_MODEL, D_MODEL)),
        "mlp_gate": draw_matrix(w_keys[11], (LAYERS, D_MODEL, FF_DIM)),
        "mlp_up": draw_matrix(w_keys[12], (LAYERS, D_MODEL, FF_DIM)),
        "mlp_down": draw_matrix(w_keys[13], (LAYERS, FF_DIM, D_MODEL)),
    }


def rms_norm(values, gain_vec):
    val32 = values.astype(jnp.float32)
    inv_rms = lax.rsqrt(jnp.mean(val32 * val32, axis=-1, keepdims=True) + 1e-6)
    return (val32 * inv_rms * gain_vec.astype(jnp.float32)).astype(jnp.bfloat16)


def project(rows, weight):
    return jnp.dot(rows, weight, preferred_element_type=jnp.float32)


def add_residual(hidden, update):
    return (hidden.astype(jnp.float32) + update).astype(jnp.bfloat16)


def head_attend(q_head, k_head, v_head, valid):
    scores = jnp.dot(q_head, k_head.T, preferred_element_type=jnp.float32) * ATT_SCALE
    scores = jnp.where(valid, scores, -1e30)
    row_max = jnp.max(scores, axis=1, keepdims=True)
    exp_vals = jnp.exp(scores - row_max)
    row_sum = jnp.sum(exp_vals, axis=1, keepdims=True)
    weighted = jnp.dot(exp_vals.astype(jnp.bfloat16), v_head, preferred_element_type=jnp.float32)
    return weighted / row_sum


def multi_head(q_rows, k_rows, v_rows, valid, group_size):
    q_len = q_rows.shape[0]
    k_len = k_rows.shape[0]
    q_heads = q_rows.reshape(q_len, HEADS, HEAD).transpose(1, 0, 2)
    k_heads = k_rows.reshape(k_len, -1, HEAD).transpose(1, 0, 2)
    v_heads = v_rows.reshape(k_len, -1, HEAD).transpose(1, 0, 2)

    def one_head(head_idx):
        kv_idx = head_idx // group_size
        return head_attend(q_heads[head_idx], k_heads[kv_idx], v_heads[kv_idx], valid)

    per_head = lax.map(one_head, jnp.arange(HEADS))
    return per_head.transpose(1, 0, 2).reshape(q_len, HEADS * HEAD).astype(jnp.bfloat16)


def reference(dec_hidden, memory, mem_len, gain_self, gain_cross, gain_mlp, self_q, self_k, self_v, self_o, cross_q, cross_k, cross_v, cross_o, mlp_gate, mlp_up, mlp_down):
    positions = jnp.arange(TQ_LEN)
    causal = positions[:, None] >= positions[None, :]
    mem_valid = (jnp.arange(TM_LEN) < mem_len[0])[None, :]

    def decoder_layer(hidden, layer_w):
        (g_self, g_cross, g_mlp, w_query, w_key, w_value, w_out, x_query, x_key, x_value, x_out, w_gate, w_up, w_down) = layer_w
        normed = rms_norm(hidden, g_self)
        q_rows = project(normed, w_query).astype(jnp.bfloat16)
        k_rows = project(normed, w_key).astype(jnp.bfloat16)
        v_rows = project(normed, w_value).astype(jnp.bfloat16)
        attn_out = multi_head(q_rows, k_rows, v_rows, causal, 1)
        hidden = add_residual(hidden, project(attn_out, w_out))
        normed = rms_norm(hidden, g_cross)
        q_rows = project(normed, x_query).astype(jnp.bfloat16)
        mem_k = project(memory, x_key).astype(jnp.bfloat16)
        mem_v = project(memory, x_value).astype(jnp.bfloat16)
        attn_out = multi_head(q_rows, mem_k, mem_v, mem_valid, GROUP_SIZE)
        hidden = add_residual(hidden, project(attn_out, x_out))
        normed = rms_norm(hidden, g_mlp)
        act_vals = (jax.nn.silu(project(normed, w_gate)) * project(normed, w_up)).astype(jnp.bfloat16)
        hidden = add_residual(hidden, project(act_vals, w_down))
        return hidden, None

    weights = (gain_self, gain_cross, gain_mlp, self_q, self_k, self_v, self_o, cross_q, cross_k, cross_v, cross_o, mlp_gate, mlp_up, mlp_down)
    return lax.scan(decoder_layer, dec_hidden, weights)[0]
```

```python
import functools

import jax
import jax.numpy as jnp
from jax import lax
from jax.experimental import pallas as pl
from jax.experimental.pallas import tpu as pltpu
from jax.sharding import PartitionSpec as P

HEAD_DIM = 64
NORM_EPS = 1e-6
MASK_VALUE = -1e30
ATT_SCALE = HEAD_DIM ** -0.5
MAX_MEM_LEN = 1536
PAIR = 2 * HEAD_DIM
TILE = 256
CHUNK = 512
NN = (((1,), (0,)), ((), ()))
NT = (((1,), (1,)), ((), ()))
F32 = jnp.float32
BF16 = jnp.bfloat16
MESH = pl.DeviceIdType.MESH
VMEM_LIMIT = 60 * 1024 * 1024
ANY = pl.BlockSpec(memory_space=pl.ANY)
VMEM = pl.BlockSpec(memory_space=pltpu.VMEM)
SMEM = pl.BlockSpec(memory_space=pltpu.SMEM)


def rms_norm(val32, gain_row):
    inv_rms = lax.rsqrt(jnp.mean(val32 * val32, axis=-1, keepdims=True) + NORM_EPS)
    return (val32 * inv_rms * gain_row.astype(F32)).astype(BF16)


def dot(lhs, rhs, dims=NN):
    return lax.dot_general(lhs, rhs, dims, preferred_element_type=F32)


def pre_kernel(hid_ref, mem_ref, gain_ref, ck_ref, cv_ref, h_ref, mkv_ref):
    h_ref[...] = rms_norm(hid_ref[...].astype(F32), gain_ref[0:1])
    mem = mem_ref[...]
    kv_dim = ck_ref.shape[2]
    for layer in range(ck_ref.shape[0]):
        mkv_ref[layer, :, :kv_dim] = dot(mem, ck_ref[layer]).astype(BF16)
        mkv_ref[layer, :, kv_dim:] = dot(mem, cv_ref[layer]).astype(BF16)


def pre_call(hidden, memory, gain_self, cross_k, cross_v):
    layers, _, kv_dim = cross_k.shape
    return pl.pallas_call(
        pre_kernel,
        out_shape=(
            jax.ShapeDtypeStruct(hidden.shape, BF16),
            jax.ShapeDtypeStruct((layers, memory.shape[0], 2 * kv_dim), BF16),
        ),
        in_specs=[VMEM] * 5,
        out_specs=(VMEM, VMEM),
        compiler_params=pltpu.CompilerParams(vmem_limit_bytes=VMEM_LIMIT),
        name="pre",
    )(hidden, memory, gain_self, cross_k, cross_v)


def col_scores(k_val, q_val, buf, size, mask, m_prev, mc):
    s = dot(k_val, q_val)
    if mask is not None:
        s = jnp.where(mask, s, MASK_VALUE)
    buf[:size] = s
    mc[...] = jnp.maximum(m_prev, jnp.max(s, axis=0, keepdims=True))


def col_softmax(buf, size, mc, n, m_ref, l_ref):
    m_new = mc[...]
    alpha = jnp.exp(m_ref[n] - m_new)
    e = jnp.exp(buf[:size] - m_new)
    l_ref[n] = l_ref[n] * alpha + jnp.sum(e, axis=0, keepdims=True)
    m_ref[n] = m_new
    return e.astype(BF16), alpha


def self_kernel(layer, n_sp, h_hbm, mkv_hbm, wq_hbm, wk_hbm, wv_hbm, o_hbm, mall_hbm,
                h_own, h_rem, wq, wk, wv, wqt, wvt, qm, k_s, vt_s, m_ref, l_ref, acc, b0, b1, mc0, mc1, o_stage, mbuf,
                w_sem, loc_sem, own_sem, ici_s, ici_r, d2d_s, d2d_r, mi_s, mi_r, mo_s, mo_r, md_s, md_r, o_sem):
    rows, d_model = h_own.shape[0] // 2, h_own.shape[1]
    half = rows // 2
    width = d_model // 2
    pairs = width // PAIR
    tiles = 2 * rows // TILE
    mrows = mbuf.shape[0]
    n_chip = n_sp // 2
    me = lax.axis_index("sp")
    chip, core = me // 2, lax.rem(me, 2)
    other = 1 - core
    right, left = lax.rem(chip + 1, n_chip), lax.rem(chip + n_chip - 1, n_chip)
    opp = lax.rem(chip + 2, n_chip)
    partner = 2 * chip + other
    dev_r, dev_l = 2 * right + core, 2 * left + core

    def remote(src, dst, send, recv, dev):
        return pltpu.make_async_remote_copy(
            src_ref=src, dst_ref=dst, send_sem=send, recv_sem=recv, device_id={"sp": dev}, device_id_type=MESH)

    cols = pl.ds(pl.multiple_of(core * width, 128), width)
    own_rows = pl.ds(pl.multiple_of(core * rows, rows), rows)
    load_h = pltpu.make_async_copy(h_hbm, h_own.at[own_rows], loc_sem.at[0])
    load_m = pltpu.make_async_copy(mkv_hbm.at[layer], mbuf, loc_sem.at[1])
    load_w = [pltpu.make_async_copy(src.at[layer, :, cols], dst, w_sem.at[i])
              for i, (src, dst) in enumerate(((wq_hbm, wq), (wk_hbm, wk), (wv_hbm, wv)))]
    load_h.start()
    load_m.start()
    for copy in load_w:
        copy.start()

    barrier = pltpu.get_barrier_semaphore()
    for dev in (dev_r, dev_l, partner):
        pl.semaphore_signal(barrier, inc=1, device_id={"sp": dev}, device_id_type=MESH)
    pl.semaphore_wait(barrier, 3)

    load_h.wait()
    mine = pl.ds(pl.multiple_of(core * half, half), half)
    own_a = h_own.at[pl.ds(pl.multiple_of(core * rows, half), half)]
    own_b = h_own.at[pl.ds(pl.multiple_of(core * rows + half, half), half)]
    send_own = remote(h_own.at[own_rows], h_own.at[own_rows], own_sem.at[0], own_sem.at[1], partner)
    sends = [
        remote(own_a, h_rem.at[0, mine], ici_s.at[0], ici_r.at[0], dev_r),
        remote(own_b, h_rem.at[1, mine], ici_s.at[1], ici_r.at[1], dev_l),
        remote(own_b, h_rem.at[2, mine], ici_s.at[2], ici_r.at[2], dev_r),
        remote(own_a, h_rem.at[3, mine], ici_s.at[3], ici_r.at[3], dev_l),
    ]
    relays = [
        remote(h_rem.at[0, mine], h_rem.at[4, mine], ici_s.at[4], ici_r.at[4], dev_r),
        remote(h_rem.at[1, mine], h_rem.at[5, mine], ici_s.at[5], ici_r.at[5], dev_l),
    ]
    arrive = [*sends, *relays]
    forward = [remote(h_rem.at[i, mine], h_rem.at[i, mine], d2d_s.at[i], d2d_r.at[i], partner) for i in range(6)]
    send_own.start()
    for copy in sends:
        copy.start()

    load_m.wait()
    mh = mrows // 2
    blk_l, blk_r, blk_o = 2 * left + core, 2 * right + core, 2 * opp + core
    m_local = pltpu.make_async_copy(mbuf, mall_hbm.at[me], loc_sem.at[2])
    m_own = [
        remote(mbuf, mall_hbm.at[me], mi_s.at[0], mi_r.at[0], dev_r),
        remote(mbuf, mall_hbm.at[me], mi_s.at[1], mi_r.at[1], dev_l),
        remote(mbuf, mall_hbm.at[me], md_s.at[0], md_r.at[0], partner),
    ]
    m_from = [
        remote(mbuf, mall_hbm.at[blk_l], mi_s.at[0], mi_r.at[0], dev_r),
        remote(mbuf, mall_hbm.at[blk_r], mi_s.at[1], mi_r.at[1], dev_l),
    ]
    m_relay = [
        remote(mall_hbm.at[blk_l, :mh], mall_hbm.at[blk_l, :mh], mo_s.at[0], mo_r.at[0], dev_r),
        remote(mall_hbm.at[blk_r, mh:], mall_hbm.at[blk_r, mh:], mo_s.at[1], mo_r.at[1], dev_l),
    ]
    m_relayed = [
        remote(mall_hbm.at[blk_o, :mh], mall_hbm.at[blk_o, :mh], mo_s.at[0], mo_r.at[0], dev_r),
        remote(mall_hbm.at[blk_o, mh:], mall_hbm.at[blk_o, mh:], mo_s.at[1], mo_r.at[1], dev_l),
    ]
    m_fwd = [
        remote(mall_hbm.at[blk_l], mall_hbm.at[blk_l], md_s.at[1], md_r.at[1], partner),
        remote(mall_hbm.at[blk_r], mall_hbm.at[blk_r], md_s.at[2], md_r.at[2], partner),
        remote(mall_hbm.at[blk_o, :mh], mall_hbm.at[blk_o, :mh], md_s.at[3], md_r.at[3], partner),
        remote(mall_hbm.at[blk_o, mh:], mall_hbm.at[blk_o, mh:], md_s.at[4], md_r.at[4], partner),
    ]
    m_local.start()
    m_own[2].start()

    m_ref[...] = jnp.full_like(m_ref, MASK_VALUE)
    l_ref[...] = jnp.zeros_like(l_ref)
    acc[...] = jnp.zeros_like(acc)
    qm[...] = jnp.zeros_like(qm)
    for copy in load_w:
        copy.wait()
    wqt[...] = wq[...].T
    wvt[...] = wv[...].T

    def project_kv(h_chunk):
        k_val = dot(h_chunk[...], wk[...]).astype(BF16)
        for p in range(pairs):
            k_s[p] = k_val[:, p * PAIR:(p + 1) * PAIR]
        v_val = dot(wvt[...], h_chunk[...], NT).astype(BF16)
        for p in range(pairs):
            vt_s[p] = v_val[p * PAIR:(p + 1) * PAIR]

    def project_q(block):
        h_blk = h_own[pl.ds(pl.multiple_of(block * rows, rows), rows)]
        q_val = (dot(wqt[...], h_blk, NT).astype(BF16) * ATT_SCALE).astype(BF16)
        for p in range(pairs):
            for t in range(rows // TILE):
                n = p * tiles + block * (rows // TILE) + t
                top = q_val[p * PAIR:p * PAIR + HEAD_DIM, t * TILE:(t + 1) * TILE]
                low = q_val[p * PAIR + HEAD_DIM:(p + 1) * PAIR, t * TILE:(t + 1) * TILE]
                qm[n, :HEAD_DIM, :TILE] = top
                qm[n, HEAD_DIM:, TILE:] = low

    def scores(p, n, buf, mc, size=CHUNK, mask=None):
        col_scores(k_s[p, :size], qm[n], buf, size, mask, m_ref[n], mc)

    def softmax(p, n, buf, mc, size=CHUNK):
        e, alpha = col_softmax(buf, size, mc, n, m_ref, l_ref)
        top = dot(vt_s[p, :HEAD_DIM, :size], e[:, :TILE])
        low = dot(vt_s[p, HEAD_DIM:, :size], e[:, TILE:])
        acc[n, :HEAD_DIM] = acc[n, :HEAD_DIM] * alpha[:, :TILE] + top
        acc[n, HEAD_DIM:] = acc[n, HEAD_DIM:] * alpha[:, TILE:] + low

    def attend(first_tile, n_tiles):
        steps = pairs * n_tiles // 2

        def item(i):
            i = jnp.minimum(i, 2 * steps - 1)
            p = i // n_tiles
            return p, p * tiles + first_tile + lax.rem(i, n_tiles)

        scores(*item(0), b0, mc0)

        def body(i, carry):
            scores(*item(2 * i + 1), b1, mc1)
            softmax(*item(2 * i), b0, mc0)
            scores(*item(2 * i + 2), b0, mc0)
            softmax(*item(2 * i + 1), b1, mc1)
            return carry

        lax.fori_loop(0, steps, body, 0)

    def attend_diagonal(block):
        key = lax.broadcasted_iota(jnp.int32, (CHUNK, 2 * TILE), 0)
        query = lax.broadcasted_iota(jnp.int32, (CHUNK, 2 * TILE), 1) % TILE
        first, second = key[:TILE] <= query[:TILE], key <= query + TILE

        def body(p, carry):
            n = p * tiles + block * (rows // TILE)
            scores(p, n, b0, mc0, TILE, first)
            scores(p, n + 1, b1, mc1, CHUNK, second)
            softmax(p, n, b0, mc0, TILE)
            softmax(p, n + 1, b1, mc1, CHUNK)
            return carry

        lax.fori_loop(0, pairs, body, 0)

    remote(h_own.at[pl.ds(pl.multiple_of(other * rows, rows), rows)],
           h_own.at[pl.ds(pl.multiple_of(other * rows, rows), rows)], own_sem.at[0], own_sem.at[1], partner).wait_recv()
    project_q(0)
    project_q(1)
    project_kv(h_own.at[:rows])
    attend_diagonal(0)
    attend(tiles // 2, tiles // 2)
    project_kv(h_own.at[rows:])
    attend_diagonal(1)

    def attend_slots(first, needed):
        for i, need in enumerate(needed):
            @pl.when(need)
            def _(i=i):
                project_kv(h_rem.at[first + i])
                attend(0, tiles)

    need_l, need_r, need_o = left < chip, right < chip, opp < chip

    arrive[0].wait_recv()
    relays[0].start()
    forward[0].start()
    arrive[1].wait_recv()
    relays[1].start()
    forward[1].start()
    m_own[0].start()
    m_own[1].start()
    forward[0].wait_recv()
    forward[1].wait_recv()
    attend_slots(0, (need_l, need_r))
    for i in (2, 3):
        arrive[i].wait_recv()
        forward[i].start()
    forward[2].wait_recv()
    forward[3].wait_recv()
    attend_slots(2, (need_l, need_r))
    for i in (4, 5):
        arrive[i].wait_recv()
        forward[i].start()
    m_from[0].wait_recv()
    m_relay[0].start()
    m_fwd[0].start()
    m_from[1].wait_recv()
    m_relay[1].start()
    m_fwd[1].start()
    forward[4].wait_recv()
    forward[5].wait_recv()
    attend_slots(4, (need_o, need_o))

    def finish(block, slot):
        for p in range(pairs):
            for t in range(rows // TILE):
                n = p * tiles + block * (rows // TILE) + t
                inv = 1.0 / l_ref[n]
                val = jnp.concatenate(
                    [acc[n, :HEAD_DIM] * inv[:, :TILE], acc[n, HEAD_DIM:] * inv[:, TILE:]], axis=0)
                o_stage[slot, t * TILE:(t + 1) * TILE, p * PAIR:(p + 1) * PAIR] = val.astype(BF16).T

    finish(other, 0)
    finish(core, 1)
    o_send = remote(o_stage.at[0], o_hbm.at[:, cols], o_sem.at[0], o_sem.at[1], partner)
    o_recv = remote(o_stage.at[0], o_hbm.at[:, pl.ds(pl.multiple_of(other * width, 128), width)], o_sem.at[0],
                    o_sem.at[1], partner)
    o_keep = pltpu.make_async_copy(o_stage.at[1], o_hbm.at[:, cols], loc_sem.at[3])
    o_send.start()
    o_keep.start()

    m_relayed[0].wait_recv()
    m_fwd[2].start()
    m_relayed[1].wait_recv()
    m_fwd[3].start()
    m_part = [2 * chip + other, 2 * left + other, 2 * right + other, 2 * opp + other]
    for i, view in enumerate((mall_hbm.at[m_part[0]], mall_hbm.at[m_part[1]], mall_hbm.at[m_part[2]],
                              mall_hbm.at[m_part[3], :mh], mall_hbm.at[m_part[3], mh:])):
        remote(view, view, md_s.at[i], md_r.at[i], partner).wait_recv()
    m_local.wait()
    send_own.wait_send()
    for copy in (*sends, *relays, *forward, *m_own, *m_relay, *m_fwd, o_send):
        copy.wait_send()
    o_keep.wait()
    o_recv.wait_recv()


def self_call(layer, n_sp, h, mkv, self_q, self_k, self_v):
    rows, d_model = h.shape
    width = d_model // 2
    pairs, tiles = width // PAIR, 2 * rows // TILE
    combos = pairs * tiles
    mrows, mcols = mkv.shape[1:]
    dma = pltpu.SemaphoreType.DMA
    return pl.pallas_call(
        functools.partial(self_kernel, layer, n_sp),
        out_shape=(
            jax.ShapeDtypeStruct((rows, d_model), BF16),
            jax.ShapeDtypeStruct((n_sp, mrows, mcols), BF16),
        ),
        in_specs=[ANY] * 5,
        out_specs=(ANY, ANY),
        scratch_shapes=[
            pltpu.VMEM((2 * rows, d_model), BF16),
            pltpu.VMEM((6, rows, d_model), BF16),
            *[pltpu.VMEM((d_model, width), BF16)] * 3,
            *[pltpu.VMEM((width, d_model), BF16)] * 2,
            pltpu.VMEM((combos, PAIR, 2 * TILE), BF16),
            pltpu.VMEM((pairs, CHUNK, PAIR), BF16),
            pltpu.VMEM((pairs, PAIR, CHUNK), BF16),
            *[pltpu.VMEM((combos, 1, 2 * TILE), F32)] * 2,
            pltpu.VMEM((combos, PAIR, TILE), F32),
            *[pltpu.VMEM((CHUNK, 2 * TILE), F32)] * 2,
            *[pltpu.VMEM((1, 2 * TILE), F32)] * 2,
            pltpu.VMEM((2, rows, width), BF16),
            pltpu.VMEM((mrows, mcols), BF16),
            dma((3,)), dma((4,)), dma((2,)), dma((6,)), dma((6,)), dma((6,)), dma((6,)),
            dma((2,)), dma((2,)), dma((2,)), dma((2,)), dma((5,)), dma((5,)), dma((2,)),
        ],
        compiler_params=pltpu.CompilerParams(
            collective_id=layer, has_side_effects=True, vmem_limit_bytes=VMEM_LIMIT),
        name=f"self{layer}",
    )(h, mkv, self_q, self_k, self_v)


def post_kernel(layer, last, len_ref, y_hbm, o_hbm, mall_hbm, gain_c, gain_m, gain_n, wo_hbm, cq_hbm, co_hbm, wg_hbm,
                wu_hbm, wd_hbm, *rest):
    n_out = 1 if last else 2
    outs, rest = rest[:n_out], rest[n_out:]
    y, o, mall, wo, cq, co, wg, wu, wd, k_s, vt_s, qm, m_ref, l_ref, acc, b0, b1, mc0, mc1, o2, act, sem = rest
    rows, d_model = y.shape
    mrows = mall.shape[1]
    kv_dim = mall.shape[2] // 2
    n_kv = kv_dim // HEAD_DIM
    pairs = d_model // PAIR
    tiles = rows // TILE
    group = pairs // n_kv
    loads = {}
    for i, (name, src, dst) in enumerate((
            ("o", o_hbm, o), ("wo", wo_hbm.at[layer], wo), ("y", y_hbm, y), ("cq", cq_hbm.at[layer], cq),
            ("mall", mall_hbm.at[:mall.shape[0]], mall), ("co", co_hbm.at[layer], co), ("wg", wg_hbm.at[layer], wg),
            ("wu", wu_hbm.at[layer], wu), ("wd", wd_hbm.at[layer], wd))):
        loads[name] = pltpu.make_async_copy(src, dst, sem.at[i])
        loads[name].start()
    m_ref[...] = jnp.full_like(m_ref, MASK_VALUE)
    l_ref[...] = jnp.zeros_like(l_ref)
    acc[...] = jnp.zeros_like(acc)

    loads["o"].wait()
    loads["wo"].wait()
    upd = dot(o[...], wo[...])
    loads["y"].wait()
    y1 = (y[...].astype(F32) + upd).astype(BF16)
    y[...] = y1
    h = rms_norm(y1.astype(F32), gain_c[layer:layer + 1])
    loads["cq"].wait()
    q_val = (dot(h, cq[...]).astype(BF16) * ATT_SCALE).astype(BF16)
    for p in range(pairs):
        qt = q_val[:, p * PAIR:(p + 1) * PAIR].T
        for t in range(tiles):
            qm[p * tiles + t, :, :TILE] = qt[:HEAD_DIM, t * TILE:(t + 1) * TILE]
            qm[p * tiles + t, :, TILE:] = qt[HEAD_DIM:, t * TILE:(t + 1) * TILE]
    loads["mall"].wait()
    for b in range(mall.shape[0]):
        span = slice(b * mrows, (b + 1) * mrows)
        vt = mall[b, :, kv_dim:].T
        for g in range(n_kv):
            k_s[g, span] = mall[b, :, g * HEAD_DIM:(g + 1) * HEAD_DIM]
            vt_s[g, :, span] = vt[g * HEAD_DIM:(g + 1) * HEAD_DIM]

    mem_len = len_ref[0]
    combos = pairs * tiles

    def chunk(c, carry):
        off = pl.multiple_of(c * CHUNK, CHUNK)
        mask = lax.broadcasted_iota(jnp.int32, (CHUNK, 2 * TILE), 0) + off < mem_len

        def item(i):
            n = jnp.minimum(i, combos - 1)
            return n // (tiles * group), n

        def scores(g, n, buf, mc):
            col_scores(k_s[g, pl.ds(off, CHUNK)], qm[n], buf, CHUNK, mask, m_ref[n], mc)

        def softmax(g, n, buf, mc):
            e, alpha = col_softmax(buf, CHUNK, mc, n, m_ref, l_ref)
            acc[n] = acc[n] * alpha + dot(vt_s[g, :, pl.ds(off, CHUNK)], e)

        scores(*item(0), b0, mc0)

        def body(i, inner):
            scores(*item(2 * i + 1), b1, mc1)
            softmax(*item(2 * i), b0, mc0)
            scores(*item(2 * i + 2), b0, mc0)
            softmax(*item(2 * i + 1), b1, mc1)
            return inner

        return lax.fori_loop(0, combos // 2, body, carry)

    lax.fori_loop(0, pl.cdiv(mem_len, CHUNK), chunk, 0)
    for p in range(pairs):
        for t in range(tiles):
            n = p * tiles + t
            val = acc[n] * (1.0 / l_ref[n])
            val = jnp.concatenate([val[:, :TILE], val[:, TILE:]], axis=0)
            o2[t * TILE:(t + 1) * TILE, p * PAIR:(p + 1) * PAIR] = val.astype(BF16).T
    loads["co"].wait()
    y2 = (y[...].astype(F32) + dot(o2[...], co[...])).astype(BF16)
    y[...] = y2
    h = rms_norm(y2.astype(F32), gain_m[layer:layer + 1])
    loads["wg"].wait()
    loads["wu"].wait()
    ff = act.shape[1]
    for c in range(0, ff, CHUNK):
        gate = dot(h, wg[:, c:c + CHUNK])
        act[:, c:c + CHUNK] = (jax.nn.silu(gate) * dot(h, wu[:, c:c + CHUNK])).astype(BF16)
    loads["wd"].wait()
    y3 = (y[...].astype(F32) + dot(act[...], wd[...])).astype(BF16)
    outs[0][...] = y3
    if not last:
        outs[1][...] = rms_norm(y3.astype(F32), gain_n[layer + 1:layer + 2])


def post_call(layer, last, mem_len, y, o, mall, gain_cross, gain_mlp, gain_self, self_o, cross_q, cross_o, gate, up, down):
    rows, d_model = y.shape
    ff = gate.shape[2]
    mrows, mcols = mall.shape[1:]
    used = min(mall.shape[0], pl.cdiv(MAX_MEM_LEN, mrows))
    kv_dim = mcols // 2
    n_kv = kv_dim // HEAD_DIM
    combos = (d_model // PAIR) * (rows // TILE)
    row = jax.ShapeDtypeStruct((rows, d_model), BF16)
    n_out = 1 if last else 2
    return pl.pallas_call(
        functools.partial(post_kernel, layer, last),
        out_shape=(row,) * n_out,
        in_specs=[SMEM, ANY, ANY, ANY, VMEM, VMEM, VMEM] + [ANY] * 6,
        out_specs=(VMEM,) * n_out,
        scratch_shapes=[
            pltpu.VMEM((rows, d_model), BF16),
            pltpu.VMEM((rows, d_model), BF16),
            pltpu.VMEM((used, mrows, mcols), BF16),
            *[pltpu.VMEM((d_model, d_model), BF16)] * 3,
            *[pltpu.VMEM((d_model, ff), BF16)] * 2,
            pltpu.VMEM((ff, d_model), BF16),
            pltpu.VMEM((n_kv, used * mrows, HEAD_DIM), BF16),
            pltpu.VMEM((n_kv, HEAD_DIM, used * mrows), BF16),
            pltpu.VMEM((combos, HEAD_DIM, 2 * TILE), BF16),
            *[pltpu.VMEM((combos, 1, 2 * TILE), F32)] * 2,
            pltpu.VMEM((combos, HEAD_DIM, 2 * TILE), F32),
            *[pltpu.VMEM((CHUNK, 2 * TILE), F32)] * 2,
            *[pltpu.VMEM((1, 2 * TILE), F32)] * 2,
            pltpu.VMEM((rows, d_model), BF16),
            pltpu.VMEM((rows, ff), BF16),
            pltpu.SemaphoreType.DMA((9,)),
        ],
        compiler_params=pltpu.CompilerParams(vmem_limit_bytes=VMEM_LIMIT),
        name=f"post{layer}",
    )(mem_len, y, o, mall, gain_cross, gain_mlp, gain_self, self_o, cross_q, cross_o, gate, up, down)


def solution(mesh):
    n_sp = mesh.shape["sp"]
    row_spec = P(("dp", "sp"), None)

    def device_fn(dec_hidden, memory, mem_len, gain_self, gain_cross, gain_mlp, self_q, self_k, self_v, self_o, cross_q,
                  cross_k, cross_v, cross_o, mlp_gate, mlp_up, mlp_down):
        layers = gain_self.shape[0]
        hidden = dec_hidden
        normed, mkv = pre_call(dec_hidden, memory, gain_self, cross_k, cross_v)
        for layer in range(layers):
            last = layer == layers - 1
            attn, mall = self_call(layer, n_sp, normed, mkv, self_q, self_k, self_v)
            out = post_call(layer, last, mem_len, hidden, attn, mall, gain_cross, gain_mlp, gain_self, self_o, cross_q,
                            cross_o, mlp_gate, mlp_up, mlp_down)
            hidden, normed = out[0], out[-1]
        return hidden

    return jax.shard_map(device_fn, mesh=mesh, in_specs=(row_spec, row_spec, P("dp")) + (P(),) * 14,
                         out_specs=row_spec, check_vma=False)
```

```python
import functools

import jax
import jax.numpy as jnp
from jax import lax
from jax.experimental import pallas as pl
from jax.experimental.pallas import tpu as pltpu
from jax.sharding import PartitionSpec as P

HEAD_DIM = 64
NORM_EPS = 1e-6
MASK_VALUE = -1e30
ATT_SCALE = HEAD_DIM ** -0.5
MAX_MEM_LEN = 1536
PAIR = 2 * HEAD_DIM
TILE = 256
CHUNK = 512
NN = (((1,), (0,)), ((), ()))
NT = (((1,), (1,)), ((), ()))
F32 = jnp.float32
BF16 = jnp.bfloat16
MESH = pl.DeviceIdType.MESH
VMEM_LIMIT = 60 * 1024 * 1024
ANY = pl.BlockSpec(memory_space=pl.ANY)
VMEM = pl.BlockSpec(memory_space=pltpu.VMEM)
SMEM = pl.BlockSpec(memory_space=pltpu.SMEM)


def rms_norm(val32, gain_row):
    inv_rms = lax.rsqrt(jnp.mean(val32 * val32, axis=-1, keepdims=True) + NORM_EPS)
    return (val32 * inv_rms * gain_row).astype(BF16)


def dot(lhs, rhs, dims=NN):
    return lax.dot_general(lhs, rhs, dims, preferred_element_type=F32)


def col_scores(k_val, q_val, buf, size, mask, m_prev, mc):
    s = dot(k_val, q_val)
    if mask is not None:
        s = jnp.where(mask, s, MASK_VALUE)
    buf[:size] = s
    mc[...] = jnp.maximum(m_prev, jnp.max(s, axis=0, keepdims=True))


def col_softmax(buf, size, mc, n, m_ref, l_ref):
    m_new = mc[...]
    alpha = jnp.exp(m_ref[n] - m_new)
    e = jnp.exp(buf[:size] - m_new)
    l_ref[n] = l_ref[n] * alpha + jnp.sum(e, axis=0, keepdims=True)
    m_ref[n] = m_new
    return e.astype(BF16), alpha


def layer_kernel(n_sp, n_layers, len_ref, hid_hbm, mem_hbm, gain_s, gain_c, gain_m, wq_hbm, wk_hbm, wv_hbm, wo_hbm, cq_hbm,
                 ck_hbm, cv_hbm, co_hbm, wg_hbm, wu_hbm, wd_hbm, out_ref,
                 y, h_own, h_rem, mem, ck, cv, mkv, mall, wq, wk, wv, wqt, wvt, wo, cq, co, wg, wu, wd,
                 qm, qc, k_s, vt_s, k_c, vt_c, m_ref, l_ref, acc, b0, b1, mc0, mc1, o_stage, o_full, act, gains,
                 w_sem, own_sem, ici_s, ici_r, d2d_s, d2d_r, mi_s, mi_r, mo_s, mo_r, md_s, md_r, o_sem):
    rows, d_model = y.shape
    half = rows // 2
    width = d_model // 2
    pairs = width // PAIR
    tiles = 2 * rows // TILE
    row_tiles = rows // TILE
    all_pairs = d_model // PAIR
    used, _, mrows, mcols = mall.shape
    mh = mrows // 2
    kv_dim = mcols // 2
    n_kv = kv_dim // HEAD_DIM
    group = all_pairs // n_kv
    ff = act.shape[1]
    n_chip = n_sp // 2
    me = lax.axis_index("sp")
    chip, core = me // 2, lax.rem(me, 2)
    other = 1 - core
    right, left = lax.rem(chip + 1, n_chip), lax.rem(chip + n_chip - 1, n_chip)
    opp = lax.rem(chip + 2, n_chip)
    partner = 2 * chip + other
    dev_r, dev_l = 2 * right + core, 2 * left + core

    def remote(src, dst, send, recv, dev):
        return pltpu.make_async_remote_copy(
            src_ref=src, dst_ref=dst, send_sem=send, recv_sem=recv, device_id={"sp": dev}, device_id_type=MESH)

    cols = pl.ds(pl.multiple_of(core * width, 128), width)
    own_rows = pl.ds(pl.multiple_of(core * rows, rows), rows)
    other_rows = pl.ds(pl.multiple_of(other * rows, rows), rows)
    mine = pl.ds(pl.multiple_of(core * half, half), half)

    def loads(layer):
        specs = [(wq_hbm.at[layer, :, cols], wq), (wk_hbm.at[layer, :, cols], wk), (wv_hbm.at[layer, :, cols], wv),
                 (wo_hbm.at[layer], wo), (cq_hbm.at[layer], cq), (co_hbm.at[layer], co), (wg_hbm.at[layer], wg),
                 (wu_hbm.at[layer], wu), (wd_hbm.at[layer], wd)]
        return [pltpu.make_async_copy(src, dst, w_sem.at[i]) for i, (src, dst) in enumerate(specs)]

    first = [pltpu.make_async_copy(src, dst, w_sem.at[9 + i])
             for i, (src, dst) in enumerate(((hid_hbm, y), (mem_hbm, mem), (ck_hbm, ck), (cv_hbm, cv)))]
    first[0].start()
    w_first = loads(0)
    for copy in (*w_first[:3], *first[1:], *w_first[3:]):
        copy.start()

    barrier = pltpu.get_barrier_semaphore()
    for dev in (dev_r, dev_l, partner):
        pl.semaphore_signal(barrier, inc=1, device_id={"sp": dev}, device_id_type=MESH)

    for i, ref in enumerate((gain_s, gain_c, gain_m)):
        for j in range(n_layers):
            gains[i, j] = ref[j:j + 1].astype(F32)

    first[0].wait()
    h_own[0, own_rows] = rms_norm(y[...].astype(F32), gains[0, 0])
    pl.semaphore_wait(barrier, 3)

    to_r, to_l = chip < right, chip < left
    b_to_l = to_l | (chip < opp)
    relay_a, relay_b = left < right, right < left
    need_l, need_r, need_o = left < chip, right < chip, opp < chip
    got_rb = need_r | relay_b
    need = (need_l, need_r, need_l, need_r, need_o, need_o)
    got = (need_l, got_rb, need_l, need_r, need_o, need_o)
    sent = (to_r, b_to_l, to_r, to_l)

    def row_copies(layer):
        own_a = h_own.at[layer, pl.ds(pl.multiple_of(core * rows, half), half)]
        own_b = h_own.at[layer, pl.ds(pl.multiple_of(core * rows + half, half), half)]
        slot = [h_rem.at[layer, i, mine] for i in range(6)]
        srcs = (own_a, own_b, own_b, own_a, slot[0], slot[1])
        ring = [remote(srcs[i], slot[i], ici_s.at[layer, i], ici_r.at[layer, i], dev_l if i % 2 else dev_r)
                for i in (0, 1)]
        ring += [remote(srcs[2], slot[2], ici_s.at[layer, 2], ici_r.at[layer, 2], dev_r),
                 remote(srcs[3], slot[3], ici_s.at[layer, 3], ici_r.at[layer, 3], dev_l),
                 remote(srcs[4], slot[4], ici_s.at[layer, 4], ici_r.at[layer, 4], dev_r),
                 remote(srcs[5], slot[5], ici_s.at[layer, 5], ici_r.at[layer, 5], dev_l)]
        fwd = [remote(slot[i], slot[i], d2d_s.at[layer, i], d2d_r.at[layer, i], partner) for i in range(6)]
        own = remote(h_own.at[layer, own_rows], h_own.at[layer, own_rows], own_sem.at[layer, 0], own_sem.at[layer, 1],
                     partner)
        return ring, fwd, own

    def when_start(cond, copy):
        @pl.when(cond)
        def _():
            copy.start()

    def when_sent(cond, copy):
        @pl.when(cond)
        def _():
            copy.wait_send()

    def when_recv(cond, copy):
        @pl.when(cond)
        def _():
            copy.wait_recv()

    has_m = 2 * chip < used
    has_l, has_r, has_o = 2 * left < used, 2 * right < used, 2 * opp < used

    def blk(who, core_of):
        return jnp.minimum(2 * who + core_of, used - 1)

    b_me, b_l, b_r, b_o = blk(chip, core), blk(left, core), blk(right, core), blk(opp, core)
    top, low = pl.ds(0, mh), pl.ds(mh, mh)
    m_own = [
        remote(mkv, mall.at[b_me], mi_s.at[0], mi_r.at[0], dev_r),
        remote(mkv, mall.at[b_me], mi_s.at[1], mi_r.at[1], dev_l),
        remote(mkv, mall.at[b_me], md_s.at[0], md_r.at[0], partner),
    ]
    m_relay = [
        remote(mall.at[b_l, :, top], mall.at[b_l, :, top], mo_s.at[0], mo_r.at[0], dev_r),
        remote(mall.at[b_r, :, low], mall.at[b_r, :, low], mo_s.at[1], mo_r.at[1], dev_l),
    ]
    m_fwd = [
        remote(mall.at[b_l], mall.at[b_l], md_s.at[1], md_r.at[1], partner),
        remote(mall.at[b_r], mall.at[b_r], md_s.at[2], md_r.at[2], partner),
        remote(mall.at[b_o, :, top], mall.at[b_o, :, top], md_s.at[3], md_r.at[3], partner),
        remote(mall.at[b_o, :, low], mall.at[b_o, :, low], md_s.at[4], md_r.at[4], partner),
    ]
    m_has = (has_l, has_r, has_o, has_o)

    def start_rows(layer):
        ring, _, own = row_copies(layer)
        own.start()
        when_start(sent[0], ring[0])
        when_start(sent[1], ring[1])

    start_rows(0)
    for copy in first[1:]:
        copy.wait()
    for i in range(n_layers):
        mkv[i, :, :kv_dim] = dot(mem[...], ck[i]).astype(BF16)
        mkv[i, :, kv_dim:] = dot(mem[...], cv[i]).astype(BF16)

    @pl.when(has_m)
    def _():
        mall[b_me] = mkv[...]

    qm[...] = jnp.zeros_like(qm)
    ones_row = (lax.broadcasted_iota(jnp.int32, (PAIR - HEAD_DIM, 2 * TILE), 0) == 0).astype(F32).astype(BF16)
    for n in range(qc.shape[0]):
        qc[n, HEAD_DIM:] = ones_row

    def reset():
        m_ref[...] = jnp.full_like(m_ref, MASK_VALUE)
        l_ref[...] = jnp.zeros_like(l_ref)
        acc[...] = jnp.zeros_like(acc)

    def scores_of(k_val, q_val, n, buf, mc, size=CHUNK, mask=None):
        col_scores(k_val, q_val, buf, size, mask, m_ref[n], mc)

    def softmax_of(vt_top, vt_low, n, buf, mc, size=CHUNK):
        e, alpha = col_softmax(buf, size, mc, n, m_ref, l_ref)
        acc[n, :HEAD_DIM] = acc[n, :HEAD_DIM] * alpha[:, :TILE] + dot(vt_top, e[:, :TILE])
        acc[n, HEAD_DIM:] = acc[n, HEAD_DIM:] * alpha[:, TILE:] + dot(vt_low, e[:, TILE:])

    def pipelined(count, unroll, item, scores, softmax):
        bufs, mcs = (b0, b1), (mc0, mc1)

        def at(i):
            return item(jnp.minimum(i, count - 1))

        scores(at(0), b0, mc0)

        def body(i, carry):
            for u in range(unroll):
                scores(at(unroll * i + u + 1), bufs[(u + 1) % 2], mcs[(u + 1) % 2])
                softmax(at(unroll * i + u), bufs[u % 2], mcs[u % 2])
            return carry

        lax.fori_loop(0, count // unroll, body, 0)

    def finish(n):
        inv = 1.0 / l_ref[n]
        val = jnp.concatenate([acc[n, :HEAD_DIM] * inv[:, :TILE], acc[n, HEAD_DIM:] * inv[:, TILE:]], axis=0)
        return val.astype(BF16).T

    def project_kv(h_chunk):
        k_val = dot(h_chunk, wk[...]).astype(BF16)
        v_val = dot(wvt[...], h_chunk, NT).astype(BF16)
        for p in range(pairs):
            k_s[p] = k_val[:, p * PAIR:(p + 1) * PAIR]
            vt_s[p] = v_val[p * PAIR:(p + 1) * PAIR]

    def self_scores(pn, buf, mc, size=CHUNK, mask=None):
        p, n = pn
        scores_of(k_s[p, :size], qm[n], n, buf, mc, size, mask)

    def self_softmax(pn, buf, mc, size=CHUNK):
        p, n = pn
        softmax_of(vt_s[p, :HEAD_DIM, :size], vt_s[p, HEAD_DIM:, :size], n, buf, mc, size)

    def attend(first_tile, n_tiles, unroll):
        def item(i):
            p = i // n_tiles
            return p, p * tiles + first_tile + lax.rem(i, n_tiles)

        pipelined(pairs * n_tiles, unroll, item, self_scores, self_softmax)

    def layer_body(layer, carry):
        ring, fwd, own = row_copies(layer)
        weights = loads(layer)
        reset()
        for copy in weights[:3]:
            copy.wait()
        wqt[...] = wq[...].T
        wvt[...] = wv[...].T
        own.wait_recv()

        def own_block(block, inner):
            h_blk = h_own[layer, pl.ds(pl.multiple_of(block * rows, rows), rows)]
            q_val = (dot(wqt[...], h_blk, NT).astype(BF16) * ATT_SCALE).astype(BF16)
            for p in range(pairs):
                for t in range(row_tiles):
                    n = p * tiles + block * row_tiles + t
                    span = slice(t * TILE, (t + 1) * TILE)
                    qm[n, :HEAD_DIM, :TILE] = q_val[p * PAIR:p * PAIR + HEAD_DIM, span]
                    qm[n, HEAD_DIM:, TILE:] = q_val[p * PAIR + HEAD_DIM:(p + 1) * PAIR, span]
            return inner

        lax.fori_loop(0, 2, own_block, 0)

        def own_keys(block, inner):
            project_kv(h_own[layer, pl.ds(pl.multiple_of(block * rows, rows), rows)])
            key = lax.broadcasted_iota(jnp.int32, (CHUNK, 2 * TILE), 0)
            query = lax.broadcasted_iota(jnp.int32, (CHUNK, 2 * TILE), 1) % TILE

            def diagonal(p, deep):
                n = p * tiles + block * row_tiles
                self_scores((p, n), b0, mc0, TILE, key[:TILE] <= query[:TILE])
                self_scores((p, n + 1), b1, mc1, CHUNK, key <= query + TILE)
                self_softmax((p, n), b0, mc0, TILE)
                self_softmax((p, n + 1), b1, mc1, CHUNK)
                return deep

            lax.fori_loop(0, pairs, diagonal, 0)

            @pl.when(block == 0)
            def _():
                attend(tiles // 2, tiles // 2, 2)

            return inner

        lax.fori_loop(0, 2, own_keys, 0)
        when_start(sent[2], ring[2])
        when_start(sent[3], ring[3])

        def take(i):
            when_recv(got[i], ring[i])
            if i == 0:
                when_start(relay_a, ring[4])
            if i == 1:
                when_start(relay_b, ring[5])
            when_start(need[i], fwd[i])

        def attend_two(stage, inner):
            @pl.when(stage == 0)
            def _():
                take(0)
                take(1)

                @pl.when(layer == 0)
                def _():
                    when_start(has_m, m_own[2])
                    when_start(has_m, m_own[0])
                    when_start(has_m, m_own[1])

                when_recv(need[0], fwd[0])
                when_recv(need[1], fwd[1])

            @pl.when(stage == 1)
            def _():
                take(2)
                take(3)
                when_recv(need[2], fwd[2])
                when_recv(need[3], fwd[3])

            @pl.when(stage == 2)
            def _():
                take(4)
                take(5)
                when_recv(need[4], fwd[4])
                when_recv(need[5], fwd[5])

            def one(i, deep):
                @pl.when((stage == 2) & (i == 1) & (layer == 0))
                def _():
                    when_recv(has_l, m_own[0])
                    when_start(has_l, m_relay[0])
                    when_start(has_l, m_fwd[0])
                    when_recv(has_r, m_own[1])
                    when_start(has_r, m_relay[1])
                    when_start(has_r, m_fwd[1])

                wanted = jnp.where(stage == 2, opp, jnp.where(i == 0, left, right)) < chip

                @pl.when(wanted)
                def _():
                    project_kv(h_rem[layer, 2 * stage + i])
                    attend(0, tiles, 4)

                return deep

            return lax.fori_loop(0, 2, one, inner)

        lax.fori_loop(0, 3, attend_two, 0)

        for block, dst in ((other, o_stage), (core, None)):
            for p in range(pairs):
                for t in range(row_tiles):
                    val = finish(p * tiles + block * row_tiles + t)
                    span = slice(t * TILE, (t + 1) * TILE)
                    if dst is not None:
                        dst[layer, span, p * PAIR:(p + 1) * PAIR] = val
                    else:
                        o_full[layer, core, span, p * PAIR:(p + 1) * PAIR] = val
        o_send = remote(o_stage.at[layer], o_full.at[layer, core], o_sem.at[layer, 0], o_sem.at[layer, 1], partner)
        o_send.start()

        @pl.when(layer + 1 < n_layers)
        def _():
            for copy in loads(layer + 1)[:3]:
                copy.start()

        @pl.when(layer == 0)
        def _():
            when_recv(has_o, m_relay[0])
            when_start(has_o, m_fwd[2])
            when_recv(has_o, m_relay[1])
            when_start(has_o, m_fwd[3])
            when_recv(has_m, m_own[2])
            for cond, copy in zip(m_has, m_fwd):
                when_recv(cond, copy)
            for copy in m_own:
                when_sent(has_m, copy)
            when_sent(has_l, m_relay[0])
            when_sent(has_r, m_relay[1])
            for cond, copy in zip(m_has, m_fwd):
                when_sent(cond, copy)

        reset()
        mem_len = len_ref[0]
        for b in range(used):
            span = slice(b * mrows, (b + 1) * mrows)
            vt = mall[b, layer, :, kv_dim:].T
            pos = lax.broadcasted_iota(jnp.int32, (mrows, HEAD_DIM), 0) + b * mrows
            lane = lax.broadcasted_iota(jnp.int32, (mrows, HEAD_DIM), 1)
            bias = jnp.where((pos >= mem_len) & (lane == 0), MASK_VALUE, 0.0).astype(BF16)
            for g in range(n_kv):
                k_c[g, span, :HEAD_DIM] = mall[b, layer, :, g * HEAD_DIM:(g + 1) * HEAD_DIM]
                k_c[g, span, HEAD_DIM:] = bias
                vt_c[g, :, span] = vt[g * HEAD_DIM:(g + 1) * HEAD_DIM]

        o_send.wait_recv()
        weights[3].wait()
        upd = dot(o_full[layer, 0], wo[:width]) + dot(o_full[layer, 1], wo[width:])
        y1 = (y[...].astype(F32) + upd).astype(BF16)
        y[...] = y1
        h = rms_norm(y1.astype(F32), gains[1, layer])
        weights[4].wait()
        q_val = (dot(h, cq[...]).astype(BF16) * ATT_SCALE).astype(BF16)
        for p in range(all_pairs):
            qt = q_val[:, p * PAIR:(p + 1) * PAIR].T
            for t in range(row_tiles):
                span = slice(t * TILE, (t + 1) * TILE)
                qc[p * row_tiles + t, :HEAD_DIM, :TILE] = qt[:HEAD_DIM, span]
                qc[p * row_tiles + t, :HEAD_DIM, TILE:] = qt[HEAD_DIM:, span]

        def chunk(c, inner):
            off = pl.multiple_of(c * CHUNK, CHUNK)

            def item(n):
                return n // (row_tiles * group), n

            def scores(gn, buf, mc):
                g, n = gn
                scores_of(k_c[g, pl.ds(off, CHUNK)], qc[n], n, buf, mc)

            def softmax(gn, buf, mc):
                g, n = gn
                vt = vt_c[g, :, pl.ds(off, CHUNK)]
                softmax_of(vt, vt, n, buf, mc)

            pipelined(all_pairs * row_tiles, 4, item, scores, softmax)
            return inner

        lax.fori_loop(0, used * mrows // CHUNK, chunk, 0)
        for p in range(all_pairs):
            for t in range(row_tiles):
                o_stage_c[t * TILE:(t + 1) * TILE, p * PAIR:(p + 1) * PAIR] = finish(p * row_tiles + t)
        weights[5].wait()
        y2 = (y[...].astype(F32) + dot(o_stage_c[...], co[...])).astype(BF16)
        y[...] = y2
        h = rms_norm(y2.astype(F32), gains[2, layer])
        weights[6].wait()
        weights[7].wait()
        for c in range(0, ff, CHUNK):
            gate = dot(h, wg[:, c:c + CHUNK])
            act[:, c:c + CHUNK] = (jax.nn.silu(gate) * dot(h, wu[:, c:c + CHUNK])).astype(BF16)
        weights[8].wait()
        y3 = (y[...].astype(F32) + dot(act[...], wd[...])).astype(BF16)
        y[...] = y3

        @pl.when(layer + 1 < n_layers)
        def _():
            h_own[layer + 1, own_rows] = rms_norm(y3.astype(F32), gains[0, layer + 1])
            for copy in loads(layer + 1)[3:]:
                copy.start()
            start_rows(layer + 1)

        own.wait_send()
        o_send.wait_send()
        for cond, copy in zip((*sent, relay_a, relay_b), ring):
            when_sent(cond, copy)
        for cond, copy in zip(need, fwd):
            when_sent(cond, copy)
        return carry

    o_stage_c = act.at[:, :d_model]
    lax.fori_loop(0, n_layers, layer_body, 0)
    out_ref[...] = y[...]


def layers_call(n_sp, mem_len, hidden, memory, gain_self, gain_cross, gain_mlp, self_q, self_k, self_v, self_o, cross_q,
                cross_k, cross_v, cross_o, gate, up, down):
    rows, d_model = hidden.shape
    layers = gain_self.shape[0]
    width = d_model // 2
    ff = gate.shape[2]
    mrows, mcols = memory.shape[0], 2 * cross_k.shape[2]
    used = min(n_sp, pl.cdiv(MAX_MEM_LEN, mrows))
    n_kv = cross_k.shape[2] // HEAD_DIM
    pairs, tiles = width // PAIR, 2 * rows // TILE
    combos = pairs * tiles
    dma = pltpu.SemaphoreType.DMA
    return pl.pallas_call(
        functools.partial(layer_kernel, n_sp, layers),
        out_shape=jax.ShapeDtypeStruct((rows, d_model), BF16),
        in_specs=[SMEM, ANY, ANY, VMEM, VMEM, VMEM] + [ANY] * 11,
        out_specs=VMEM,
        scratch_shapes=[
            pltpu.VMEM((rows, d_model), BF16),
            pltpu.VMEM((layers, 2 * rows, d_model), BF16),
            pltpu.VMEM((layers, 6, rows, d_model), BF16),
            pltpu.VMEM((mrows, d_model), BF16),
            *[pltpu.VMEM(cross_k.shape, BF16)] * 2,
            pltpu.VMEM((layers, mrows, mcols), BF16),
            pltpu.VMEM((used, layers, mrows, mcols), BF16),
            *[pltpu.VMEM((d_model, width), BF16)] * 3,
            *[pltpu.VMEM((width, d_model), BF16)] * 2,
            *[pltpu.VMEM((d_model, d_model), BF16)] * 3,
            *[pltpu.VMEM((d_model, ff), BF16)] * 2,
            pltpu.VMEM((ff, d_model), BF16),
            *[pltpu.VMEM((combos, PAIR, 2 * TILE), BF16)] * 2,
            pltpu.VMEM((pairs, CHUNK, PAIR), BF16),
            pltpu.VMEM((pairs, PAIR, CHUNK), BF16),
            pltpu.VMEM((n_kv, used * mrows, PAIR), BF16),
            pltpu.VMEM((n_kv, HEAD_DIM, used * mrows), BF16),
            *[pltpu.VMEM((combos, 1, 2 * TILE), F32)] * 2,
            pltpu.VMEM((combos, PAIR, TILE), F32),
            *[pltpu.VMEM((CHUNK, 2 * TILE), F32)] * 2,
            *[pltpu.VMEM((1, 2 * TILE), F32)] * 2,
            pltpu.VMEM((layers, rows, width), BF16),
            pltpu.VMEM((layers, 2, rows, width), BF16),
            pltpu.VMEM((rows, ff), BF16),
            pltpu.VMEM((3, layers, 1, d_model), F32),
            dma((13,)), dma((layers, 2)), *[dma((layers, 6))] * 4,
            *[dma((2,))] * 4, *[dma((5,))] * 2, dma((layers, 2)),
        ],
        compiler_params=pltpu.CompilerParams(collective_id=0, has_side_effects=True, vmem_limit_bytes=VMEM_LIMIT),
        name="layers",
    )(mem_len, hidden, memory, gain_self, gain_cross, gain_mlp, self_q, self_k, self_v, self_o, cross_q, cross_k, cross_v,
      cross_o, gate, up, down)


def solution(mesh):
    n_sp = mesh.shape["sp"]
    row_spec = P(("dp", "sp"), None)

    def device_fn(dec_hidden, memory, mem_len, *weights):
        return layers_call(n_sp, mem_len, dec_hidden, memory, *weights)

    return jax.shard_map(device_fn, mesh=mesh, in_specs=(row_spec, row_spec, P("dp")) + (P(),) * 14,
                         out_specs=row_spec, check_vma=False)
```

```python
import functools

import jax
import jax.numpy as jnp
from jax import lax
from jax.experimental import pallas as pl
from jax.experimental.pallas import tpu as pltpu
from jax.sharding import PartitionSpec as P

HEAD_DIM = 64
NORM_EPS = 1e-6
MASK_VALUE = -1e30
ATT_SCALE = HEAD_DIM ** -0.5
MAX_MEM_LEN = 1536
PAIR = 2 * HEAD_DIM
TILE = 256
CHUNK = 512
NN = (((1,), (0,)), ((), ()))
NT = (((1,), (1,)), ((), ()))
F32 = jnp.float32
BF16 = jnp.bfloat16
MESH = pl.DeviceIdType.MESH
VMEM_LIMIT = 60 * 1024 * 1024
ANY = pl.BlockSpec(memory_space=pl.ANY)
VMEM = pl.BlockSpec(memory_space=pltpu.VMEM)
SMEM = pl.BlockSpec(memory_space=pltpu.SMEM)


def rms_norm(val32, gain_row):
    inv_rms = lax.rsqrt(jnp.mean(val32 * val32, axis=-1, keepdims=True) + NORM_EPS)
    return (val32 * inv_rms * gain_row).astype(BF16)


def dot(lhs, rhs, dims=NN):
    return lax.dot_general(lhs, rhs, dims, preferred_element_type=F32)


def col_scores(k_val, q_val, buf, size, mask, m_prev, mc):
    s = dot(k_val, q_val)
    if mask is not None:
        s = jnp.where(mask, s, MASK_VALUE)
    buf[:size] = s
    mc[...] = jnp.maximum(m_prev, jnp.max(s, axis=0, keepdims=True))


def col_softmax(buf, size, mc, n, m_ref, l_ref):
    m_new = mc[...]
    alpha = jnp.exp(m_ref[n] - m_new)
    e = jnp.exp(buf[:size] - m_new)
    l_ref[n] = l_ref[n] * alpha + jnp.sum(e, axis=0, keepdims=True)
    m_ref[n] = m_new
    return e.astype(BF16), alpha


def layer_kernel(n_sp, n_layers, len_ref, hid_hbm, mem_hbm, gain_s, gain_c, gain_m, wq_hbm, wk_hbm, wv_hbm, wo_hbm, cq_hbm,
                 ck_hbm, cv_hbm, co_hbm, wg_hbm, wu_hbm, wd_hbm, out_ref,
                 y, h_own, h_rem, mem, ck, cv, mkv, mall, wq, wk, wv, wqt, wvt, wo, cq, co, wg, wu, wd,
                 qm, qc, k_s, vt_s, k_c, vt_c, m_ref, l_ref, acc, b0, b1, mc0, mc1, o_stage, o_full, act, gains,
                 w_sem, own_sem, ici_s, ici_r, d2d_s, d2d_r, mi_s, mi_r, mo_s, mo_r, md_s, md_r, o_sem):
    rows, d_model = y.shape
    half = rows // 2
    width = d_model // 2
    pairs = width // PAIR
    tiles = 2 * rows // TILE
    row_tiles = rows // TILE
    all_pairs = d_model // PAIR
    used, _, mrows, mcols = mall.shape
    mh = mrows // 2
    kv_dim = mcols // 2
    n_kv = kv_dim // HEAD_DIM
    group = all_pairs // n_kv
    ff = act.shape[1]
    n_chip = n_sp // 2
    me = lax.axis_index("sp")
    chip, core = me // 2, lax.rem(me, 2)
    other = 1 - core
    right, left = lax.rem(chip + 1, n_chip), lax.rem(chip + n_chip - 1, n_chip)
    opp = lax.rem(chip + 2, n_chip)
    partner = 2 * chip + other
    dev_r, dev_l = 2 * right + core, 2 * left + core

    def remote(src, dst, send, recv, dev):
        return pltpu.make_async_remote_copy(
            src_ref=src, dst_ref=dst, send_sem=send, recv_sem=recv, device_id={"sp": dev}, device_id_type=MESH)

    cols = pl.ds(pl.multiple_of(core * width, 128), width)
    own_rows = pl.ds(pl.multiple_of(core * rows, rows), rows)
    other_rows = pl.ds(pl.multiple_of(other * rows, rows), rows)

    def loads(layer):
        specs = [(wq_hbm.at[layer, :, cols], wq), (wk_hbm.at[layer, :, cols], wk), (wv_hbm.at[layer, :, cols], wv),
                 (wo_hbm.at[layer], wo), (cq_hbm.at[layer], cq), (co_hbm.at[layer], co), (wg_hbm.at[layer], wg),
                 (wu_hbm.at[layer], wu), (wd_hbm.at[layer], wd)]
        return [pltpu.make_async_copy(src, dst, w_sem.at[i]) for i, (src, dst) in enumerate(specs)]

    first = [pltpu.make_async_copy(src, dst, w_sem.at[9 + i])
             for i, (src, dst) in enumerate(((hid_hbm, y), (mem_hbm, mem), (ck_hbm, ck), (cv_hbm, cv)))]
    first[0].start()
    w_first = loads(0)
    for copy in (*w_first[:3], *first[1:], *w_first[3:]):
        copy.start()

    barrier = pltpu.get_barrier_semaphore()
    for dev in (dev_r, dev_l, partner):
        pl.semaphore_signal(barrier, inc=1, device_id={"sp": dev}, device_id_type=MESH)

    for i, ref in enumerate((gain_s, gain_c, gain_m)):
        for j in range(n_layers):
            gains[i, j] = ref[j:j + 1].astype(F32)

    first[0].wait()
    h_own[0, own_rows] = rms_norm(y[...].astype(F32), gains[0, 0])
    pl.semaphore_wait(barrier, 3)

    to_r, to_l = chip < right, chip < left
    b_to_l = to_l | (chip < opp)
    relay_a, relay_b = left < right, right < left
    need_l, need_r, need_o = left < chip, right < chip, opp < chip
    got_rb = need_r | relay_b
    need = (need_l, need_r, need_l, need_r, need_o, need_o)
    got = (need_l, got_rb, need_l, need_r, need_o, need_o)
    sent = (to_r, b_to_l, to_r, to_l)

    def row_copies(layer):
        own_a = h_own.at[layer, pl.ds(pl.multiple_of(core * rows, half), half)]
        own_b = h_own.at[layer, pl.ds(pl.multiple_of(core * rows + half, half), half)]
        slot = [h_rem.at[layer, i, core] for i in range(6)]
        srcs = (own_a, own_b, own_b, own_a, slot[0], slot[1])
        ring = [remote(srcs[i], slot[i], ici_s.at[layer, i], ici_r.at[layer, i], dev_l if i % 2 else dev_r)
                for i in (0, 1)]
        ring += [remote(srcs[2], slot[2], ici_s.at[layer, 2], ici_r.at[layer, 2], dev_r),
                 remote(srcs[3], slot[3], ici_s.at[layer, 3], ici_r.at[layer, 3], dev_l),
                 remote(srcs[4], slot[4], ici_s.at[layer, 4], ici_r.at[layer, 4], dev_r),
                 remote(srcs[5], slot[5], ici_s.at[layer, 5], ici_r.at[layer, 5], dev_l)]
        fwd = [remote(slot[i], slot[i], d2d_s.at[layer, i], d2d_r.at[layer, i], partner) for i in range(6)]
        own = remote(h_own.at[layer, own_rows], h_own.at[layer, own_rows], own_sem.at[layer, 0], own_sem.at[layer, 1],
                     partner)
        return ring, fwd, own

    def when_start(cond, copy):
        @pl.when(cond)
        def _():
            copy.start()

    def when_sent(cond, copy):
        @pl.when(cond)
        def _():
            copy.wait_send()

    def when_recv(cond, copy):
        @pl.when(cond)
        def _():
            copy.wait_recv()

    has_m = 2 * chip < used
    has_l, has_r, has_o = 2 * left < used, 2 * right < used, 2 * opp < used

    def blk(who, core_of):
        return jnp.minimum(2 * who + core_of, used - 1)

    b_me, b_l, b_r, b_o = blk(chip, core), blk(left, core), blk(right, core), blk(opp, core)
    top, low = pl.ds(0, mh), pl.ds(mh, mh)
    m_own = [
        remote(mkv, mall.at[b_me], mi_s.at[0], mi_r.at[0], dev_r),
        remote(mkv, mall.at[b_me], mi_s.at[1], mi_r.at[1], dev_l),
        remote(mkv, mall.at[b_me], md_s.at[0], md_r.at[0], partner),
    ]
    m_relay = [
        remote(mall.at[b_l, :, top], mall.at[b_l, :, top], mo_s.at[0], mo_r.at[0], dev_r),
        remote(mall.at[b_r, :, low], mall.at[b_r, :, low], mo_s.at[1], mo_r.at[1], dev_l),
    ]
    m_fwd = [
        remote(mall.at[b_l], mall.at[b_l], md_s.at[1], md_r.at[1], partner),
        remote(mall.at[b_r], mall.at[b_r], md_s.at[2], md_r.at[2], partner),
        remote(mall.at[b_o, :, top], mall.at[b_o, :, top], md_s.at[3], md_r.at[3], partner),
        remote(mall.at[b_o, :, low], mall.at[b_o, :, low], md_s.at[4], md_r.at[4], partner),
    ]
    m_has = (has_l, has_r, has_o, has_o)

    def start_rows(layer):
        ring, _, own = row_copies(layer)
        own.start()
        when_start(sent[0], ring[0])
        when_start(sent[1], ring[1])

    start_rows(0)
    for copy in first[1:]:
        copy.wait()

    @pl.when(has_m)
    def _():
        for i in range(n_layers):
            mkv[i, :, :kv_dim] = dot(mem[...], ck[i]).astype(BF16)
            mkv[i, :, kv_dim:] = dot(mem[...], cv[i]).astype(BF16)
        mall[b_me] = mkv[...]

    qm[...] = jnp.zeros_like(qm)
    ones_row = (lax.broadcasted_iota(jnp.int32, (PAIR - HEAD_DIM, 2 * TILE), 0) == 0).astype(F32).astype(BF16)
    for n in range(qc.shape[0]):
        qc[n, HEAD_DIM:] = ones_row

    def reset():
        m_ref[...] = jnp.full_like(m_ref, MASK_VALUE)
        l_ref[...] = jnp.zeros_like(l_ref)
        acc[...] = jnp.zeros_like(acc)

    def scores_of(k_val, q_val, n, buf, mc, size=CHUNK, mask=None):
        col_scores(k_val, q_val, buf, size, mask, m_ref[n], mc)

    def softmax_of(vt_top, vt_low, n, buf, mc, size=CHUNK):
        e, alpha = col_softmax(buf, size, mc, n, m_ref, l_ref)
        acc[n, :HEAD_DIM] = acc[n, :HEAD_DIM] * alpha[:, :TILE] + dot(vt_top, e[:, :TILE])
        acc[n, HEAD_DIM:] = acc[n, HEAD_DIM:] * alpha[:, TILE:] + dot(vt_low, e[:, TILE:])

    def pipelined(count, unroll, item, scores, softmax):
        bufs, mcs = (b0, b1), (mc0, mc1)

        def at(i):
            return item(jnp.minimum(i, count - 1))

        scores(at(0), b0, mc0)

        def body(i, carry):
            for u in range(unroll):
                scores(at(unroll * i + u + 1), bufs[(u + 1) % 2], mcs[(u + 1) % 2])
                softmax(at(unroll * i + u), bufs[u % 2], mcs[u % 2])
            return carry

        lax.fori_loop(0, count // unroll, body, 0)

    def finish(n):
        inv = 1.0 / l_ref[n]
        val = jnp.concatenate([acc[n, :HEAD_DIM] * inv[:, :TILE], acc[n, HEAD_DIM:] * inv[:, TILE:]], axis=0)
        return val.astype(BF16).T

    def project_kv(pieces):
        size = CHUNK // len(pieces)
        for i, piece in enumerate(pieces):
            span = slice(i * size, (i + 1) * size)
            k_val = dot(piece, wk[...]).astype(BF16)
            v_val = dot(wvt[...], piece, NT).astype(BF16)
            for p in range(pairs):
                k_s[p, span] = k_val[:, p * PAIR:(p + 1) * PAIR]
                vt_s[p, :, span] = v_val[p * PAIR:(p + 1) * PAIR]

    def self_scores(pn, buf, mc, size=CHUNK, mask=None):
        p, n = pn
        scores_of(k_s[p, :size], qm[n], n, buf, mc, size, mask)

    def self_softmax(pn, buf, mc, size=CHUNK):
        p, n = pn
        softmax_of(vt_s[p, :HEAD_DIM, :size], vt_s[p, HEAD_DIM:, :size], n, buf, mc, size)

    def attend(first_tile, n_tiles, unroll):
        def item(i):
            p = i // n_tiles
            return p, p * tiles + first_tile + lax.rem(i, n_tiles)

        pipelined(pairs * n_tiles, unroll, item, self_scores, self_softmax)

    def layer_body(layer, carry):
        ring, fwd, own = row_copies(layer)
        weights = loads(layer)
        reset()
        for copy in weights[:3]:
            copy.wait()
        wqt[...] = wq[...].T
        wvt[...] = wv[...].T

        def own_block(i, inner):
            block = jnp.where(i == 0, core, other)

            @pl.when(i == 1)
            def _():
                own.wait_recv()

            h_blk = h_own[layer, pl.ds(pl.multiple_of(block * rows, rows), rows)]
            q_val = (dot(wqt[...], h_blk, NT).astype(BF16) * ATT_SCALE).astype(BF16)
            for p in range(pairs):
                for t in range(row_tiles):
                    n = p * tiles + block * row_tiles + t
                    span = slice(t * TILE, (t + 1) * TILE)
                    qm[n, :HEAD_DIM, :TILE] = q_val[p * PAIR:p * PAIR + HEAD_DIM, span]
                    qm[n, HEAD_DIM:, TILE:] = q_val[p * PAIR + HEAD_DIM:(p + 1) * PAIR, span]
            return inner

        lax.fori_loop(0, 2, own_block, 0)

        def own_keys(block, inner):
            project_kv([h_own[layer, pl.ds(pl.multiple_of(block * rows, rows), rows)]])
            key = lax.broadcasted_iota(jnp.int32, (CHUNK, 2 * TILE), 0)
            query = lax.broadcasted_iota(jnp.int32, (CHUNK, 2 * TILE), 1) % TILE

            def diagonal(p, deep):
                n = p * tiles + block * row_tiles
                self_scores((p, n), b0, mc0, TILE, key[:TILE] <= query[:TILE])
                self_scores((p, n + 1), b1, mc1, CHUNK, key <= query + TILE)
                self_softmax((p, n), b0, mc0, TILE)
                self_softmax((p, n + 1), b1, mc1, CHUNK)
                return deep

            lax.fori_loop(0, pairs, diagonal, 0)

            @pl.when(block == 0)
            def _():
                attend(tiles // 2, tiles // 2, 2)
                when_start(sent[2], ring[2])
                when_start(sent[3], ring[3])

            return inner

        lax.fori_loop(0, 2, own_keys, 0)

        def take(i):
            when_recv(got[i], ring[i])
            if i == 0:
                when_start(relay_a, ring[4])
            if i == 1:
                when_start(relay_b, ring[5])
            when_start(need[i], fwd[i])

        def attend_two(stage, inner):
            @pl.when(stage == 0)
            def _():
                take(0)
                take(1)

                @pl.when(layer == 0)
                def _():
                    when_start(has_m, m_own[2])
                    when_start(has_m, m_own[0])
                    when_start(has_m, m_own[1])


            @pl.when(stage == 1)
            def _():
                take(2)
                take(3)

            @pl.when(stage == 2)
            def _():
                take(4)
                take(5)

            any_need = jnp.where(stage == 2, opp, left) < chip
            both = jnp.where(stage == 2, opp, right) < chip

            def one(i, deep):
                @pl.when(i == 1)
                def _():
                    for j in range(3):
                        @pl.when(stage == j)
                        def _(j=j):
                            when_recv(need[2 * j], fwd[2 * j])
                            when_recv(need[2 * j + 1], fwd[2 * j + 1])

                @pl.when((stage == 2) & (i == 1) & (layer == 0))
                def _():
                    when_recv(has_l, m_own[0])
                    when_start(has_l, m_relay[0])
                    when_start(has_l, m_fwd[0])
                    when_recv(has_r, m_own[1])
                    when_start(has_r, m_relay[1])
                    when_start(has_r, m_fwd[1])

                @pl.when(any_need & ((i == 1) | both))
                def _():
                    from_a = jnp.where((i == 1) & both, other, core)
                    from_b = jnp.where(i == 1, other, core)
                    slot_b = jnp.where(both, 2 * stage + 1, 2 * stage)
                    project_kv([h_rem[layer, 2 * stage, from_a], h_rem[layer, slot_b, from_b]])
                    attend(0, tiles, 6)

                return deep

            return lax.fori_loop(0, 2, one, inner)

        lax.fori_loop(0, 3, attend_two, 0)

        for block, dst in ((other, o_stage), (core, None)):
            for p in range(pairs):
                for t in range(row_tiles):
                    val = finish(p * tiles + block * row_tiles + t)
                    span = slice(t * TILE, (t + 1) * TILE)
                    if dst is not None:
                        dst[layer, span, p * PAIR:(p + 1) * PAIR] = val
                    else:
                        o_full[layer, core, span, p * PAIR:(p + 1) * PAIR] = val
        o_send = remote(o_stage.at[layer], o_full.at[layer, core], o_sem.at[layer, 0], o_sem.at[layer, 1], partner)
        o_send.start()

        @pl.when(layer + 1 < n_layers)
        def _():
            for copy in loads(layer + 1)[:3]:
                copy.start()

        @pl.when(layer == 0)
        def _():
            when_recv(has_o, m_relay[0])
            when_start(has_o, m_fwd[2])
            when_recv(has_o, m_relay[1])
            when_start(has_o, m_fwd[3])
            when_recv(has_m, m_own[2])
            for cond, copy in zip(m_has, m_fwd):
                when_recv(cond, copy)
            for copy in m_own:
                when_sent(has_m, copy)
            when_sent(has_l, m_relay[0])
            when_sent(has_r, m_relay[1])
            for cond, copy in zip(m_has, m_fwd):
                when_sent(cond, copy)

        reset()
        mem_len = len_ref[0]
        for b in range(used):
            span = slice(b * mrows, (b + 1) * mrows)
            vt = mall[b, layer, :, kv_dim:].T
            pos = lax.broadcasted_iota(jnp.int32, (mrows, HEAD_DIM), 0) + b * mrows
            lane = lax.broadcasted_iota(jnp.int32, (mrows, HEAD_DIM), 1)
            bias = jnp.where((pos >= mem_len) & (lane == 0), MASK_VALUE, 0.0).astype(BF16)
            for g in range(n_kv):
                k_c[g, span, :HEAD_DIM] = mall[b, layer, :, g * HEAD_DIM:(g + 1) * HEAD_DIM]
                k_c[g, span, HEAD_DIM:] = bias
                vt_c[g, :, span] = vt[g * HEAD_DIM:(g + 1) * HEAD_DIM]

        o_send.wait_recv()
        weights[3].wait()
        upd = dot(o_full[layer, 0], wo[:width]) + dot(o_full[layer, 1], wo[width:])
        y1 = (y[...].astype(F32) + upd).astype(BF16)
        y[...] = y1
        h = rms_norm(y1.astype(F32), gains[1, layer])
        weights[4].wait()
        q_val = (dot(h, cq[...]).astype(BF16) * ATT_SCALE).astype(BF16)
        for p in range(all_pairs):
            qt = q_val[:, p * PAIR:(p + 1) * PAIR].T
            for t in range(row_tiles):
                span = slice(t * TILE, (t + 1) * TILE)
                qc[p * row_tiles + t, :HEAD_DIM, :TILE] = qt[:HEAD_DIM, span]
                qc[p * row_tiles + t, :HEAD_DIM, TILE:] = qt[HEAD_DIM:, span]

        def chunk(c, inner):
            off = pl.multiple_of(c * CHUNK, CHUNK)

            def item(n):
                return n // (row_tiles * group), n

            def scores(gn, buf, mc):
                g, n = gn
                scores_of(k_c[g, pl.ds(off, CHUNK)], qc[n], n, buf, mc)

            def softmax(gn, buf, mc):
                g, n = gn
                vt = vt_c[g, :, pl.ds(off, CHUNK)]
                softmax_of(vt, vt, n, buf, mc)

            pipelined(all_pairs * row_tiles, 6, item, scores, softmax)
            return inner

        lax.fori_loop(0, used * mrows // CHUNK, chunk, 0)
        for p in range(all_pairs):
            for t in range(row_tiles):
                o_stage_c[t * TILE:(t + 1) * TILE, p * PAIR:(p + 1) * PAIR] = finish(p * row_tiles + t)
        weights[5].wait()
        y2 = (y[...].astype(F32) + dot(o_stage_c[...], co[...])).astype(BF16)
        y[...] = y2
        h = rms_norm(y2.astype(F32), gains[2, layer])
        weights[6].wait()
        weights[7].wait()
        for c in range(0, ff, CHUNK):
            gate = dot(h, wg[:, c:c + CHUNK])
            act[:, c:c + CHUNK] = (jax.nn.silu(gate) * dot(h, wu[:, c:c + CHUNK])).astype(BF16)
        weights[8].wait()
        y3 = (y[...].astype(F32) + dot(act[...], wd[...])).astype(BF16)
        y[...] = y3

        @pl.when(layer + 1 < n_layers)
        def _():
            h_own[layer + 1, own_rows] = rms_norm(y3.astype(F32), gains[0, layer + 1])
            for copy in loads(layer + 1)[3:]:
                copy.start()
            start_rows(layer + 1)

        own.wait_send()
        o_send.wait_send()
        for cond, copy in zip((*sent, relay_a, relay_b), ring):
            when_sent(cond, copy)
        for cond, copy in zip(need, fwd):
            when_sent(cond, copy)
        return carry

    o_stage_c = act.at[:, :d_model]
    lax.fori_loop(0, n_layers, layer_body, 0)
    out_ref[...] = y[...]


def layers_call(n_sp, mem_len, hidden, memory, gain_self, gain_cross, gain_mlp, self_q, self_k, self_v, self_o, cross_q,
                cross_k, cross_v, cross_o, gate, up, down):
    rows, d_model = hidden.shape
    layers = gain_self.shape[0]
    width = d_model // 2
    ff = gate.shape[2]
    mrows, mcols = memory.shape[0], 2 * cross_k.shape[2]
    used = min(n_sp, pl.cdiv(MAX_MEM_LEN, mrows))
    n_kv = cross_k.shape[2] // HEAD_DIM
    pairs, tiles = width // PAIR, 2 * rows // TILE
    combos = pairs * tiles
    dma = pltpu.SemaphoreType.DMA
    return pl.pallas_call(
        functools.partial(layer_kernel, n_sp, layers),
        out_shape=jax.ShapeDtypeStruct((rows, d_model), BF16),
        in_specs=[SMEM, ANY, ANY, VMEM, VMEM, VMEM] + [ANY] * 11,
        out_specs=VMEM,
        scratch_shapes=[
            pltpu.VMEM((rows, d_model), BF16),
            pltpu.VMEM((layers, 2 * rows, d_model), BF16),
            pltpu.VMEM((layers, 6, 2, rows // 2, d_model), BF16),
            pltpu.VMEM((mrows, d_model), BF16),
            *[pltpu.VMEM(cross_k.shape, BF16)] * 2,
            pltpu.VMEM((layers, mrows, mcols), BF16),
            pltpu.VMEM((used, layers, mrows, mcols), BF16),
            *[pltpu.VMEM((d_model, width), BF16)] * 3,
            *[pltpu.VMEM((width, d_model), BF16)] * 2,
            *[pltpu.VMEM((d_model, d_model), BF16)] * 3,
            *[pltpu.VMEM((d_model, ff), BF16)] * 2,
            pltpu.VMEM((ff, d_model), BF16),
            *[pltpu.VMEM((combos, PAIR, 2 * TILE), BF16)] * 2,
            pltpu.VMEM((pairs, CHUNK, PAIR), BF16),
            pltpu.VMEM((pairs, PAIR, CHUNK), BF16),
            pltpu.VMEM((n_kv, used * mrows, PAIR), BF16),
            pltpu.VMEM((n_kv, HEAD_DIM, used * mrows), BF16),
            *[pltpu.VMEM((combos, 1, 2 * TILE), F32)] * 2,
            pltpu.VMEM((combos, PAIR, TILE), F32),
            *[pltpu.VMEM((CHUNK, 2 * TILE), F32)] * 2,
            *[pltpu.VMEM((1, 2 * TILE), F32)] * 2,
            pltpu.VMEM((layers, rows, width), BF16),
            pltpu.VMEM((layers, 2, rows, width), BF16),
            pltpu.VMEM((rows, ff), BF16),
            pltpu.VMEM((3, layers, 1, d_model), F32),
            dma((13,)), dma((layers, 2)), *[dma((layers, 6))] * 4,
            *[dma((2,))] * 4, *[dma((5,))] * 2, dma((layers, 2)),
        ],
        compiler_params=pltpu.CompilerParams(collective_id=0, has_side_effects=True, vmem_limit_bytes=VMEM_LIMIT),
        name="layers",
    )(mem_len, hidden, memory, gain_self, gain_cross, gain_mlp, self_q, self_k, self_v, self_o, cross_q, cross_k, cross_v,
      cross_o, gate, up, down)


def solution(mesh):
    n_sp = mesh.shape["sp"]
    row_spec = P(("dp", "sp"), None)

    def device_fn(dec_hidden, memory, mem_len, *weights):
        return layers_call(n_sp, mem_len, dec_hidden, memory, *weights)

    return jax.shard_map(device_fn, mesh=mesh, in_specs=(row_spec, row_spec, P("dp")) + (P(),) * 14,
                         out_specs=row_spec, check_vma=False)
```

```python
import functools

import jax
import jax.numpy as jnp
from jax import lax
from jax.experimental import pallas as pl
from jax.experimental.pallas import tpu as pltpu
from jax.sharding import PartitionSpec as P

HEAD_DIM = 64
NORM_EPS = 1e-6
MASK_VALUE = -1e30
ATT_SCALE = HEAD_DIM ** -0.5
MAX_MEM_LEN = 1536
HANDED = 128
PAIR = 2 * HEAD_DIM
TILE = 256
CHUNK = 512
NN = (((1,), (0,)), ((), ()))
NT = (((1,), (1,)), ((), ()))
F32 = jnp.float32
BF16 = jnp.bfloat16
MESH = pl.DeviceIdType.MESH
VMEM_LIMIT = 60 * 1024 * 1024
ANY = pl.BlockSpec(memory_space=pl.ANY)
VMEM = pl.BlockSpec(memory_space=pltpu.VMEM)
SMEM = pl.BlockSpec(memory_space=pltpu.SMEM)


def rms_norm(val32, gain_row):
    inv_rms = lax.rsqrt(jnp.mean(val32 * val32, axis=-1, keepdims=True) + NORM_EPS)
    return (val32 * inv_rms * gain_row).astype(BF16)


def dot(lhs, rhs, dims=NN):
    return lax.dot_general(lhs, rhs, dims, preferred_element_type=F32)


def col_scores(k_val, q_val, buf, size, mask, n, m_ref, mc):
    width = q_val.shape[1]
    s = dot(k_val, q_val)
    if mask is not None:
        s = jnp.where(mask, s, MASK_VALUE)
    buf[:size, :width] = s
    mc[:, :width] = jnp.maximum(m_ref[n, :, :width], jnp.max(s, axis=0, keepdims=True))


def col_softmax(buf, size, width, mc, n, m_ref, l_ref):
    m_new = mc[:, :width]
    alpha = jnp.exp(m_ref[n, :, :width] - m_new)
    e = jnp.exp(buf[:size, :width] - m_new)
    l_ref[n, :, :width] = l_ref[n, :, :width] * alpha + jnp.sum(e, axis=0, keepdims=True)
    m_ref[n, :, :width] = m_new
    return e.astype(BF16), alpha


def layer_kernel(n_sp, n_layers, len_ref, hid_hbm, mem_hbm, gain_s, gain_c, gain_m, wq_hbm, wk_hbm, wv_hbm, wo_hbm, cq_hbm,
                 ck_hbm, cv_hbm, co_hbm, wg_hbm, wu_hbm, wd_hbm, out_ref,
                 y, h_own, h_rem, mem, ck, cv, mkv, mall, wq, wk, wv, wqt, wvt, wo, cq, co, wg, wu, wd,
                 qm, qc, k_s, vt_s, k_c, vt_c, m_ref, l_ref, acc, b0, b1, mc0, mc1, o_stage, o_full, act, gains,
                 y_give, y_take, o_take, y_back, y_done, o_part,
                 w_sem, own_sem, ici_s, ici_r, d2d_s, d2d_r, mi_s, mi_r, mo_s, mo_r, md_s, md_r, o_sem,
                 give_s, give_r):
    rows, d_model = y.shape
    half = rows // 2
    width = d_model // 2
    pairs = width // PAIR
    tiles = 2 * rows // TILE
    row_tiles = rows // TILE
    all_pairs = d_model // PAIR
    used, _, mrows, mcols = mall.shape
    mh = mrows // 2
    kv_dim = mcols // 2
    n_kv = kv_dim // HEAD_DIM
    group = all_pairs // n_kv
    ff = act.shape[1]
    n_chip = n_sp // 2
    me = lax.axis_index("sp")
    chip, core = me // 2, lax.rem(me, 2)
    other = 1 - core
    right, left = lax.rem(chip + 1, n_chip), lax.rem(chip + n_chip - 1, n_chip)
    opp = lax.rem(chip + 2, n_chip)
    partner = 2 * chip + other
    dev_r, dev_l = 2 * right + core, 2 * left + core
    gives = 2 * chip >= n_chip
    mate = 2 * (n_chip - 1 - chip) + core
    keep = rows - HANDED

    def remote(src, dst, send, recv, dev):
        return pltpu.make_async_remote_copy(
            src_ref=src, dst_ref=dst, send_sem=send, recv_sem=recv, device_id={"sp": dev}, device_id_type=MESH)

    cols = pl.ds(pl.multiple_of(core * width, 128), width)
    own_rows = pl.ds(pl.multiple_of(core * rows, rows), rows)
    other_rows = pl.ds(pl.multiple_of(other * rows, rows), rows)

    def loads(layer):
        specs = [(wq_hbm.at[layer, :, cols], wq), (wk_hbm.at[layer, :, cols], wk), (wv_hbm.at[layer, :, cols], wv),
                 (wo_hbm.at[layer], wo), (cq_hbm.at[layer], cq), (co_hbm.at[layer], co), (wg_hbm.at[layer], wg),
                 (wu_hbm.at[layer], wu), (wd_hbm.at[layer], wd)]
        return [pltpu.make_async_copy(src, dst, w_sem.at[i]) for i, (src, dst) in enumerate(specs)]

    first = [pltpu.make_async_copy(src, dst, w_sem.at[9 + i])
             for i, (src, dst) in enumerate(((hid_hbm, y), (mem_hbm, mem), (ck_hbm, ck), (cv_hbm, cv)))]
    first[0].start()
    w_first = loads(0)
    for copy in (*w_first[:3], *first[1:], *w_first[3:]):
        copy.start()

    barrier = pltpu.get_barrier_semaphore()
    for dev in (dev_r, dev_l, partner):
        pl.semaphore_signal(barrier, inc=1, device_id={"sp": dev}, device_id_type=MESH)

    for i, ref in enumerate((gain_s, gain_c, gain_m)):
        for j in range(n_layers):
            gains[i, j] = ref[j:j + 1].astype(F32)

    first[0].wait()
    h_own[0, own_rows] = rms_norm(y[...].astype(F32), gains[0, 0])
    pl.semaphore_wait(barrier, 3)

    to_r, to_l = chip < right, chip < left
    b_to_l = to_l | (chip < opp)
    relay_a, relay_b = left < right, right < left
    need_l, need_r, need_o = left < chip, right < chip, opp < chip
    got_rb = need_r | relay_b
    need = (need_l, need_r, need_l, need_r, need_o, need_o)
    got = (need_l, got_rb, need_l, need_r, need_o, need_o)
    sent = (to_r, b_to_l, to_r, to_l)

    def row_copies(layer):
        own_a = h_own.at[layer, pl.ds(pl.multiple_of(core * rows, half), half)]
        own_b = h_own.at[layer, pl.ds(pl.multiple_of(core * rows + half, half), half)]
        slot = [h_rem.at[layer, i, core] for i in range(6)]
        srcs = (own_a, own_b, own_b, own_a, slot[0], slot[1])
        ring = [remote(srcs[i], slot[i], ici_s.at[layer, i], ici_r.at[layer, i], dev_l if i % 2 else dev_r)
                for i in (0, 1)]
        ring += [remote(srcs[2], slot[2], ici_s.at[layer, 2], ici_r.at[layer, 2], dev_r),
                 remote(srcs[3], slot[3], ici_s.at[layer, 3], ici_r.at[layer, 3], dev_l),
                 remote(srcs[4], slot[4], ici_s.at[layer, 4], ici_r.at[layer, 4], dev_r),
                 remote(srcs[5], slot[5], ici_s.at[layer, 5], ici_r.at[layer, 5], dev_l)]
        fwd = [remote(slot[i], slot[i], d2d_s.at[layer, i], d2d_r.at[layer, i], partner) for i in range(6)]
        own = remote(h_own.at[layer, own_rows], h_own.at[layer, own_rows], own_sem.at[layer, 0], own_sem.at[layer, 1],
                     partner)
        return ring, fwd, own

    def give_copies(layer):
        return [remote(y_give.at[layer], y_take.at[layer], give_s.at[layer, 0], give_r.at[layer, 0], mate),
                remote(o_full.at[layer, :, pl.ds(keep, HANDED)], o_take.at[layer], give_s.at[layer, 1],
                       give_r.at[layer, 1], mate),
                remote(y_back.at[layer], y_done.at[layer], give_s.at[layer, 2], give_r.at[layer, 2], mate)]

    def give_y(layer):
        @pl.when(gives)
        def _():
            give_copies(layer)[0].start()

    def when_start(cond, copy):
        @pl.when(cond)
        def _():
            copy.start()

    def when_sent(cond, copy):
        @pl.when(cond)
        def _():
            copy.wait_send()

    def when_recv(cond, copy):
        @pl.when(cond)
        def _():
            copy.wait_recv()

    has_m = 2 * chip < used
    has_l, has_r, has_o = 2 * left < used, 2 * right < used, 2 * opp < used

    def blk(who, core_of):
        return jnp.minimum(2 * who + core_of, used - 1)

    b_me, b_l, b_r, b_o = blk(chip, core), blk(left, core), blk(right, core), blk(opp, core)
    top, low = pl.ds(0, mh), pl.ds(mh, mh)
    m_own = [
        remote(mkv, mall.at[b_me], mi_s.at[0], mi_r.at[0], dev_r),
        remote(mkv, mall.at[b_me], mi_s.at[1], mi_r.at[1], dev_l),
        remote(mkv, mall.at[b_me], md_s.at[0], md_r.at[0], partner),
    ]
    m_relay = [
        remote(mall.at[b_l, :, top], mall.at[b_l, :, top], mo_s.at[0], mo_r.at[0], dev_r),
        remote(mall.at[b_r, :, low], mall.at[b_r, :, low], mo_s.at[1], mo_r.at[1], dev_l),
    ]
    m_fwd = [
        remote(mall.at[b_l], mall.at[b_l], md_s.at[1], md_r.at[1], partner),
        remote(mall.at[b_r], mall.at[b_r], md_s.at[2], md_r.at[2], partner),
        remote(mall.at[b_o, :, top], mall.at[b_o, :, top], md_s.at[3], md_r.at[3], partner),
        remote(mall.at[b_o, :, low], mall.at[b_o, :, low], md_s.at[4], md_r.at[4], partner),
    ]
    m_has = (has_l, has_r, has_o, has_o)

    def start_rows(layer):
        ring, _, own = row_copies(layer)
        own.start()
        when_start(sent[0], ring[0])
        when_start(sent[1], ring[1])

    y_give[0] = y[keep:]
    start_rows(0)
    give_y(0)
    for copy in first[1:]:
        copy.wait()

    @pl.when(has_m)
    def _():
        for i in range(n_layers):
            mkv[i, :, :kv_dim] = dot(mem[...], ck[i]).astype(BF16)
            mkv[i, :, kv_dim:] = dot(mem[...], cv[i]).astype(BF16)
        mall[b_me] = mkv[...]

    qm[...] = jnp.zeros_like(qm)
    ones_row = (lax.broadcasted_iota(jnp.int32, (PAIR - HEAD_DIM, qc.shape[2]), 0) == 0).astype(F32).astype(BF16)
    for n in range(qc.shape[0]):
        qc[n, HEAD_DIM:] = ones_row

    def reset():
        m_ref[...] = jnp.full_like(m_ref, MASK_VALUE)
        l_ref[...] = jnp.zeros_like(l_ref)
        acc[...] = jnp.zeros_like(acc)

    def pipelined(count, unroll, item, scores, softmax):
        bufs, mcs = (b0, b1), (mc0, mc1)

        def at(i):
            return item(jnp.minimum(i, count - 1))

        scores(at(0), b0, mc0)

        def body(i, carry):
            for u in range(unroll):
                scores(at(unroll * i + u + 1), bufs[(u + 1) % 2], mcs[(u + 1) % 2])
                softmax(at(unroll * i + u), bufs[u % 2], mcs[u % 2])
            return carry

        lax.fori_loop(0, count // unroll, body, 0)

    def finish(n, m):
        val = acc[n, :, :2 * m] * (1.0 / l_ref[n, :, :2 * m])
        return jnp.concatenate([val[:, :m], val[:, m:]], axis=0).astype(BF16).T

    def project_kv(pieces):
        size = CHUNK // len(pieces)
        for i, piece in enumerate(pieces):
            span = slice(i * size, (i + 1) * size)
            k_val = dot(piece, wk[...]).astype(BF16)
            v_val = dot(wvt[...], piece, NT).astype(BF16)
            for p in range(pairs):
                k_s[p, span] = k_val[:, p * PAIR:(p + 1) * PAIR]
                vt_s[p, :, span] = v_val[p * PAIR:(p + 1) * PAIR]

    def self_scores(pn, buf, mc, size=CHUNK, mask=None):
        p, n = pn
        col_scores(k_s[p, :size], qm[n], buf, size, mask, n, m_ref, mc)

    def self_softmax(pn, buf, mc, size=CHUNK):
        p, n = pn
        w = 2 * TILE
        e, alpha = col_softmax(buf, size, w, mc, n, m_ref, l_ref)
        acc[n, :, :TILE] = acc[n, :, :TILE] * alpha[:, :TILE] + dot(vt_s[p, :HEAD_DIM, :size], e[:, :TILE])
        acc[n, :, TILE:w] = acc[n, :, TILE:w] * alpha[:, TILE:] + dot(vt_s[p, HEAD_DIM:, :size], e[:, TILE:])

    def attend(first_tile, n_tiles, unroll):
        def item(i):
            p = i // n_tiles
            return p, p * tiles + first_tile + lax.rem(i, n_tiles)

        pipelined(pairs * n_tiles, unroll, item, self_scores, self_softmax)

    def rest_of_layer(layer, y_rows, o_rows, m):
        w = 2 * m
        m_ref[:all_pairs, :, :w] = jnp.full((all_pairs, 1, w), MASK_VALUE, F32)
        l_ref[:all_pairs, :, :w] = jnp.zeros((all_pairs, 1, w), F32)
        acc[:all_pairs, :, :w] = jnp.zeros((all_pairs, HEAD_DIM, w), F32)
        upd = dot(o_rows[0], wo[:width]) + dot(o_rows[1], wo[width:])
        y1 = (y_rows[...].astype(F32) + upd).astype(BF16)
        y_rows[...] = y1
        h = rms_norm(y1.astype(F32), gains[1, layer])
        q_val = (dot(h, cq[...]).astype(BF16) * ATT_SCALE).astype(BF16)
        for p in range(all_pairs):
            qt = q_val[:, p * PAIR:(p + 1) * PAIR].T
            qc[p, :HEAD_DIM, :m] = qt[:HEAD_DIM]
            qc[p, :HEAD_DIM, m:w] = qt[HEAD_DIM:]

        def chunk(c, inner):
            off = pl.multiple_of(c * CHUNK, CHUNK)

            def item(n):
                return n // group, n

            def scores(gn, buf, mc):
                g, n = gn
                col_scores(k_c[g, pl.ds(off, CHUNK)], qc[n, :, :w], buf, CHUNK, None, n, m_ref, mc)

            def softmax(gn, buf, mc):
                g, n = gn
                e, alpha = col_softmax(buf, CHUNK, w, mc, n, m_ref, l_ref)
                acc[n, :, :w] = acc[n, :, :w] * alpha + dot(vt_c[g, :, pl.ds(off, CHUNK)], e)

            pipelined(all_pairs, all_pairs, item, scores, softmax)
            return inner

        lax.fori_loop(0, used * mrows // CHUNK, chunk, 0)
        o2 = act.at[:m, :d_model]
        for p in range(all_pairs):
            o2[:, p * PAIR:(p + 1) * PAIR] = finish(p, m)
        y2 = (y_rows[...].astype(F32) + dot(o2[...], co[...])).astype(BF16)
        y_rows[...] = y2
        h = rms_norm(y2.astype(F32), gains[2, layer])
        for c in range(0, ff, CHUNK):
            gate = dot(h, wg[:, c:c + CHUNK])
            act[:m, c:c + CHUNK] = (jax.nn.silu(gate) * dot(h, wu[:, c:c + CHUNK])).astype(BF16)
        y_rows[...] = (y_rows[...].astype(F32) + dot(act[:m], wd[...])).astype(BF16)

    def layer_body(layer, carry):
        ring, fwd, own = row_copies(layer)
        weights = loads(layer)
        reset()
        for copy in weights[:3]:
            copy.wait()
        wqt[...] = wq[...].T
        wvt[...] = wv[...].T

        def own_block(i, inner):
            block = jnp.where(i == 0, core, other)

            @pl.when(i == 1)
            def _():
                own.wait_recv()

            h_blk = h_own[layer, pl.ds(pl.multiple_of(block * rows, rows), rows)]
            q_val = (dot(wqt[...], h_blk, NT).astype(BF16) * ATT_SCALE).astype(BF16)
            for p in range(pairs):
                for t in range(row_tiles):
                    n = p * tiles + block * row_tiles + t
                    span = slice(t * TILE, (t + 1) * TILE)
                    qm[n, :HEAD_DIM, :TILE] = q_val[p * PAIR:p * PAIR + HEAD_DIM, span]
                    qm[n, HEAD_DIM:, TILE:] = q_val[p * PAIR + HEAD_DIM:(p + 1) * PAIR, span]
            return inner

        lax.fori_loop(0, 2, own_block, 0)

        def own_keys(block, inner):
            project_kv([h_own[layer, pl.ds(pl.multiple_of(block * rows, rows), rows)]])
            key = lax.broadcasted_iota(jnp.int32, (CHUNK, 2 * TILE), 0)
            query = lax.broadcasted_iota(jnp.int32, (CHUNK, 2 * TILE), 1) % TILE

            def diagonal(p, deep):
                n = p * tiles + block * row_tiles
                self_scores((p, n), b0, mc0, TILE, key[:TILE] <= query[:TILE])
                self_scores((p, n + 1), b1, mc1, CHUNK, key <= query + TILE)
                self_softmax((p, n), b0, mc0, TILE)
                self_softmax((p, n + 1), b1, mc1, CHUNK)
                return deep

            lax.fori_loop(0, pairs, diagonal, 0)

            @pl.when(block == 0)
            def _():
                attend(tiles // 2, tiles // 2, 2)
                when_start(sent[2], ring[2])
                when_start(sent[3], ring[3])

            return inner

        lax.fori_loop(0, 2, own_keys, 0)

        def take(i):
            when_recv(got[i], ring[i])
            if i == 0:
                when_start(relay_a, ring[4])
            if i == 1:
                when_start(relay_b, ring[5])
            when_start(need[i], fwd[i])

        def attend_two(stage, inner):
            @pl.when(stage == 0)
            def _():
                take(0)
                take(1)

                @pl.when(layer == 0)
                def _():
                    when_start(has_m, m_own[2])
                    when_start(has_m, m_own[0])
                    when_start(has_m, m_own[1])


            @pl.when(stage == 1)
            def _():
                take(2)
                take(3)

            @pl.when(stage == 2)
            def _():
                take(4)
                take(5)

            any_need = jnp.where(stage == 2, opp, left) < chip
            both = jnp.where(stage == 2, opp, right) < chip

            def one(i, deep):
                @pl.when(i == 1)
                def _():
                    for j in range(3):
                        @pl.when(stage == j)
                        def _(j=j):
                            when_recv(need[2 * j], fwd[2 * j])
                            when_recv(need[2 * j + 1], fwd[2 * j + 1])

                @pl.when((stage == 2) & (i == 1) & (layer == 0))
                def _():
                    when_recv(has_l, m_own[0])
                    when_start(has_l, m_relay[0])
                    when_start(has_l, m_fwd[0])
                    when_recv(has_r, m_own[1])
                    when_start(has_r, m_relay[1])
                    when_start(has_r, m_fwd[1])

                @pl.when(any_need & ((i == 1) | both))
                def _():
                    from_a = jnp.where((i == 1) & both, other, core)
                    from_b = jnp.where(i == 1, other, core)
                    slot_b = jnp.where(both, 2 * stage + 1, 2 * stage)
                    project_kv([h_rem[layer, 2 * stage, from_a], h_rem[layer, slot_b, from_b]])
                    attend(0, tiles, 6)

                return deep

            return lax.fori_loop(0, 2, one, inner)

        lax.fori_loop(0, 3, attend_two, 0)

        for block, dst in ((other, o_stage), (core, None)):
            for p in range(pairs):
                for t in range(row_tiles):
                    val = finish(p * tiles + block * row_tiles + t, TILE)
                    span = slice(t * TILE, (t + 1) * TILE)
                    if dst is not None:
                        dst[layer, span, p * PAIR:(p + 1) * PAIR] = val
                    else:
                        o_full[layer, core, span, p * PAIR:(p + 1) * PAIR] = val
        o_send = remote(o_stage.at[layer], o_full.at[layer, core], o_sem.at[layer, 0], o_sem.at[layer, 1], partner)
        o_send.start()

        @pl.when(layer + 1 < n_layers)
        def _():
            for copy in loads(layer + 1)[:3]:
                copy.start()

        @pl.when(layer == 0)
        def _():
            when_recv(has_o, m_relay[0])
            when_start(has_o, m_fwd[2])
            when_recv(has_o, m_relay[1])
            when_start(has_o, m_fwd[3])
            when_recv(has_m, m_own[2])
            for cond, copy in zip(m_has, m_fwd):
                when_recv(cond, copy)
            for copy in m_own:
                when_sent(has_m, copy)
            when_sent(has_l, m_relay[0])
            when_sent(has_r, m_relay[1])
            for cond, copy in zip(m_has, m_fwd):
                when_sent(cond, copy)

        mem_len = len_ref[0]
        for b in range(used):
            span = slice(b * mrows, (b + 1) * mrows)
            vt = mall[b, layer, :, kv_dim:].T
            pos = lax.broadcasted_iota(jnp.int32, (mrows, HEAD_DIM), 0) + b * mrows
            lane = lax.broadcasted_iota(jnp.int32, (mrows, HEAD_DIM), 1)
            bias = jnp.where((pos >= mem_len) & (lane == 0), MASK_VALUE, 0.0).astype(BF16)
            for g in range(n_kv):
                k_c[g, span, :HEAD_DIM] = mall[b, layer, :, g * HEAD_DIM:(g + 1) * HEAD_DIM]
                k_c[g, span, HEAD_DIM:] = bias
                vt_c[g, :, span] = vt[g * HEAD_DIM:(g + 1) * HEAD_DIM]

        o_send.wait_recv()
        y_copy, o_copy, back_copy = give_copies(layer)
        when_start(gives, o_copy)
        for copy in weights[3:]:
            copy.wait()
        rest_of_layer(layer, y.at[:keep], o_full.at[layer, :, pl.ds(0, keep)], keep)

        def next_rows(span):
            h_own[layer + 1, pl.ds(core * rows + span.start, span.stop - span.start)] = rms_norm(
                y[span].astype(F32), gains[0, layer + 1])

        @pl.when(layer + 1 < n_layers)
        def _():
            next_rows(slice(0, keep))

        def next_start():
            @pl.when(layer + 1 < n_layers)
            def _():
                next_rows(slice(keep, rows))
                y_give[layer + 1] = y[keep:]
                start_rows(layer + 1)
                give_y(layer + 1)

        def handed(i, inner):
            @pl.when(i == 0)
            def _():
                y_back[layer] = y[keep:]
                o_part[...] = o_full[layer, :, keep:]

            @pl.when(i == 1)
            def _():
                y_copy.wait_recv()
                o_copy.wait_recv()
                y_back[layer] = y_take[layer]
                o_part[...] = o_take[layer]

            rest_of_layer(layer, y_back.at[layer], o_part, HANDED)

            @pl.when(i == 0)
            def _():
                y[keep:] = y_back[layer]
                next_start()

            return inner

        @pl.when(jnp.logical_not(gives))
        def _():
            lax.fori_loop(0, 2, handed, 0)
            back_copy.start()
            back_copy.wait_send()

        @pl.when(gives)
        def _():
            back_copy.wait_recv()
            y[keep:] = y_done[layer]
            next_start()
            y_copy.wait_send()
            o_copy.wait_send()

        @pl.when(layer + 1 < n_layers)
        def _():
            for copy in loads(layer + 1)[3:]:
                copy.start()

        own.wait_send()
        o_send.wait_send()
        for cond, copy in zip((*sent, relay_a, relay_b), ring):
            when_sent(cond, copy)
        for cond, copy in zip(need, fwd):
            when_sent(cond, copy)
        return carry

    lax.fori_loop(0, n_layers, layer_body, 0)
    out_ref[...] = y[...]


def layers_call(n_sp, mem_len, hidden, memory, gain_self, gain_cross, gain_mlp, self_q, self_k, self_v, self_o, cross_q,
                cross_k, cross_v, cross_o, gate, up, down):
    rows, d_model = hidden.shape
    layers = gain_self.shape[0]
    width = d_model // 2
    ff = gate.shape[2]
    mrows, mcols = memory.shape[0], 2 * cross_k.shape[2]
    used = min(n_sp, pl.cdiv(MAX_MEM_LEN, mrows))
    n_kv = cross_k.shape[2] // HEAD_DIM
    pairs, tiles = width // PAIR, 2 * rows // TILE
    combos = pairs * tiles
    wide = max(2 * TILE, 2 * (rows - HANDED))
    dma = pltpu.SemaphoreType.DMA
    return pl.pallas_call(
        functools.partial(layer_kernel, n_sp, layers),
        out_shape=jax.ShapeDtypeStruct((rows, d_model), BF16),
        in_specs=[SMEM, ANY, ANY, VMEM, VMEM, VMEM] + [ANY] * 11,
        out_specs=VMEM,
        scratch_shapes=[
            pltpu.VMEM((rows, d_model), BF16),
            pltpu.VMEM((layers, 2 * rows, d_model), BF16),
            pltpu.VMEM((layers, 6, 2, rows // 2, d_model), BF16),
            pltpu.VMEM((mrows, d_model), BF16),
            *[pltpu.VMEM(cross_k.shape, BF16)] * 2,
            pltpu.VMEM((layers, mrows, mcols), BF16),
            pltpu.VMEM((used, layers, mrows, mcols), BF16),
            *[pltpu.VMEM((d_model, width), BF16)] * 3,
            *[pltpu.VMEM((width, d_model), BF16)] * 2,
            *[pltpu.VMEM((d_model, d_model), BF16)] * 3,
            *[pltpu.VMEM((d_model, ff), BF16)] * 2,
            pltpu.VMEM((ff, d_model), BF16),
            pltpu.VMEM((combos, PAIR, 2 * TILE), BF16),
            pltpu.VMEM((2 * pairs, PAIR, wide), BF16),
            pltpu.VMEM((pairs, CHUNK, PAIR), BF16),
            pltpu.VMEM((pairs, PAIR, CHUNK), BF16),
            pltpu.VMEM((n_kv, used * mrows, PAIR), BF16),
            pltpu.VMEM((n_kv, HEAD_DIM, used * mrows), BF16),
            *[pltpu.VMEM((combos, 1, wide), F32)] * 2,
            pltpu.VMEM((combos, HEAD_DIM, wide), F32),
            *[pltpu.VMEM((CHUNK, wide), F32)] * 2,
            *[pltpu.VMEM((1, wide), F32)] * 2,
            pltpu.VMEM((layers, rows, width), BF16),
            pltpu.VMEM((layers, 2, rows, width), BF16),
            pltpu.VMEM((rows, ff), BF16),
            pltpu.VMEM((3, layers, 1, d_model), F32),
            *[pltpu.VMEM((layers, HANDED, d_model), BF16)] * 2,
            pltpu.VMEM((layers, 2, HANDED, width), BF16),
            *[pltpu.VMEM((layers, HANDED, d_model), BF16)] * 2,
            pltpu.VMEM((2, HANDED, width), BF16),
            dma((13,)), dma((layers, 2)), *[dma((layers, 6))] * 4,
            *[dma((2,))] * 4, *[dma((5,))] * 2, dma((layers, 2)), *[dma((layers, 3))] * 2,
        ],
        compiler_params=pltpu.CompilerParams(collective_id=0, has_side_effects=True, vmem_limit_bytes=VMEM_LIMIT),
        name="layers",
    )(mem_len, hidden, memory, gain_self, gain_cross, gain_mlp, self_q, self_k, self_v, self_o, cross_q, cross_k, cross_v,
      cross_o, gate, up, down)


def solution(mesh):
    n_sp = mesh.shape["sp"]
    row_spec = P(("dp", "sp"), None)

    def device_fn(dec_hidden, memory, mem_len, *weights):
        return layers_call(n_sp, mem_len, dec_hidden, memory, *weights)

    return jax.shard_map(device_fn, mesh=mesh, in_specs=(row_spec, row_spec, P("dp")) + (P(),) * 14,
                         out_specs=row_spec, check_vma=False)
```

```python
import functools

import jax
import jax.numpy as jnp
from jax import lax
from jax.experimental import pallas as pl
from jax.experimental.pallas import tpu as pltpu
from jax.sharding import PartitionSpec as P

HEAD_DIM = 64
NORM_EPS = 1e-6
MASK_VALUE = -1e30
ATT_SCALE = HEAD_DIM ** -0.5
MAX_MEM_LEN = 1536
HANDED = 128
PAIR = 2 * HEAD_DIM
TILE = 256
CHUNK = 512
NN = (((1,), (0,)), ((), ()))
NT = (((1,), (1,)), ((), ()))
F32 = jnp.float32
BF16 = jnp.bfloat16
MESH = pl.DeviceIdType.MESH
VMEM_LIMIT = 60 * 1024 * 1024
ANY = pl.BlockSpec(memory_space=pl.ANY)
VMEM = pl.BlockSpec(memory_space=pltpu.VMEM)
SMEM = pl.BlockSpec(memory_space=pltpu.SMEM)


def rms_norm(val32, gain_row):
    inv_rms = lax.rsqrt(jnp.mean(val32 * val32, axis=-1, keepdims=True) + NORM_EPS)
    return (val32 * inv_rms * gain_row).astype(BF16)


def dot(lhs, rhs, dims=NN):
    return lax.dot_general(lhs, rhs, dims, preferred_element_type=F32)


def col_scores(k_val, q_val, buf, size, mask, n, m_ref, mc):
    width = q_val.shape[1]
    s = dot(k_val, q_val)
    if mask is not None:
        s = jnp.where(mask, s, MASK_VALUE)
    buf[:size, :width] = s
    mc[:, :width] = jnp.maximum(m_ref[n, :, :width], jnp.max(s, axis=0, keepdims=True))


def col_softmax(buf, size, width, mc, n, m_ref, l_ref):
    m_new = mc[:, :width]
    alpha = jnp.exp(m_ref[n, :, :width] - m_new)
    e = jnp.exp(buf[:size, :width] - m_new)
    l_ref[n, :, :width] = l_ref[n, :, :width] * alpha + jnp.sum(e, axis=0, keepdims=True)
    m_ref[n, :, :width] = m_new
    return e.astype(BF16), alpha


def layer_kernel(n_sp, n_layers, len_ref, hid_hbm, mem_hbm, gain_s, gain_c, gain_m, wq_hbm, wk_hbm, wv_hbm, wo_hbm, cq_hbm,
                 ck_hbm, cv_hbm, co_hbm, wg_hbm, wu_hbm, wd_hbm, out_ref,
                 y, h_own, h_rem, mem, ck, cv, mkv, mall, wq, wk, wv, wqt, wvt, wo, cq, co, wg, wu, wd,
                 qm, qc, k_s, vt_s, k_c, vt_c, m_ref, l_ref, acc, b0, b1, mc0, mc1, o_stage, o_full, act, gains,
                 y_give, y_take, o_take, y_back, y_done, o_part,
                 w_sem, own_sem, ici_s, ici_r, d2d_s, d2d_r, mi_s, mi_r, mo_s, mo_r, md_s, md_r, o_sem,
                 give_s, give_r):
    rows, d_model = y.shape
    half = rows // 2
    width = d_model // 2
    pairs = width // PAIR
    tiles = 2 * rows // TILE
    row_tiles = rows // TILE
    all_pairs = d_model // PAIR
    used, _, mrows, mcols = mall.shape
    mh = mrows // 2
    kv_dim = mcols // 2
    n_kv = kv_dim // HEAD_DIM
    group = all_pairs // n_kv
    ff = act.shape[1]
    n_chip = n_sp // 2
    me = lax.axis_index("sp")
    chip, core = me // 2, lax.rem(me, 2)
    other = 1 - core
    right, left = lax.rem(chip + 1, n_chip), lax.rem(chip + n_chip - 1, n_chip)
    opp = lax.rem(chip + 2, n_chip)
    partner = 2 * chip + other
    dev_r, dev_l = 2 * right + core, 2 * left + core
    last = n_chip - 1
    gives, takes = chip == last, chip == 0
    mate = 2 * (n_chip - 1 - chip) + core
    keep = rows - HANDED
    wide = 2 * keep

    def remote(src, dst, send, recv, dev):
        return pltpu.make_async_remote_copy(
            src_ref=src, dst_ref=dst, send_sem=send, recv_sem=recv, device_id={"sp": dev}, device_id_type=MESH)

    cols = pl.ds(pl.multiple_of(core * width, 128), width)
    own_rows = pl.ds(pl.multiple_of(core * rows, rows), rows)
    other_rows = pl.ds(pl.multiple_of(other * rows, rows), rows)

    def loads(layer):
        specs = [(wq_hbm.at[layer, :, cols], wq), (wk_hbm.at[layer, :, cols], wk), (wv_hbm.at[layer, :, cols], wv),
                 (wo_hbm.at[layer], wo), (cq_hbm.at[layer], cq), (co_hbm.at[layer], co), (wg_hbm.at[layer], wg),
                 (wu_hbm.at[layer], wu), (wd_hbm.at[layer], wd)]
        return [pltpu.make_async_copy(src, dst, w_sem.at[i]) for i, (src, dst) in enumerate(specs)]

    first = [pltpu.make_async_copy(src, dst, w_sem.at[9 + i])
             for i, (src, dst) in enumerate(((hid_hbm, y), (mem_hbm, mem), (ck_hbm, ck), (cv_hbm, cv)))]
    first[0].start()
    w_first = loads(0)
    for copy in (*w_first[:3], *first[1:], *w_first[3:]):
        copy.start()

    barrier = pltpu.get_barrier_semaphore()
    for dev in (dev_r, dev_l, partner):
        pl.semaphore_signal(barrier, inc=1, device_id={"sp": dev}, device_id_type=MESH)

    for i, ref in enumerate((gain_s, gain_c, gain_m)):
        for j in range(n_layers):
            gains[i, j] = ref[j:j + 1].astype(F32)

    first[0].wait()
    h_own[0, own_rows] = rms_norm(y[...].astype(F32), gains[0, 0])
    pl.semaphore_wait(barrier, 3)

    to_r, to_l = chip < right, chip < left
    b_to_l = to_l | (chip < opp)
    relay_a, relay_b = left < right, right < left
    need_l, need_r, need_o = left < chip, right < chip, opp < chip
    got_rb = need_r | relay_b
    need = (need_l, need_r, need_l, need_r, need_o, need_o)
    got = (need_l, got_rb, need_l, need_r, need_o, need_o)
    sent = (to_r, b_to_l, to_r, to_l)

    def row_copies(layer):
        own_a = h_own.at[layer, pl.ds(pl.multiple_of(core * rows, half), half)]
        own_b = h_own.at[layer, pl.ds(pl.multiple_of(core * rows + half, half), half)]
        slot = [h_rem.at[layer, i, core] for i in range(6)]
        srcs = (own_a, own_b, own_b, own_a, slot[0], slot[1])
        ring = [remote(srcs[i], slot[i], ici_s.at[layer, i], ici_r.at[layer, i], dev_l if i % 2 else dev_r)
                for i in (0, 1)]
        ring += [remote(srcs[2], slot[2], ici_s.at[layer, 2], ici_r.at[layer, 2], dev_r),
                 remote(srcs[3], slot[3], ici_s.at[layer, 3], ici_r.at[layer, 3], dev_l),
                 remote(srcs[4], slot[4], ici_s.at[layer, 4], ici_r.at[layer, 4], dev_r),
                 remote(srcs[5], slot[5], ici_s.at[layer, 5], ici_r.at[layer, 5], dev_l)]
        fwd = [remote(slot[i], slot[i], d2d_s.at[layer, i], d2d_r.at[layer, i], partner) for i in range(6)]
        own = remote(h_own.at[layer, own_rows], h_own.at[layer, own_rows], own_sem.at[layer, 0], own_sem.at[layer, 1],
                     partner)
        return ring, fwd, own

    def give_copies(layer):
        return [remote(y_give.at[layer], y_take.at[layer], give_s.at[layer, 0], give_r.at[layer, 0], mate),
                remote(o_full.at[layer, :, pl.ds(keep, HANDED)], o_take.at[layer], give_s.at[layer, 1],
                       give_r.at[layer, 1], mate),
                remote(y_back.at[layer], y_done.at[layer], give_s.at[layer, 2], give_r.at[layer, 2], mate)]

    def give_y(layer):
        @pl.when(gives)
        def _():
            give_copies(layer)[0].start()

    def when_start(cond, copy):
        @pl.when(cond)
        def _():
            copy.start()

    def when_sent(cond, copy):
        @pl.when(cond)
        def _():
            copy.wait_send()

    def when_recv(cond, copy):
        @pl.when(cond)
        def _():
            copy.wait_recv()

    has_m = 2 * chip < used
    has_l, has_r, has_o = 2 * left < used, 2 * right < used, 2 * opp < used

    def blk(who, core_of):
        return jnp.minimum(2 * who + core_of, used - 1)

    b_me, b_l, b_r, b_o = blk(chip, core), blk(left, core), blk(right, core), blk(opp, core)
    top, low = pl.ds(0, mh), pl.ds(mh, mh)
    m_own = [
        remote(mkv, mall.at[b_me], mi_s.at[0], mi_r.at[0], dev_r),
        remote(mkv, mall.at[b_me], mi_s.at[1], mi_r.at[1], dev_l),
        remote(mkv, mall.at[b_me], md_s.at[0], md_r.at[0], partner),
    ]
    m_relay_l = [
        (remote(mall.at[b_l, :, top], mall.at[b_l, :, top], mo_s.at[0], mo_r.at[0], dev_r), has_l & (chip < last)),
        (remote(mall.at[b_l, :, low], mall.at[b_l, :, low], mo_s.at[1], mo_r.at[1], dev_r),
         has_l & (chip < last) & (right < last)),
    ]
    m_relay_r = [
        (remote(mall.at[b_r, :, top], mall.at[b_r, :, top], mo_s.at[2], mo_r.at[0], dev_l),
         has_r & (chip < last) & (left < last)),
        (remote(mall.at[b_r, :, low], mall.at[b_r, :, low], mo_s.at[3], mo_r.at[1], dev_l), has_r & (chip < last)),
    ]
    m_halves = [
        remote(mall.at[b_o, :, top], mall.at[b_o, :, top], mo_s.at[0], mo_r.at[0], dev_r),
        remote(mall.at[b_o, :, low], mall.at[b_o, :, low], mo_s.at[1], mo_r.at[1], dev_r),
    ]
    m_fwd = [
        remote(mall.at[b_l], mall.at[b_l], md_s.at[1], md_r.at[1], partner),
        remote(mall.at[b_r], mall.at[b_r], md_s.at[2], md_r.at[2], partner),
        remote(mall.at[b_o, :, top], mall.at[b_o, :, top], md_s.at[3], md_r.at[3], partner),
        remote(mall.at[b_o, :, low], mall.at[b_o, :, low], md_s.at[4], md_r.at[4], partner),
    ]
    m_has = (has_l, has_r, has_o, has_o)

    def start_rows(layer):
        ring, _, own = row_copies(layer)
        own.start()
        when_start(sent[0], ring[0])
        when_start(sent[1], ring[1])

    y_give[0] = y[keep:]
    start_rows(0)
    give_y(0)
    for copy in first[1:]:
        copy.wait()

    @pl.when(has_m)
    def _():
        for i in range(n_layers):
            mkv[i, :, :kv_dim] = dot(mem[...], ck[i]).astype(BF16)
            mkv[i, :, kv_dim:] = dot(mem[...], cv[i]).astype(BF16)
        mall[b_me] = mkv[...]
    def from_left():
        when_recv(has_l, m_own[0])
        when_start(has_l, m_fwd[0])
        for copy, cond in m_relay_l:
            when_start(cond, copy)

    def from_right():
        when_recv(has_r, m_own[1])
        when_start(has_r, m_fwd[1])
        for copy, cond in m_relay_r:
            when_start(cond, copy)

    qm[...] = jnp.zeros_like(qm)
    ones_row = (lax.broadcasted_iota(jnp.int32, (PAIR - HEAD_DIM, qc.shape[2]), 0) == 0).astype(F32).astype(BF16)
    for n in range(qc.shape[0]):
        qc[n, HEAD_DIM:] = ones_row
    when_start(has_m, m_own[2])
    when_start(has_m & (left < chip), m_own[1])

    def reset():
        m_ref[...] = jnp.full_like(m_ref, MASK_VALUE)
        l_ref[...] = jnp.zeros_like(l_ref)
        acc[...] = jnp.zeros_like(acc)

    def pipelined(count, unroll, item, scores, softmax):
        bufs, mcs = (b0, b1), (mc0, mc1)

        def at(i):
            return item(jnp.minimum(i, count - 1))

        scores(at(0), b0, mc0)

        def body(i, carry):
            for u in range(unroll):
                scores(at(unroll * i + u + 1), bufs[(u + 1) % 2], mcs[(u + 1) % 2])
                softmax(at(unroll * i + u), bufs[u % 2], mcs[u % 2])
            return carry

        lax.fori_loop(0, count // unroll, body, 0)

    def finish(n, m, first=0):
        span = slice(first, first + 2 * m)
        val = acc[n, :, span] * (1.0 / l_ref[n, :, span])
        return jnp.concatenate([val[:, :m], val[:, m:]], axis=0).astype(BF16).T

    def project_kv(pieces):
        size = CHUNK // len(pieces)
        for i, piece in enumerate(pieces):
            span = slice(i * size, (i + 1) * size)
            k_val = dot(piece, wk[...]).astype(BF16)
            v_val = dot(wvt[...], piece, NT).astype(BF16)
            for p in range(pairs):
                k_s[p, span] = k_val[:, p * PAIR:(p + 1) * PAIR]
                vt_s[p, :, span] = v_val[p * PAIR:(p + 1) * PAIR]

    def self_scores(pn, buf, mc, size=CHUNK, mask=None):
        p, n = pn
        col_scores(k_s[p, :size], qm[n], buf, size, mask, n, m_ref, mc)

    def self_softmax(pn, buf, mc, size=CHUNK):
        p, n = pn
        w = 2 * TILE
        e, alpha = col_softmax(buf, size, w, mc, n, m_ref, l_ref)
        acc[n, :, :TILE] = acc[n, :, :TILE] * alpha[:, :TILE] + dot(vt_s[p, :HEAD_DIM, :size], e[:, :TILE])
        acc[n, :, TILE:w] = acc[n, :, TILE:w] * alpha[:, TILE:] + dot(vt_s[p, HEAD_DIM:, :size], e[:, TILE:])

    def attend(first_tile, n_tiles, unroll):
        def item(i):
            p = i // n_tiles
            return p, p * tiles + first_tile + lax.rem(i, n_tiles)

        pipelined(pairs * n_tiles, unroll, item, self_scores, self_softmax)

    def rest_of_layer(layer, y_rows, o_rows, m):
        per = wide // (2 * m)
        w = 2 * m * per
        sets = all_pairs // per
        per_group = group // per
        m_ref[:sets, :, :w] = jnp.full((sets, 1, w), MASK_VALUE, F32)
        l_ref[:sets, :, :w] = jnp.zeros((sets, 1, w), F32)
        acc[:sets, :, :w] = jnp.zeros((sets, HEAD_DIM, w), F32)
        upd = dot(o_rows[0], wo[:width]) + dot(o_rows[1], wo[width:])
        y1 = (y_rows[...].astype(F32) + upd).astype(BF16)
        y_rows[...] = y1
        h = rms_norm(y1.astype(F32), gains[1, layer])
        q_val = (dot(h, cq[...]).astype(BF16) * ATT_SCALE).astype(BF16)
        for p in range(all_pairs):
            qt = q_val[:, p * PAIR:(p + 1) * PAIR].T
            n, at = p // per, (p % per) * 2 * m
            qc[n, :HEAD_DIM, at:at + m] = qt[:HEAD_DIM]
            qc[n, :HEAD_DIM, at + m:at + 2 * m] = qt[HEAD_DIM:]

        def item(i):
            c, n = i // sets, lax.rem(i, sets)
            return pl.ds(pl.multiple_of(c * CHUNK, CHUNK), CHUNK), n // per_group, n

        def scores(cgn, buf, mc):
            keys, g, n = cgn
            col_scores(k_c[g, keys], qc[n, :, :w], buf, CHUNK, None, n, m_ref, mc)

        def softmax(cgn, buf, mc):
            keys, g, n = cgn
            e, alpha = col_softmax(buf, CHUNK, w, mc, n, m_ref, l_ref)
            acc[n, :, :w] = acc[n, :, :w] * alpha + dot(vt_c[g, :, keys], e)

        pipelined(sets * (used * mrows // CHUNK), 6, item, scores, softmax)
        o2 = act.at[:m, :d_model]
        for p in range(all_pairs):
            o2[:, p * PAIR:(p + 1) * PAIR] = finish(p // per, m, (p % per) * 2 * m)
        y2 = (y_rows[...].astype(F32) + dot(o2[...], co[...])).astype(BF16)
        y_rows[...] = y2
        h = rms_norm(y2.astype(F32), gains[2, layer])
        for c in range(0, ff, CHUNK):
            gate = dot(h, wg[:, c:c + CHUNK])
            act[:m, c:c + CHUNK] = (jax.nn.silu(gate) * dot(h, wu[:, c:c + CHUNK])).astype(BF16)
        y_rows[...] = (y_rows[...].astype(F32) + dot(act[:m], wd[...])).astype(BF16)

    def layer_body(layer, carry):
        ring, fwd, own = row_copies(layer)
        weights = loads(layer)
        reset()
        for copy in weights[:3]:
            copy.wait()
        wqt[...] = wq[...].T
        wvt[...] = wv[...].T

        def own_block(i, inner):
            block = jnp.where(i == 0, core, other)

            @pl.when(i == 1)
            def _():
                own.wait_recv()

            h_blk = h_own[layer, pl.ds(pl.multiple_of(block * rows, rows), rows)]
            q_val = (dot(wqt[...], h_blk, NT).astype(BF16) * ATT_SCALE).astype(BF16)
            for p in range(pairs):
                for t in range(row_tiles):
                    n = p * tiles + block * row_tiles + t
                    span = slice(t * TILE, (t + 1) * TILE)
                    qm[n, :HEAD_DIM, :TILE] = q_val[p * PAIR:p * PAIR + HEAD_DIM, span]
                    qm[n, HEAD_DIM:, TILE:] = q_val[p * PAIR + HEAD_DIM:(p + 1) * PAIR, span]
            return inner

        lax.fori_loop(0, 2, own_block, 0)

        def own_keys(block, inner):
            project_kv([h_own[layer, pl.ds(pl.multiple_of(block * rows, rows), rows)]])
            key = lax.broadcasted_iota(jnp.int32, (CHUNK, 2 * TILE), 0)
            query = lax.broadcasted_iota(jnp.int32, (CHUNK, 2 * TILE), 1) % TILE

            def diagonal(p, deep):
                n = p * tiles + block * row_tiles
                self_scores((p, n), b0, mc0, TILE, key[:TILE] <= query[:TILE])
                self_scores((p, n + 1), b1, mc1, CHUNK, key <= query + TILE)
                self_softmax((p, n), b0, mc0, TILE)
                self_softmax((p, n + 1), b1, mc1, CHUNK)
                return deep

            lax.fori_loop(0, pairs, diagonal, 0)

            @pl.when(block == 0)
            def _():
                attend(tiles // 2, tiles // 2, 2)
                when_start(sent[2], ring[2])
                when_start(sent[3], ring[3])

            return inner

        lax.fori_loop(0, 2, own_keys, 0)

        def take(i):
            when_recv(got[i], ring[i])
            if i == 0:
                when_start(relay_a, ring[4])
            if i == 1:
                when_start(relay_b, ring[5])
            when_start(need[i], fwd[i])

        def attend_two(stage, inner):
            @pl.when(stage == 0)
            def _():
                take(0)
                take(1)

                @pl.when(layer == 0)
                def _():
                    when_start(has_m, m_own[0])
                    when_start(has_m & (left > chip), m_own[1])

                    @pl.when(chip < last)
                    def _():
                        from_right()


            @pl.when(stage == 1)
            def _():
                take(2)
                take(3)

            @pl.when(stage == 2)
            def _():
                take(4)
                take(5)

            any_need = jnp.where(stage == 2, opp, left) < chip
            both = jnp.where(stage == 2, opp, right) < chip

            def one(i, deep):
                @pl.when(i == 1)
                def _():
                    for j in range(3):
                        @pl.when(stage == j)
                        def _(j=j):
                            when_recv(need[2 * j], fwd[2 * j])
                            when_recv(need[2 * j + 1], fwd[2 * j + 1])

                @pl.when((stage == 2) & (i == 1) & (layer == 0))
                def _():
                    from_left()

                    @pl.when(chip == last)
                    def _():
                        from_right()

                @pl.when(any_need & ((i == 1) | both))
                def _():
                    from_a = jnp.where((i == 1) & both, other, core)
                    from_b = jnp.where(i == 1, other, core)
                    slot_b = jnp.where(both, 2 * stage + 1, 2 * stage)
                    project_kv([h_rem[layer, 2 * stage, from_a], h_rem[layer, slot_b, from_b]])
                    attend(0, tiles, 6)

                return deep

            return lax.fori_loop(0, 2, one, inner)

        lax.fori_loop(0, 3, attend_two, 0)

        for block, dst in ((other, o_stage), (core, None)):
            for p in range(pairs):
                for t in range(row_tiles):
                    val = finish(p * tiles + block * row_tiles + t, TILE)
                    span = slice(t * TILE, (t + 1) * TILE)
                    if dst is not None:
                        dst[layer, span, p * PAIR:(p + 1) * PAIR] = val
                    else:
                        o_full[layer, core, span, p * PAIR:(p + 1) * PAIR] = val
        o_send = remote(o_stage.at[layer], o_full.at[layer, core], o_sem.at[layer, 0], o_sem.at[layer, 1], partner)
        o_send.start()

        @pl.when(layer + 1 < n_layers)
        def _():
            for copy in loads(layer + 1)[:3]:
                copy.start()

        @pl.when(layer == 0)
        def _():
            when_recv(has_o, m_halves[0])
            when_start(has_o, m_fwd[2])
            when_recv(has_o, m_halves[1])
            when_start(has_o, m_fwd[3])
            when_recv(has_m, m_own[2])
            for cond, copy in zip(m_has, m_fwd):
                when_recv(cond, copy)
            for copy in m_own:
                when_sent(has_m, copy)
            for copy, cond in (*m_relay_l, *m_relay_r):
                when_sent(cond, copy)
            for cond, copy in zip(m_has, m_fwd):
                when_sent(cond, copy)

        mem_len = len_ref[0]
        for b in range(used):
            span = slice(b * mrows, (b + 1) * mrows)
            vt = mall[b, layer, :, kv_dim:].T
            pos = lax.broadcasted_iota(jnp.int32, (mrows, HEAD_DIM), 0) + b * mrows
            lane = lax.broadcasted_iota(jnp.int32, (mrows, HEAD_DIM), 1)
            bias = jnp.where((pos >= mem_len) & (lane == 0), MASK_VALUE, 0.0).astype(BF16)
            for g in range(n_kv):
                k_c[g, span, :HEAD_DIM] = mall[b, layer, :, g * HEAD_DIM:(g + 1) * HEAD_DIM]
                k_c[g, span, HEAD_DIM:] = bias
                vt_c[g, :, span] = vt[g * HEAD_DIM:(g + 1) * HEAD_DIM]

        o_send.wait_recv()
        y_copy, o_copy, back_copy = give_copies(layer)
        when_start(gives, o_copy)
        for copy in weights[3:]:
            copy.wait()
        rest_of_layer(layer, y.at[:keep], o_full.at[layer, :, pl.ds(0, keep)], keep)

        def next_rows(span):
            h_own[layer + 1, pl.ds(core * rows + span.start, span.stop - span.start)] = rms_norm(
                y[span].astype(F32), gains[0, layer + 1])

        @pl.when(layer + 1 < n_layers)
        def _():
            next_rows(slice(0, keep))

        def next_start():
            @pl.when(layer + 1 < n_layers)
            def _():
                next_rows(slice(keep, rows))
                y_give[layer + 1] = y[keep:]
                start_rows(layer + 1)
                give_y(layer + 1)

        def handed(i, inner):
            @pl.when(i == 0)
            def _():
                y_back[layer] = y[keep:]
                o_part[...] = o_full[layer, :, keep:]

            @pl.when(i == 1)
            def _():
                y_copy.wait_recv()
                o_copy.wait_recv()
                y_back[layer] = y_take[layer]
                o_part[...] = o_take[layer]

            rest_of_layer(layer, y_back.at[layer], o_part, HANDED)

            @pl.when(i == 0)
            def _():
                y[keep:] = y_back[layer]
                next_start()

            return inner

        @pl.when(jnp.logical_not(gives))
        def _():
            lax.fori_loop(0, jnp.where(takes, 2, 1), handed, 0)

        @pl.when(takes)
        def _():
            back_copy.start()
            back_copy.wait_send()

        @pl.when(gives)
        def _():
            back_copy.wait_recv()
            y[keep:] = y_done[layer]
            next_start()
            y_copy.wait_send()
            o_copy.wait_send()

        @pl.when(layer + 1 < n_layers)
        def _():
            for copy in loads(layer + 1)[3:]:
                copy.start()

        own.wait_send()
        o_send.wait_send()
        for cond, copy in zip((*sent, relay_a, relay_b), ring):
            when_sent(cond, copy)
        for cond, copy in zip(need, fwd):
            when_sent(cond, copy)
        return carry

    lax.fori_loop(0, n_layers, layer_body, 0)
    out_ref[...] = y[...]


def layers_call(n_sp, mem_len, hidden, memory, gain_self, gain_cross, gain_mlp, self_q, self_k, self_v, self_o, cross_q,
                cross_k, cross_v, cross_o, gate, up, down):
    rows, d_model = hidden.shape
    layers = gain_self.shape[0]
    width = d_model // 2
    ff = gate.shape[2]
    mrows, mcols = memory.shape[0], 2 * cross_k.shape[2]
    used = min(n_sp, pl.cdiv(MAX_MEM_LEN, mrows))
    n_kv = cross_k.shape[2] // HEAD_DIM
    pairs, tiles = width // PAIR, 2 * rows // TILE
    combos = pairs * tiles
    wide = 2 * (rows - HANDED)
    dma = pltpu.SemaphoreType.DMA
    return pl.pallas_call(
        functools.partial(layer_kernel, n_sp, layers),
        out_shape=jax.ShapeDtypeStruct((rows, d_model), BF16),
        in_specs=[SMEM, ANY, ANY, VMEM, VMEM, VMEM] + [ANY] * 11,
        out_specs=VMEM,
        scratch_shapes=[
            pltpu.VMEM((rows, d_model), BF16),
            pltpu.VMEM((layers, 2 * rows, d_model), BF16),
            pltpu.VMEM((layers, 6, 2, rows // 2, d_model), BF16),
            pltpu.VMEM((mrows, d_model), BF16),
            *[pltpu.VMEM(cross_k.shape, BF16)] * 2,
            pltpu.VMEM((layers, mrows, mcols), BF16),
            pltpu.VMEM((used, layers, mrows, mcols), BF16),
            *[pltpu.VMEM((d_model, width), BF16)] * 3,
            *[pltpu.VMEM((width, d_model), BF16)] * 2,
            *[pltpu.VMEM((d_model, d_model), BF16)] * 3,
            *[pltpu.VMEM((d_model, ff), BF16)] * 2,
            pltpu.VMEM((ff, d_model), BF16),
            pltpu.VMEM((combos, PAIR, 2 * TILE), BF16),
            pltpu.VMEM((2 * pairs, PAIR, wide), BF16),
            pltpu.VMEM((pairs, CHUNK, PAIR), BF16),
            pltpu.VMEM((pairs, PAIR, CHUNK), BF16),
            pltpu.VMEM((n_kv, used * mrows, PAIR), BF16),
            pltpu.VMEM((n_kv, HEAD_DIM, used * mrows), BF16),
            *[pltpu.VMEM((combos, 1, wide), F32)] * 2,
            pltpu.VMEM((combos, HEAD_DIM, wide), F32),
            *[pltpu.VMEM((CHUNK, wide), F32)] * 2,
            *[pltpu.VMEM((1, wide), F32)] * 2,
            pltpu.VMEM((layers, rows, width), BF16),
            pltpu.VMEM((layers, 2, rows, width), BF16),
            pltpu.VMEM((rows, ff), BF16),
            pltpu.VMEM((3, layers, 1, d_model), F32),
            *[pltpu.VMEM((layers, HANDED, d_model), BF16)] * 2,
            pltpu.VMEM((layers, 2, HANDED, width), BF16),
            *[pltpu.VMEM((layers, HANDED, d_model), BF16)] * 2,
            pltpu.VMEM((2, HANDED, width), BF16),
            dma((13,)), dma((layers, 2)), *[dma((layers, 6))] * 4,
            *[dma((2,))] * 2, dma((4,)), dma((2,)), *[dma((5,))] * 2, dma((layers, 2)), *[dma((layers, 3))] * 2,
        ],
        compiler_params=pltpu.CompilerParams(collective_id=0, has_side_effects=True, vmem_limit_bytes=VMEM_LIMIT),
        name="layers",
    )(mem_len, hidden, memory, gain_self, gain_cross, gain_mlp, self_q, self_k, self_v, self_o, cross_q, cross_k, cross_v,
      cross_o, gate, up, down)


def solution(mesh):
    n_sp = mesh.shape["sp"]
    row_spec = P(("dp", "sp"), None)

    def device_fn(dec_hidden, memory, mem_len, *weights):
        return layers_call(n_sp, mem_len, dec_hidden, memory, *weights)

    return jax.shard_map(device_fn, mesh=mesh, in_specs=(row_spec, row_spec, P("dp")) + (P(),) * 14,
                         out_specs=row_spec, check_vma=False)
```

```python
import functools

import jax
import jax.numpy as jnp
from jax import lax
from jax.experimental import pallas as pl
from jax.experimental.pallas import tpu as pltpu
from jax.sharding import PartitionSpec as P

HEAD_DIM = 64
NORM_EPS = 1e-6
MASK_VALUE = -1e30
ATT_SCALE = HEAD_DIM ** -0.5
MAX_MEM_LEN = 1536
HANDED = 128
PAIR = 2 * HEAD_DIM
TILE = 256
CHUNK = 512
NN = (((1,), (0,)), ((), ()))
NT = (((1,), (1,)), ((), ()))
F32 = jnp.float32
BF16 = jnp.bfloat16
MESH = pl.DeviceIdType.MESH
VMEM_LIMIT = 60 * 1024 * 1024
ANY = pl.BlockSpec(memory_space=pl.ANY)
VMEM = pl.BlockSpec(memory_space=pltpu.VMEM)
SMEM = pl.BlockSpec(memory_space=pltpu.SMEM)


def rms_norm(val32, gain_row):
    inv_rms = lax.rsqrt(jnp.mean(val32 * val32, axis=-1, keepdims=True) + NORM_EPS)
    return (val32 * inv_rms * gain_row).astype(BF16)


def dot(lhs, rhs, dims=NN):
    return lax.dot_general(lhs, rhs, dims, preferred_element_type=F32)


def col_scores(k_val, q_val, buf, size, mask, n, m_ref, mc):
    width = q_val.shape[1]
    s = dot(k_val, q_val)
    if mask is not None:
        s = jnp.where(mask, s, MASK_VALUE)
    buf[:size, :width] = s
    mc[:, :width] = jnp.maximum(m_ref[n, :, :width], jnp.max(s, axis=0, keepdims=True))


def col_softmax(buf, size, width, mc, n, m_ref, l_ref):
    m_new = mc[:, :width]
    alpha = jnp.exp(m_ref[n, :, :width] - m_new)
    e = jnp.exp(buf[:size, :width] - m_new)
    l_ref[n, :, :width] = l_ref[n, :, :width] * alpha + jnp.sum(e, axis=0, keepdims=True)
    m_ref[n, :, :width] = m_new
    return e.astype(BF16), alpha


def layer_kernel(n_sp, n_layers, len_ref, hid_hbm, mem_hbm, gain_s, gain_c, gain_m, wq_hbm, wk_hbm, wv_hbm, wo_hbm, cq_hbm,
                 ck_hbm, cv_hbm, co_hbm, wg_hbm, wu_hbm, wd_hbm, out_ref,
                 y, h_own, h_rem, mem, ck, cv, mkv, mall, wq, wk, wv, wqt, wvt, wo, cq, co, wg, wu, wd,
                 qm, qc, k_s, vt_s, k_c, vt_c, m_ref, l_ref, acc, b0, b1, mc0, mc1, o_stage, o_full, act, gains,
                 y_give, y_take, o_take, y_back, y_done, o_part,
                 w_sem, own_sem, ici_s, ici_r, d2d_s, d2d_r, mi_s, mi_r, mo_s, mo_r, md_s, md_r, o_sem,
                 give_s, give_r):
    rows, d_model = y.shape
    half = rows // 2
    width = d_model // 2
    pairs = width // PAIR
    tiles = 2 * rows // TILE
    row_tiles = rows // TILE
    all_pairs = d_model // PAIR
    used, _, mrows, mcols = mall.shape
    mh = mrows // 2
    kv_dim = mcols // 2
    n_kv = kv_dim // HEAD_DIM
    group = all_pairs // n_kv
    ff = act.shape[1]
    n_chip = n_sp // 2
    me = lax.axis_index("sp")
    chip, core = me // 2, lax.rem(me, 2)
    other = 1 - core
    right, left = lax.rem(chip + 1, n_chip), lax.rem(chip + n_chip - 1, n_chip)
    opp = lax.rem(chip + 2, n_chip)
    partner = 2 * chip + other
    dev_r, dev_l = 2 * right + core, 2 * left + core
    last = n_chip - 1
    gives, takes = chip == last, chip == 0
    mate = 2 * (n_chip - 1 - chip) + core
    keep = rows - HANDED
    wide = 2 * keep

    def remote(src, dst, send, recv, dev):
        return pltpu.make_async_remote_copy(
            src_ref=src, dst_ref=dst, send_sem=send, recv_sem=recv, device_id={"sp": dev}, device_id_type=MESH)

    cols = pl.ds(pl.multiple_of(core * width, 128), width)
    own_rows = pl.ds(pl.multiple_of(core * rows, rows), rows)
    other_rows = pl.ds(pl.multiple_of(other * rows, rows), rows)

    def loads(layer):
        specs = [(wq_hbm.at[layer, :, cols], wq), (wk_hbm.at[layer, :, cols], wk), (wv_hbm.at[layer, :, cols], wv),
                 (wo_hbm.at[layer], wo), (cq_hbm.at[layer], cq), (co_hbm.at[layer], co), (wg_hbm.at[layer], wg),
                 (wu_hbm.at[layer], wu), (wd_hbm.at[layer], wd)]
        return [pltpu.make_async_copy(src, dst, w_sem.at[i]) for i, (src, dst) in enumerate(specs)]

    first = [pltpu.make_async_copy(src, dst, w_sem.at[9 + i])
             for i, (src, dst) in enumerate(((hid_hbm, y), (mem_hbm, mem), (ck_hbm, ck), (cv_hbm, cv)))]
    first[0].start()
    w_first = loads(0)
    for copy in (*w_first[:3], *first[1:], *w_first[3:]):
        copy.start()

    barrier = pltpu.get_barrier_semaphore()
    for dev in (dev_r, dev_l, partner):
        pl.semaphore_signal(barrier, inc=1, device_id={"sp": dev}, device_id_type=MESH)

    for i, ref in enumerate((gain_s, gain_c, gain_m)):
        for j in range(n_layers):
            gains[i, j] = ref[j:j + 1].astype(F32)

    first[0].wait()
    h_own[0, own_rows] = rms_norm(y[...].astype(F32), gains[0, 0])
    pl.semaphore_wait(barrier, 3)

    to_r, to_l = chip < right, chip < left
    b_to_l = to_l | (chip < opp)
    relay_a, relay_b = left < right, right < left
    need_l, need_r, need_o = left < chip, right < chip, opp < chip
    got_rb = need_r | relay_b
    need = (need_l, need_r, need_l, need_r, need_o, need_o)
    got = (need_l, got_rb, need_l, need_r, need_o, need_o)
    sent = (to_r, b_to_l, to_r, to_l)

    def row_copies(layer):
        own_a = h_own.at[layer, pl.ds(pl.multiple_of(core * rows, half), half)]
        own_b = h_own.at[layer, pl.ds(pl.multiple_of(core * rows + half, half), half)]
        slot = [h_rem.at[layer, i, core] for i in range(6)]
        srcs = (own_a, own_b, own_b, own_a, slot[0], slot[1])
        ring = [remote(srcs[i], slot[i], ici_s.at[layer, i], ici_r.at[layer, i], dev_l if i % 2 else dev_r)
                for i in (0, 1)]
        ring += [remote(srcs[2], slot[2], ici_s.at[layer, 2], ici_r.at[layer, 2], dev_r),
                 remote(srcs[3], slot[3], ici_s.at[layer, 3], ici_r.at[layer, 3], dev_l),
                 remote(srcs[4], slot[4], ici_s.at[layer, 4], ici_r.at[layer, 4], dev_r),
                 remote(srcs[5], slot[5], ici_s.at[layer, 5], ici_r.at[layer, 5], dev_l)]
        fwd = [remote(slot[i], slot[i], d2d_s.at[layer, i], d2d_r.at[layer, i], partner) for i in range(6)]
        own = remote(h_own.at[layer, own_rows], h_own.at[layer, own_rows], own_sem.at[layer, 0], own_sem.at[layer, 1],
                     partner)
        return ring, fwd, own

    def give_copies(layer):
        return [remote(y_give.at[layer], y_take.at[layer], give_s.at[layer, 0], give_r.at[layer, 0], mate),
                remote(o_full.at[layer, :, pl.ds(keep, HANDED)], o_take.at[layer], give_s.at[layer, 1],
                       give_r.at[layer, 1], mate),
                remote(y_back.at[layer], y_done.at[layer], give_s.at[layer, 2], give_r.at[layer, 2], mate)]

    def give_y(layer):
        @pl.when(gives)
        def _():
            give_copies(layer)[0].start()

    def when_start(cond, copy):
        @pl.when(cond)
        def _():
            copy.start()

    def when_sent(cond, copy):
        @pl.when(cond)
        def _():
            copy.wait_send()

    def when_recv(cond, copy):
        @pl.when(cond)
        def _():
            copy.wait_recv()

    has_m = 2 * chip < used
    has_l, has_r, has_o = 2 * left < used, 2 * right < used, 2 * opp < used

    def blk(who, core_of):
        return jnp.minimum(2 * who + core_of, used - 1)

    b_me, b_l, b_r, b_o = blk(chip, core), blk(left, core), blk(right, core), blk(opp, core)
    top, low = pl.ds(0, mh), pl.ds(mh, mh)
    m_own = [
        remote(mkv, mall.at[b_me], mi_s.at[0], mi_r.at[0], dev_r),
        remote(mkv, mall.at[b_me], mi_s.at[1], mi_r.at[1], dev_l),
        remote(mkv, mall.at[b_me], md_s.at[0], md_r.at[0], partner),
    ]
    m_relay_l = [
        (remote(mall.at[b_l, :, top], mall.at[b_l, :, top], mo_s.at[0], mo_r.at[0], dev_r), has_l & (chip < last)),
        (remote(mall.at[b_l, :, low], mall.at[b_l, :, low], mo_s.at[1], mo_r.at[1], dev_r),
         has_l & (chip < last) & (right < last)),
    ]
    m_relay_r = [
        (remote(mall.at[b_r, :, top], mall.at[b_r, :, top], mo_s.at[2], mo_r.at[0], dev_l),
         has_r & (chip < last) & (left < last)),
        (remote(mall.at[b_r, :, low], mall.at[b_r, :, low], mo_s.at[3], mo_r.at[1], dev_l), has_r & (chip < last)),
    ]
    m_halves = [
        remote(mall.at[b_o, :, top], mall.at[b_o, :, top], mo_s.at[0], mo_r.at[0], dev_r),
        remote(mall.at[b_o, :, low], mall.at[b_o, :, low], mo_s.at[1], mo_r.at[1], dev_r),
    ]
    m_fwd = [
        remote(mall.at[b_l], mall.at[b_l], md_s.at[1], md_r.at[1], partner),
        remote(mall.at[b_r], mall.at[b_r], md_s.at[2], md_r.at[2], partner),
        remote(mall.at[b_o, :, top], mall.at[b_o, :, top], md_s.at[3], md_r.at[3], partner),
        remote(mall.at[b_o, :, low], mall.at[b_o, :, low], md_s.at[4], md_r.at[4], partner),
    ]
    m_has = (has_l, has_r, has_o, has_o)

    def start_rows(layer):
        ring, _, own = row_copies(layer)
        own.start()
        when_start(sent[0], ring[0])
        when_start(sent[1], ring[1])

    y_give[0] = y[keep:]
    start_rows(0)
    give_y(0)
    for copy in first[1:]:
        copy.wait()

    @pl.when(has_m)
    def _():
        for i in range(n_layers):
            mkv[i, :, :kv_dim] = dot(mem[...], ck[i]).astype(BF16)
            mkv[i, :, kv_dim:] = dot(mem[...], cv[i]).astype(BF16)
        mall[b_me] = mkv[...]
    def from_left():
        when_recv(has_l, m_own[0])
        when_start(has_l, m_fwd[0])
        for copy, cond in m_relay_l:
            when_start(cond, copy)

    def from_right():
        when_recv(has_r, m_own[1])
        when_start(has_r, m_fwd[1])
        for copy, cond in m_relay_r:
            when_start(cond, copy)

    qm[...] = jnp.zeros_like(qm)
    ones_row = (lax.broadcasted_iota(jnp.int32, (PAIR - HEAD_DIM, qc.shape[2]), 0) == 0).astype(F32).astype(BF16)
    for n in range(qc.shape[0]):
        qc[n, HEAD_DIM:] = ones_row
    when_start(has_m, m_own[2])
    when_start(has_m & (left < chip), m_own[1])

    def reset():
        m_ref[...] = jnp.full_like(m_ref, MASK_VALUE)
        l_ref[...] = jnp.zeros_like(l_ref)
        acc[...] = jnp.zeros_like(acc)

    def pipelined(count, unroll, item, scores, softmax):
        bufs, mcs = (b0, b1), (mc0, mc1)

        def at(i):
            return item(jnp.minimum(i, count - 1))

        scores(at(0), b0, mc0)

        def body(i, carry):
            for u in range(unroll):
                scores(at(unroll * i + u + 1), bufs[(u + 1) % 2], mcs[(u + 1) % 2])
                softmax(at(unroll * i + u), bufs[u % 2], mcs[u % 2])
            return carry

        lax.fori_loop(0, count // unroll, body, 0)

    def finish(n, m, first=0):
        span = slice(first, first + 2 * m)
        val = acc[n, :, span] * (1.0 / l_ref[n, :, span])
        return jnp.concatenate([val[:, :m], val[:, m:]], axis=0).astype(BF16).T

    def project_kv(pieces):
        size = CHUNK // len(pieces)
        for i, piece in enumerate(pieces):
            span = slice(i * size, (i + 1) * size)
            k_val = dot(piece, wk[...]).astype(BF16)
            v_val = dot(wvt[...], piece, NT).astype(BF16)
            for p in range(pairs):
                k_s[p, span] = k_val[:, p * PAIR:(p + 1) * PAIR]
                vt_s[p, :, span] = v_val[p * PAIR:(p + 1) * PAIR]

    def self_scores(pn, buf, mc, size=CHUNK, mask=None):
        p, n = pn
        col_scores(k_s[p, :size], qm[n], buf, size, mask, n, m_ref, mc)

    def self_softmax(pn, buf, mc, size=CHUNK):
        p, n = pn
        w = 2 * TILE
        e, alpha = col_softmax(buf, size, w, mc, n, m_ref, l_ref)
        acc[n, :, :TILE] = acc[n, :, :TILE] * alpha[:, :TILE] + dot(vt_s[p, :HEAD_DIM, :size], e[:, :TILE])
        acc[n, :, TILE:w] = acc[n, :, TILE:w] * alpha[:, TILE:] + dot(vt_s[p, HEAD_DIM:, :size], e[:, TILE:])

    def attend(first_tile, n_tiles, unroll):
        def item(i):
            p = i // n_tiles
            return p, p * tiles + first_tile + lax.rem(i, n_tiles)

        pipelined(pairs * n_tiles, unroll, item, self_scores, self_softmax)

    def rest_of_layer(layer, y_rows, o_rows, m):
        per = wide // (2 * m)
        w = 2 * m * per
        sets = all_pairs // per
        per_group = group // per
        m_ref[:sets, :, :w] = jnp.full((sets, 1, w), MASK_VALUE, F32)
        l_ref[:sets, :, :w] = jnp.zeros((sets, 1, w), F32)
        acc[:sets, :, :w] = jnp.zeros((sets, HEAD_DIM, w), F32)
        upd = dot(o_rows[0], wo[:width]) + dot(o_rows[1], wo[width:])
        y1 = (y_rows[...].astype(F32) + upd).astype(BF16)
        y_rows[...] = y1
        h = rms_norm(y1.astype(F32), gains[1, layer])
        q_val = (dot(h, cq[...]).astype(BF16) * ATT_SCALE).astype(BF16)
        for p in range(all_pairs):
            qt = q_val[:, p * PAIR:(p + 1) * PAIR].T
            n, at = p // per, (p % per) * 2 * m
            qc[n, :HEAD_DIM, at:at + m] = qt[:HEAD_DIM]
            qc[n, :HEAD_DIM, at + m:at + 2 * m] = qt[HEAD_DIM:]

        def item(i):
            c, n = i // sets, lax.rem(i, sets)
            return pl.ds(pl.multiple_of(c * CHUNK, CHUNK), CHUNK), n // per_group, n

        def scores(cgn, buf, mc):
            keys, g, n = cgn
            col_scores(k_c[g, keys], qc[n, :, :w], buf, CHUNK, None, n, m_ref, mc)

        def softmax(cgn, buf, mc):
            keys, g, n = cgn
            e, alpha = col_softmax(buf, CHUNK, w, mc, n, m_ref, l_ref)
            acc[n, :, :w] = acc[n, :, :w] * alpha + dot(vt_c[g, :, keys], e)

        count = sets * (used * mrows // CHUNK)
        pipelined(count, count, item, scores, softmax)
        o2 = act.at[:m, :d_model]
        for p in range(all_pairs):
            o2[:, p * PAIR:(p + 1) * PAIR] = finish(p // per, m, (p % per) * 2 * m)
        y2 = (y_rows[...].astype(F32) + dot(o2[...], co[...])).astype(BF16)
        y_rows[...] = y2
        h = rms_norm(y2.astype(F32), gains[2, layer])
        for c in range(0, ff, CHUNK):
            gate = dot(h, wg[:, c:c + CHUNK])
            act[:m, c:c + CHUNK] = (jax.nn.silu(gate) * dot(h, wu[:, c:c + CHUNK])).astype(BF16)
        y_rows[...] = (y_rows[...].astype(F32) + dot(act[:m], wd[...])).astype(BF16)

    def layer_body(layer, carry):
        ring, fwd, own = row_copies(layer)
        weights = loads(layer)
        reset()
        for copy in weights[:3]:
            copy.wait()
        wqt[...] = wq[...].T
        wvt[...] = wv[...].T

        def own_block(i, inner):
            block = jnp.where(i == 0, core, other)

            @pl.when(i == 1)
            def _():
                own.wait_recv()

            h_blk = h_own[layer, pl.ds(pl.multiple_of(block * rows, rows), rows)]
            q_val = (dot(wqt[...], h_blk, NT).astype(BF16) * ATT_SCALE).astype(BF16)
            for p in range(pairs):
                for t in range(row_tiles):
                    n = p * tiles + block * row_tiles + t
                    span = slice(t * TILE, (t + 1) * TILE)
                    qm[n, :HEAD_DIM, :TILE] = q_val[p * PAIR:p * PAIR + HEAD_DIM, span]
                    qm[n, HEAD_DIM:, TILE:] = q_val[p * PAIR + HEAD_DIM:(p + 1) * PAIR, span]
            return inner

        lax.fori_loop(0, 2, own_block, 0)

        def own_keys(block, inner):
            project_kv([h_own[layer, pl.ds(pl.multiple_of(block * rows, rows), rows)]])
            key = lax.broadcasted_iota(jnp.int32, (CHUNK, 2 * TILE), 0)
            query = lax.broadcasted_iota(jnp.int32, (CHUNK, 2 * TILE), 1) % TILE

            order = [(p, t) for p in range(pairs) for t in range(row_tiles)]
            bufs, mcs = (b0, b1), (mc0, mc1)
            masks = (key[:TILE] <= query[:TILE], key <= query + TILE)

            def diagonal(j, step):
                p, t = order[j]
                step((p, p * tiles + block * row_tiles + t), bufs[j % 2], mcs[j % 2], t)

            def diagonal_scores(pn, buf, mc, t):
                self_scores(pn, buf, mc, (t + 1) * TILE, masks[t])

            def diagonal_softmax(pn, buf, mc, t):
                self_softmax(pn, buf, mc, (t + 1) * TILE)

            diagonal(0, diagonal_scores)
            for j in range(len(order)):
                if j + 1 < len(order):
                    diagonal(j + 1, diagonal_scores)
                diagonal(j, diagonal_softmax)

            @pl.when(block == 0)
            def _():
                attend(tiles // 2, tiles // 2, pairs * tiles // 2)
                when_start(sent[2], ring[2])
                when_start(sent[3], ring[3])

            return inner

        lax.fori_loop(0, 2, own_keys, 0)

        def take(i):
            when_recv(got[i], ring[i])
            if i == 0:
                when_start(relay_a, ring[4])
            if i == 1:
                when_start(relay_b, ring[5])
            when_start(need[i], fwd[i])

        def attend_two(stage, inner):
            @pl.when(stage == 0)
            def _():
                take(0)
                take(1)

                @pl.when(layer == 0)
                def _():
                    when_start(has_m, m_own[0])
                    when_start(has_m & (left > chip), m_own[1])

                    @pl.when(chip < last)
                    def _():
                        from_right()


            @pl.when(stage == 1)
            def _():
                take(2)
                take(3)

            @pl.when(stage == 2)
            def _():
                take(4)
                take(5)

            any_need = jnp.where(stage == 2, opp, left) < chip
            both = jnp.where(stage == 2, opp, right) < chip

            def one(i, deep):
                @pl.when(i == 1)
                def _():
                    for j in range(3):
                        @pl.when(stage == j)
                        def _(j=j):
                            when_recv(need[2 * j], fwd[2 * j])
                            when_recv(need[2 * j + 1], fwd[2 * j + 1])

                @pl.when((stage == 2) & (i == 1) & (layer == 0))
                def _():
                    from_left()

                    @pl.when(chip == last)
                    def _():
                        from_right()

                @pl.when(any_need & ((i == 1) | both))
                def _():
                    from_a = jnp.where((i == 1) & both, other, core)
                    from_b = jnp.where(i == 1, other, core)
                    slot_b = jnp.where(both, 2 * stage + 1, 2 * stage)
                    project_kv([h_rem[layer, 2 * stage, from_a], h_rem[layer, slot_b, from_b]])
                    attend(0, tiles, pairs * tiles)

                return deep

            return lax.fori_loop(0, 2, one, inner)

        lax.fori_loop(0, 3, attend_two, 0)

        for block, dst in ((other, o_stage), (core, None)):
            for p in range(pairs):
                for t in range(row_tiles):
                    val = finish(p * tiles + block * row_tiles + t, TILE)
                    span = slice(t * TILE, (t + 1) * TILE)
                    if dst is not None:
                        dst[layer, span, p * PAIR:(p + 1) * PAIR] = val
                    else:
                        o_full[layer, core, span, p * PAIR:(p + 1) * PAIR] = val
        o_send = remote(o_stage.at[layer], o_full.at[layer, core], o_sem.at[layer, 0], o_sem.at[layer, 1], partner)
        o_send.start()

        @pl.when(layer + 1 < n_layers)
        def _():
            for copy in loads(layer + 1)[:3]:
                copy.start()

        @pl.when(layer == 0)
        def _():
            when_recv(has_o, m_halves[0])
            when_start(has_o, m_fwd[2])
            when_recv(has_o, m_halves[1])
            when_start(has_o, m_fwd[3])
            when_recv(has_m, m_own[2])
            for cond, copy in zip(m_has, m_fwd):
                when_recv(cond, copy)

        mem_len = len_ref[0]
        for b in range(used):
            span = slice(b * mrows, (b + 1) * mrows)
            vt = mall[b, layer, :, kv_dim:].T
            pos = lax.broadcasted_iota(jnp.int32, (mrows, HEAD_DIM), 0) + b * mrows
            lane = lax.broadcasted_iota(jnp.int32, (mrows, HEAD_DIM), 1)
            bias = jnp.where((pos >= mem_len) & (lane == 0), MASK_VALUE, 0.0).astype(BF16)
            for g in range(n_kv):
                k_c[g, span, :HEAD_DIM] = mall[b, layer, :, g * HEAD_DIM:(g + 1) * HEAD_DIM]
                k_c[g, span, HEAD_DIM:] = bias
                vt_c[g, :, span] = vt[g * HEAD_DIM:(g + 1) * HEAD_DIM]

        o_send.wait_recv()
        y_copy, o_copy, back_copy = give_copies(layer)
        when_start(gives, o_copy)
        for copy in weights[3:]:
            copy.wait()
        rest_of_layer(layer, y.at[:keep], o_full.at[layer, :, pl.ds(0, keep)], keep)

        def next_rows(span):
            h_own[layer + 1, pl.ds(core * rows + span.start, span.stop - span.start)] = rms_norm(
                y[span].astype(F32), gains[0, layer + 1])

        @pl.when(layer + 1 < n_layers)
        def _():
            next_rows(slice(0, keep))

        def next_start():
            @pl.when(layer + 1 < n_layers)
            def _():
                next_rows(slice(keep, rows))
                y_give[layer + 1] = y[keep:]
                start_rows(layer + 1)
                give_y(layer + 1)

        def handed(i, inner):
            @pl.when(i == 0)
            def _():
                y_back[layer] = y[keep:]
                o_part[...] = o_full[layer, :, keep:]

            @pl.when(i == 1)
            def _():
                y_copy.wait_recv()
                o_copy.wait_recv()
                y_back[layer] = y_take[layer]
                o_part[...] = o_take[layer]

            rest_of_layer(layer, y_back.at[layer], o_part, HANDED)

            @pl.when(i == 0)
            def _():
                y[keep:] = y_back[layer]
                next_start()

            return inner

        @pl.when(jnp.logical_not(gives))
        def _():
            lax.fori_loop(0, jnp.where(takes, 2, 1), handed, 0)

        @pl.when(takes)
        def _():
            back_copy.start()

        @pl.when(gives)
        def _():
            back_copy.wait_recv()
            y[keep:] = y_done[layer]
            next_start()

        @pl.when(layer + 1 < n_layers)
        def _():
            for copy in loads(layer + 1)[3:]:
                copy.start()

        return carry

    lax.fori_loop(0, n_layers, layer_body, 0)
    out_ref[...] = y[...]

    for copy in m_own:
        when_sent(has_m, copy)
    for copy, cond in (*m_relay_l, *m_relay_r):
        when_sent(cond, copy)
    for cond, copy in zip(m_has, m_fwd):
        when_sent(cond, copy)

    def sent_all(layer, carry):
        ring, fwd, own = row_copies(layer)
        y_copy, o_copy, back_copy = give_copies(layer)
        own.wait_send()
        remote(o_stage.at[layer], o_full.at[layer, core], o_sem.at[layer, 0], o_sem.at[layer, 1], partner).wait_send()
        for cond, copy in zip((*sent, relay_a, relay_b), ring):
            when_sent(cond, copy)
        for cond, copy in zip(need, fwd):
            when_sent(cond, copy)
        when_sent(gives, y_copy)
        when_sent(gives, o_copy)
        when_sent(takes, back_copy)
        return carry

    lax.fori_loop(0, n_layers, sent_all, 0)


def layers_call(n_sp, mem_len, hidden, memory, gain_self, gain_cross, gain_mlp, self_q, self_k, self_v, self_o, cross_q,
                cross_k, cross_v, cross_o, gate, up, down):
    rows, d_model = hidden.shape
    layers = gain_self.shape[0]
    width = d_model // 2
    ff = gate.shape[2]
    mrows, mcols = memory.shape[0], 2 * cross_k.shape[2]
    used = min(n_sp, pl.cdiv(MAX_MEM_LEN, mrows))
    n_kv = cross_k.shape[2] // HEAD_DIM
    pairs, tiles = width // PAIR, 2 * rows // TILE
    combos = pairs * tiles
    wide = 2 * (rows - HANDED)
    dma = pltpu.SemaphoreType.DMA
    return pl.pallas_call(
        functools.partial(layer_kernel, n_sp, layers),
        out_shape=jax.ShapeDtypeStruct((rows, d_model), BF16),
        in_specs=[SMEM, ANY, ANY, VMEM, VMEM, VMEM] + [ANY] * 11,
        out_specs=VMEM,
        scratch_shapes=[
            pltpu.VMEM((rows, d_model), BF16),
            pltpu.VMEM((layers, 2 * rows, d_model), BF16),
            pltpu.VMEM((layers, 6, 2, rows // 2, d_model), BF16),
            pltpu.VMEM((mrows, d_model), BF16),
            *[pltpu.VMEM(cross_k.shape, BF16)] * 2,
            pltpu.VMEM((layers, mrows, mcols), BF16),
            pltpu.VMEM((used, layers, mrows, mcols), BF16),
            *[pltpu.VMEM((d_model, width), BF16)] * 3,
            *[pltpu.VMEM((width, d_model), BF16)] * 2,
            *[pltpu.VMEM((d_model, d_model), BF16)] * 3,
            *[pltpu.VMEM((d_model, ff), BF16)] * 2,
            pltpu.VMEM((ff, d_model), BF16),
            pltpu.VMEM((combos, PAIR, 2 * TILE), BF16),
            pltpu.VMEM((2 * pairs, PAIR, wide), BF16),
            pltpu.VMEM((pairs, CHUNK, PAIR), BF16),
            pltpu.VMEM((pairs, PAIR, CHUNK), BF16),
            pltpu.VMEM((n_kv, used * mrows, PAIR), BF16),
            pltpu.VMEM((n_kv, HEAD_DIM, used * mrows), BF16),
            *[pltpu.VMEM((combos, 1, wide), F32)] * 2,
            pltpu.VMEM((combos, HEAD_DIM, wide), F32),
            *[pltpu.VMEM((CHUNK, wide), F32)] * 2,
            *[pltpu.VMEM((1, wide), F32)] * 2,
            pltpu.VMEM((layers, rows, width), BF16),
            pltpu.VMEM((layers, 2, rows, width), BF16),
            pltpu.VMEM((rows, ff), BF16),
            pltpu.VMEM((3, layers, 1, d_model), F32),
            *[pltpu.VMEM((layers, HANDED, d_model), BF16)] * 2,
            pltpu.VMEM((layers, 2, HANDED, width), BF16),
            *[pltpu.VMEM((layers, HANDED, d_model), BF16)] * 2,
            pltpu.VMEM((2, HANDED, width), BF16),
            dma((13,)), dma((layers, 2)), *[dma((layers, 6))] * 4,
            *[dma((2,))] * 2, dma((4,)), dma((2,)), *[dma((5,))] * 2, dma((layers, 2)), *[dma((layers, 3))] * 2,
        ],
        compiler_params=pltpu.CompilerParams(collective_id=0, has_side_effects=True, vmem_limit_bytes=VMEM_LIMIT),
        name="layers",
    )(mem_len, hidden, memory, gain_self, gain_cross, gain_mlp, self_q, self_k, self_v, self_o, cross_q, cross_k, cross_v,
      cross_o, gate, up, down)


def solution(mesh):
    n_sp = mesh.shape["sp"]
    row_spec = P(("dp", "sp"), None)

    def device_fn(dec_hidden, memory, mem_len, *weights):
        return layers_call(n_sp, mem_len, dec_hidden, memory, *weights)

    return jax.shard_map(device_fn, mesh=mesh, in_specs=(row_spec, row_spec, P("dp")) + (P(),) * 14,
                         out_specs=row_spec, check_vma=False)
```

```python
import functools

import jax
import jax.numpy as jnp
from jax import lax
from jax.experimental import pallas as pl
from jax.experimental.pallas import tpu as pltpu
from jax.sharding import PartitionSpec as P

HEAD_DIM = 64
NORM_EPS = 1e-6
MASK_VALUE = -1e30
ATT_SCALE = HEAD_DIM ** -0.5
MAX_MEM_LEN = 1536
HANDED = 128
PAIR = 2 * HEAD_DIM
TILE = 256
CHUNK = 512
NN = (((1,), (0,)), ((), ()))
NT = (((1,), (1,)), ((), ()))
F32 = jnp.float32
BF16 = jnp.bfloat16
MESH = pl.DeviceIdType.MESH
VMEM_LIMIT = 60 * 1024 * 1024
ANY = pl.BlockSpec(memory_space=pl.ANY)
VMEM = pl.BlockSpec(memory_space=pltpu.VMEM)
SMEM = pl.BlockSpec(memory_space=pltpu.SMEM)


def rms_norm(val32, gain_row):
    inv_rms = lax.rsqrt(jnp.mean(val32 * val32, axis=-1, keepdims=True) + NORM_EPS)
    return (val32 * inv_rms * gain_row).astype(BF16)


def dot(lhs, rhs, dims=NN):
    return lax.dot_general(lhs, rhs, dims, preferred_element_type=F32)


def col_scores(k_val, q_val, buf, size, mask, n, m_ref, mc):
    width = q_val.shape[1]
    s = dot(k_val, q_val)
    if mask is not None:
        s = jnp.where(mask, s, MASK_VALUE)
    buf[:size, :width] = s
    mc[:, :width] = jnp.maximum(m_ref[n, :, :width], jnp.max(s, axis=0, keepdims=True))


def col_softmax(buf, size, width, mc, n, m_ref, l_ref):
    m_new = mc[:, :width]
    alpha = jnp.exp(m_ref[n, :, :width] - m_new)
    e = jnp.exp(buf[:size, :width] - m_new)
    l_ref[n, :, :width] = l_ref[n, :, :width] * alpha + jnp.sum(e, axis=0, keepdims=True)
    m_ref[n, :, :width] = m_new
    return e.astype(BF16), alpha


def layer_kernel(n_sp, n_layers, len_ref, hid_hbm, mem_hbm, gain_s, gain_c, gain_m, wq_hbm, wk_hbm, wv_hbm, wo_hbm, cq_hbm,
                 ck_hbm, cv_hbm, co_hbm, wg_hbm, wu_hbm, wd_hbm, out_ref,
                 y, h_own, h_rem, mem, ck, cv, mkv, mall, wq, wk, wv, wqt, wvt, wo, cq, co, wg, wu, wd,
                 qm, qc, k_s, vt_s, k_c, vt_c, m_ref, l_ref, acc, b0, b1, mc0, mc1, o_stage, o_full, act, gains,
                 y_give, y_take, o_take, y_back, y_done, o_part,
                 w_sem, own_sem, ici_s, ici_r, d2d_s, d2d_r, mi_s, mi_r, mo_s, mo_r, md_s, md_r, o_sem,
                 give_s, give_r):
    rows, d_model = y.shape
    half = rows // 2
    width = d_model // 2
    pairs = width // PAIR
    tiles = 2 * rows // TILE
    row_tiles = rows // TILE
    all_pairs = d_model // PAIR
    used, _, mrows, mcols = mall.shape
    mh = mrows // 2
    kv_dim = mcols // 2
    n_kv = kv_dim // HEAD_DIM
    group = all_pairs // n_kv
    ff = act.shape[1]
    n_chip = n_sp // 2
    me = lax.axis_index("sp")
    chip, core = me // 2, lax.rem(me, 2)
    other = 1 - core
    right, left = lax.rem(chip + 1, n_chip), lax.rem(chip + n_chip - 1, n_chip)
    opp = lax.rem(chip + 2, n_chip)
    partner = 2 * chip + other
    dev_r, dev_l = 2 * right + core, 2 * left + core
    last = n_chip - 1
    gives, takes = chip == last, chip == 0
    mate = 2 * (n_chip - 1 - chip) + core
    mate_other = 2 * (n_chip - 1 - chip) + other
    keep = rows - HANDED
    wide = 2 * keep

    def remote(src, dst, send, recv, dev):
        return pltpu.make_async_remote_copy(
            src_ref=src, dst_ref=dst, send_sem=send, recv_sem=recv, device_id={"sp": dev}, device_id_type=MESH)

    cols = pl.ds(pl.multiple_of(core * width, 128), width)
    own_rows = pl.ds(pl.multiple_of(core * rows, rows), rows)
    other_rows = pl.ds(pl.multiple_of(other * rows, rows), rows)

    def loads(layer):
        specs = [(wq_hbm.at[layer, :, cols], wq), (wk_hbm.at[layer, :, cols], wk), (wv_hbm.at[layer, :, cols], wv),
                 (wo_hbm.at[layer], wo), (cq_hbm.at[layer], cq), (co_hbm.at[layer], co), (wg_hbm.at[layer], wg),
                 (wu_hbm.at[layer], wu), (wd_hbm.at[layer], wd)]
        return [pltpu.make_async_copy(src, dst, w_sem.at[i]) for i, (src, dst) in enumerate(specs)]

    first = [pltpu.make_async_copy(src, dst, w_sem.at[9 + i])
             for i, (src, dst) in enumerate(((hid_hbm, y), (mem_hbm, mem), (ck_hbm, ck), (cv_hbm, cv)))]
    first[0].start()
    w_first = loads(0)
    for copy in (*w_first[:3], *first[1:], *w_first[3:]):
        copy.start()

    barrier = pltpu.get_barrier_semaphore()
    for dev in (dev_r, dev_l, partner, mate_other):
        pl.semaphore_signal(barrier, inc=1, device_id={"sp": dev}, device_id_type=MESH)

    for i, ref in enumerate((gain_s, gain_c, gain_m)):
        for j in range(n_layers):
            gains[i, j] = ref[j:j + 1].astype(F32)

    first[0].wait()
    h_own[0, own_rows] = rms_norm(y[...].astype(F32), gains[0, 0])
    pl.semaphore_wait(barrier, 4)

    to_r, to_l = chip < right, chip < left
    b_to_l = to_l | (chip < opp)
    relay_a, relay_b = left < right, right < left
    need_l, need_r, need_o = left < chip, right < chip, opp < chip
    got_rb = need_r | relay_b
    need = (need_l, need_r, need_l, need_r, need_o, need_o)
    got = (need_l, got_rb, need_l, need_r, need_o, need_o)
    sent = (to_r, b_to_l, to_r, to_l)

    def row_copies(layer):
        own_a = h_own.at[layer, pl.ds(pl.multiple_of(core * rows, half), half)]
        own_b = h_own.at[layer, pl.ds(pl.multiple_of(core * rows + half, half), half)]
        slot = [h_rem.at[layer, i, core] for i in range(6)]
        srcs = (own_a, own_b, own_b, own_a, slot[0], slot[1])
        ring = [remote(srcs[i], slot[i], ici_s.at[layer, i], ici_r.at[layer, i], dev_l if i % 2 else dev_r)
                for i in (0, 1)]
        ring += [remote(srcs[2], slot[2], ici_s.at[layer, 2], ici_r.at[layer, 2], dev_r),
                 remote(srcs[3], slot[3], ici_s.at[layer, 3], ici_r.at[layer, 3], dev_l),
                 remote(srcs[4], slot[4], ici_s.at[layer, 4], ici_r.at[layer, 4], dev_r),
                 remote(srcs[5], slot[5], ici_s.at[layer, 5], ici_r.at[layer, 5], dev_l)]
        fwd = [remote(slot[i], slot[i], d2d_s.at[layer, i], d2d_r.at[layer, i], partner) for i in range(6)]
        own = remote(h_own.at[layer, own_rows], h_own.at[layer, own_rows], own_sem.at[layer, 0], own_sem.at[layer, 1],
                     partner)
        return ring, fwd, own

    def give_copies(layer):
        handed_rows = pl.ds(keep, HANDED)
        return [remote(y_give.at[layer], y_take.at[layer], give_s.at[layer, 0], give_r.at[layer, 0], mate),
                remote(y_back.at[layer], y_done.at[layer], give_s.at[layer, 1], give_r.at[layer, 1], mate),
                remote(o_full.at[layer, core, handed_rows], o_take.at[layer, core], give_s.at[layer, 2],
                       give_r.at[layer, 2 + core], mate),
                remote(o_stage.at[layer, handed_rows], o_take.at[layer, core], give_s.at[layer, 3],
                       give_r.at[layer, 2 + core], mate_other)]

    def take_copies(layer):
        rows_of = o_full.at[layer, core, pl.ds(keep, HANDED)]
        return [remote(rows_of, o_take.at[layer, j], give_s.at[layer, 2], give_r.at[layer, 2 + j], mate)
                for j in range(2)]

    def give_y(layer):
        @pl.when(gives)
        def _():
            give_copies(layer)[0].start()

    def when_start(cond, copy):
        @pl.when(cond)
        def _():
            copy.start()

    def when_sent(cond, copy):
        @pl.when(cond)
        def _():
            copy.wait_send()

    def when_recv(cond, copy):
        @pl.when(cond)
        def _():
            copy.wait_recv()

    has_m = 2 * chip < used
    has_l, has_r, has_o = 2 * left < used, 2 * right < used, 2 * opp < used

    def blk(who, core_of):
        return jnp.minimum(2 * who + core_of, used - 1)

    b_me, b_l, b_r, b_o = blk(chip, core), blk(left, core), blk(right, core), blk(opp, core)
    top, low = pl.ds(0, mh), pl.ds(mh, mh)
    m_own = [
        remote(mkv, mall.at[b_me], mi_s.at[0], mi_r.at[0], dev_r),
        remote(mkv, mall.at[b_me], mi_s.at[1], mi_r.at[1], dev_l),
        remote(mkv, mall.at[b_me], md_s.at[0], md_r.at[0], partner),
    ]
    m_relay_l = [
        (remote(mall.at[b_l, :, top], mall.at[b_l, :, top], mo_s.at[0], mo_r.at[0], dev_r), has_l & (chip < last)),
        (remote(mall.at[b_l, :, low], mall.at[b_l, :, low], mo_s.at[1], mo_r.at[1], dev_r),
         has_l & (chip < last) & (right < last)),
    ]
    m_relay_r = [
        (remote(mall.at[b_r, :, top], mall.at[b_r, :, top], mo_s.at[2], mo_r.at[0], dev_l),
         has_r & (chip < last) & (left < last)),
        (remote(mall.at[b_r, :, low], mall.at[b_r, :, low], mo_s.at[3], mo_r.at[1], dev_l), has_r & (chip < last)),
    ]
    m_halves = [
        remote(mall.at[b_o, :, top], mall.at[b_o, :, top], mo_s.at[0], mo_r.at[0], dev_r),
        remote(mall.at[b_o, :, low], mall.at[b_o, :, low], mo_s.at[1], mo_r.at[1], dev_r),
    ]
    m_fwd = [
        remote(mall.at[b_l], mall.at[b_l], md_s.at[1], md_r.at[1], partner),
        remote(mall.at[b_r], mall.at[b_r], md_s.at[2], md_r.at[2], partner),
        remote(mall.at[b_o, :, top], mall.at[b_o, :, top], md_s.at[3], md_r.at[3], partner),
        remote(mall.at[b_o, :, low], mall.at[b_o, :, low], md_s.at[4], md_r.at[4], partner),
    ]
    m_has = (has_l, has_r, has_o, has_o)

    def start_rows(layer):
        ring, _, own = row_copies(layer)
        own.start()
        when_start(sent[0], ring[0])
        when_start(sent[1], ring[1])

    y_give[0] = y[keep:]
    start_rows(0)
    give_y(0)
    for copy in first[1:]:
        copy.wait()

    @pl.when(has_m)
    def _():
        for i in range(n_layers):
            mkv[i, :, :kv_dim] = dot(mem[...], ck[i]).astype(BF16)
            mkv[i, :, kv_dim:] = dot(mem[...], cv[i]).astype(BF16)
        mall[b_me] = mkv[...]
    def from_left():
        when_recv(has_l, m_own[0])
        when_start(has_l, m_fwd[0])
        for copy, cond in m_relay_l:
            when_start(cond, copy)

    def from_right():
        when_recv(has_r, m_own[1])
        when_start(has_r, m_fwd[1])
        for copy, cond in m_relay_r:
            when_start(cond, copy)

    qm[...] = jnp.zeros_like(qm)
    ones_row = (lax.broadcasted_iota(jnp.int32, (PAIR - HEAD_DIM, qc.shape[2]), 0) == 0).astype(F32).astype(BF16)
    for n in range(qc.shape[0]):
        qc[n, HEAD_DIM:] = ones_row
    when_start(has_m, m_own[2])
    when_start(has_m & (left < chip), m_own[1])

    def reset():
        m_ref[...] = jnp.full_like(m_ref, MASK_VALUE)
        l_ref[...] = jnp.zeros_like(l_ref)
        acc[...] = jnp.zeros_like(acc)

    def pipelined(count, unroll, item, scores, softmax):
        bufs, mcs = (b0, b1), (mc0, mc1)

        def at(i):
            return item(jnp.minimum(i, count - 1))

        scores(at(0), b0, mc0)

        def body(i, carry):
            for u in range(unroll):
                scores(at(unroll * i + u + 1), bufs[(u + 1) % 2], mcs[(u + 1) % 2])
                softmax(at(unroll * i + u), bufs[u % 2], mcs[u % 2])
            return carry

        lax.fori_loop(0, count // unroll, body, 0)

    def finish(n, m, first=0):
        span = slice(first, first + 2 * m)
        val = acc[n, :, span] * (1.0 / l_ref[n, :, span])
        return jnp.concatenate([val[:, :m], val[:, m:]], axis=0).astype(BF16).T

    def project_kv(pieces):
        size = CHUNK // len(pieces)
        for i, piece in enumerate(pieces):
            span = slice(i * size, (i + 1) * size)
            k_val = dot(piece, wk[...]).astype(BF16)
            v_val = dot(wvt[...], piece, NT).astype(BF16)
            for p in range(pairs):
                k_s[p, span] = k_val[:, p * PAIR:(p + 1) * PAIR]
                vt_s[p, :, span] = v_val[p * PAIR:(p + 1) * PAIR]

    def self_scores(pn, buf, mc, size=CHUNK, mask=None):
        p, n = pn
        col_scores(k_s[p, :size], qm[n], buf, size, mask, n, m_ref, mc)

    def self_softmax(pn, buf, mc, size=CHUNK):
        p, n = pn
        w = 2 * TILE
        e, alpha = col_softmax(buf, size, w, mc, n, m_ref, l_ref)
        acc[n, :, :TILE] = acc[n, :, :TILE] * alpha[:, :TILE] + dot(vt_s[p, :HEAD_DIM, :size], e[:, :TILE])
        acc[n, :, TILE:w] = acc[n, :, TILE:w] * alpha[:, TILE:] + dot(vt_s[p, HEAD_DIM:, :size], e[:, TILE:])

    def attend(first_tile, n_tiles, unroll):
        def item(i):
            p = i // n_tiles
            return p, p * tiles + first_tile + lax.rem(i, n_tiles)

        pipelined(pairs * n_tiles, unroll, item, self_scores, self_softmax)

    def rest_of_layer(layer, y_rows, o_rows, m):
        per = wide // (2 * m)
        w = 2 * m * per
        sets = all_pairs // per
        per_group = group // per
        m_ref[:sets, :, :w] = jnp.full((sets, 1, w), MASK_VALUE, F32)
        l_ref[:sets, :, :w] = jnp.zeros((sets, 1, w), F32)
        acc[:sets, :, :w] = jnp.zeros((sets, HEAD_DIM, w), F32)
        upd = dot(o_rows[0], wo[:width]) + dot(o_rows[1], wo[width:])
        y1 = (y_rows[...].astype(F32) + upd).astype(BF16)
        y_rows[...] = y1
        h = rms_norm(y1.astype(F32), gains[1, layer])
        q_val = (dot(h, cq[...]).astype(BF16) * ATT_SCALE).astype(BF16)
        for p in range(all_pairs):
            qt = q_val[:, p * PAIR:(p + 1) * PAIR].T
            n, at = p // per, (p % per) * 2 * m
            qc[n, :HEAD_DIM, at:at + m] = qt[:HEAD_DIM]
            qc[n, :HEAD_DIM, at + m:at + 2 * m] = qt[HEAD_DIM:]

        def item(i):
            c, n = i // sets, lax.rem(i, sets)
            return pl.ds(pl.multiple_of(c * CHUNK, CHUNK), CHUNK), n // per_group, n

        def scores(cgn, buf, mc):
            keys, g, n = cgn
            col_scores(k_c[g, keys], qc[n, :, :w], buf, CHUNK, None, n, m_ref, mc)

        def softmax(cgn, buf, mc):
            keys, g, n = cgn
            e, alpha = col_softmax(buf, CHUNK, w, mc, n, m_ref, l_ref)
            acc[n, :, :w] = acc[n, :, :w] * alpha + dot(vt_c[g, :, keys], e)

        count = sets * (used * mrows // CHUNK)
        pipelined(count, count, item, scores, softmax)
        o2 = act.at[:m, :d_model]
        for p in range(all_pairs):
            o2[:, p * PAIR:(p + 1) * PAIR] = finish(p // per, m, (p % per) * 2 * m)
        y2 = (y_rows[...].astype(F32) + dot(o2[...], co[...])).astype(BF16)
        y_rows[...] = y2
        h = rms_norm(y2.astype(F32), gains[2, layer])
        for c in range(0, ff, CHUNK):
            gate = dot(h, wg[:, c:c + CHUNK])
            act[:m, c:c + CHUNK] = (jax.nn.silu(gate) * dot(h, wu[:, c:c + CHUNK])).astype(BF16)
        y_rows[...] = (y_rows[...].astype(F32) + dot(act[:m], wd[...])).astype(BF16)

    def prepare(layer):
        for copy in loads(layer)[:3]:
            copy.wait()
        wqt[...] = wq[...].T
        wvt[...] = wv[...].T
        reset()

    def layer_body(layer, carry):
        ring, fwd, own = row_copies(layer)
        weights = loads(layer)
        def own_block(i, inner):
            block = jnp.where(i == 0, core, other)

            @pl.when(i == 1)
            def _():
                own.wait_recv()

            h_blk = h_own[layer, pl.ds(pl.multiple_of(block * rows, rows), rows)]
            q_val = (dot(wqt[...], h_blk, NT).astype(BF16) * ATT_SCALE).astype(BF16)
            for p in range(pairs):
                for t in range(row_tiles):
                    n = p * tiles + block * row_tiles + t
                    span = slice(t * TILE, (t + 1) * TILE)
                    qm[n, :HEAD_DIM, :TILE] = q_val[p * PAIR:p * PAIR + HEAD_DIM, span]
                    qm[n, HEAD_DIM:, TILE:] = q_val[p * PAIR + HEAD_DIM:(p + 1) * PAIR, span]
            return inner

        lax.fori_loop(0, 2, own_block, 0)

        def own_keys(block, inner):
            project_kv([h_own[layer, pl.ds(pl.multiple_of(block * rows, rows), rows)]])
            key = lax.broadcasted_iota(jnp.int32, (CHUNK, 2 * TILE), 0)
            query = lax.broadcasted_iota(jnp.int32, (CHUNK, 2 * TILE), 1) % TILE

            order = [(p, t) for p in range(pairs) for t in range(row_tiles)]
            bufs, mcs = (b0, b1), (mc0, mc1)
            masks = (key[:TILE] <= query[:TILE], key <= query + TILE)

            def diagonal(j, step):
                p, t = order[j]
                step((p, p * tiles + block * row_tiles + t), bufs[j % 2], mcs[j % 2], t)

            def diagonal_scores(pn, buf, mc, t):
                self_scores(pn, buf, mc, (t + 1) * TILE, masks[t])

            def diagonal_softmax(pn, buf, mc, t):
                self_softmax(pn, buf, mc, (t + 1) * TILE)

            diagonal(0, diagonal_scores)
            for j in range(len(order)):
                if j + 1 < len(order):
                    diagonal(j + 1, diagonal_scores)
                diagonal(j, diagonal_softmax)

            @pl.when(block == 0)
            def _():
                attend(tiles // 2, tiles // 2, pairs * tiles // 2)
                when_start(sent[2], ring[2])
                when_start(sent[3], ring[3])

            return inner

        lax.fori_loop(0, 2, own_keys, 0)

        def take(i):
            when_recv(got[i], ring[i])
            if i == 0:
                when_start(relay_a, ring[4])
            if i == 1:
                when_start(relay_b, ring[5])
            when_start(need[i], fwd[i])

        def attend_two(stage, inner):
            @pl.when(stage == 0)
            def _():
                take(0)
                take(1)

                @pl.when(layer == 0)
                def _():
                    when_start(has_m, m_own[0])
                    when_start(has_m & (left > chip), m_own[1])

                    @pl.when(chip < last)
                    def _():
                        from_right()


            @pl.when(stage == 1)
            def _():
                take(2)
                take(3)

            @pl.when(stage == 2)
            def _():
                take(4)
                take(5)

            any_need = jnp.where(stage == 2, opp, left) < chip
            both = jnp.where(stage == 2, opp, right) < chip

            def one(i, deep):
                @pl.when(i == 1)
                def _():
                    for j in range(3):
                        @pl.when(stage == j)
                        def _(j=j):
                            when_recv(need[2 * j], fwd[2 * j])
                            when_recv(need[2 * j + 1], fwd[2 * j + 1])

                @pl.when((stage == 2) & (i == 1) & (layer == 0))
                def _():
                    from_left()

                    @pl.when(chip == last)
                    def _():
                        from_right()

                @pl.when(any_need & ((i == 1) | both))
                def _():
                    from_a = jnp.where((i == 1) & both, other, core)
                    from_b = jnp.where(i == 1, other, core)
                    slot_b = jnp.where(both, 2 * stage + 1, 2 * stage)
                    project_kv([h_rem[layer, 2 * stage, from_a], h_rem[layer, slot_b, from_b]])
                    attend(0, tiles, pairs * tiles)

                return deep

            return lax.fori_loop(0, 2, one, inner)

        lax.fori_loop(0, 3, attend_two, 0)

        for t in reversed(range(row_tiles)):
            span = slice(t * TILE, (t + 1) * TILE)
            for p in range(pairs):
                o_stage[layer, span, p * PAIR:(p + 1) * PAIR] = finish(p * tiles + other * row_tiles + t, TILE)
            for p in range(pairs):
                if t == 0 and p == 1:
                    for copy in give_copies(layer)[2:]:
                        when_start(gives, copy)
                o_full[layer, core, span, p * PAIR:(p + 1) * PAIR] = finish(p * tiles + core * row_tiles + t, TILE)
        o_send = remote(o_stage.at[layer], o_full.at[layer, core], o_sem.at[layer, 0], o_sem.at[layer, 1], partner)
        o_send.start()

        @pl.when(layer + 1 < n_layers)
        def _():
            for copy in loads(layer + 1)[:3]:
                copy.start()

        @pl.when(layer == 0)
        def _():
            when_recv(has_o, m_halves[0])
            when_start(has_o, m_fwd[2])
            when_recv(has_o, m_halves[1])
            when_start(has_o, m_fwd[3])
            when_recv(has_m, m_own[2])
            for cond, copy in zip(m_has, m_fwd):
                when_recv(cond, copy)

        mem_len = len_ref[0]
        for b in range(used):
            span = slice(b * mrows, (b + 1) * mrows)
            vt = mall[b, layer, :, kv_dim:].T
            pos = lax.broadcasted_iota(jnp.int32, (mrows, HEAD_DIM), 0) + b * mrows
            lane = lax.broadcasted_iota(jnp.int32, (mrows, HEAD_DIM), 1)
            bias = jnp.where((pos >= mem_len) & (lane == 0), MASK_VALUE, 0.0).astype(BF16)
            for g in range(n_kv):
                k_c[g, span, :HEAD_DIM] = mall[b, layer, :, g * HEAD_DIM:(g + 1) * HEAD_DIM]
                k_c[g, span, HEAD_DIM:] = bias
                vt_c[g, :, span] = vt[g * HEAD_DIM:(g + 1) * HEAD_DIM]

        o_send.wait_recv()
        y_copy, back_copy = give_copies(layer)[:2]
        for copy in weights[3:]:
            copy.wait()
        rest_of_layer(layer, y.at[:keep], o_full.at[layer, :, pl.ds(0, keep)], keep)

        def next_rows(span):
            h_own[layer + 1, pl.ds(core * rows + span.start, span.stop - span.start)] = rms_norm(
                y[span].astype(F32), gains[0, layer + 1])

        @pl.when(layer + 1 < n_layers)
        def _():
            next_rows(slice(0, keep))

        def next_start():
            @pl.when(layer + 1 < n_layers)
            def _():
                next_rows(slice(keep, rows))
                y_give[layer + 1] = y[keep:]
                start_rows(layer + 1)
                give_y(layer + 1)

        def handed(i, inner):
            @pl.when(i == 0)
            def _():
                y_back[layer] = y[keep:]
                o_part[...] = o_full[layer, :, keep:]

            @pl.when(i == 1)
            def _():
                y_copy.wait_recv()
                for copy in take_copies(layer):
                    copy.wait_recv()
                y_back[layer] = y_take[layer]
                o_part[...] = o_take[layer]

            rest_of_layer(layer, y_back.at[layer], o_part, HANDED)

            @pl.when(i == 0)
            def _():
                y[keep:] = y_back[layer]
                next_start()

            return inner

        @pl.when(jnp.logical_not(gives))
        def _():
            lax.fori_loop(0, jnp.where(takes, 2, 1), handed, 0)

        @pl.when(takes)
        def _():
            back_copy.start()

        @pl.when(layer + 1 < n_layers)
        def _():
            prepare(layer + 1)

        @pl.when(gives)
        def _():
            back_copy.wait_recv()
            y[keep:] = y_done[layer]
            next_start()

        @pl.when(layer + 1 < n_layers)
        def _():
            for copy in loads(layer + 1)[3:]:
                copy.start()

        return carry

    prepare(0)
    lax.fori_loop(0, n_layers, layer_body, 0)
    out_ref[...] = y[...]

    for copy in m_own:
        when_sent(has_m, copy)
    for copy, cond in (*m_relay_l, *m_relay_r):
        when_sent(cond, copy)
    for cond, copy in zip(m_has, m_fwd):
        when_sent(cond, copy)

    def sent_all(layer, carry):
        ring, fwd, own = row_copies(layer)
        y_copy, back_copy, *o_copies = give_copies(layer)
        own.wait_send()
        remote(o_stage.at[layer], o_full.at[layer, core], o_sem.at[layer, 0], o_sem.at[layer, 1], partner).wait_send()
        for cond, copy in zip((*sent, relay_a, relay_b), ring):
            when_sent(cond, copy)
        for cond, copy in zip(need, fwd):
            when_sent(cond, copy)
        when_sent(gives, y_copy)
        for copy in o_copies:
            when_sent(gives, copy)
        when_sent(takes, back_copy)
        return carry

    lax.fori_loop(0, n_layers, sent_all, 0)


def layers_call(n_sp, mem_len, hidden, memory, gain_self, gain_cross, gain_mlp, self_q, self_k, self_v, self_o, cross_q,
                cross_k, cross_v, cross_o, gate, up, down):
    rows, d_model = hidden.shape
    layers = gain_self.shape[0]
    width = d_model // 2
    ff = gate.shape[2]
    mrows, mcols = memory.shape[0], 2 * cross_k.shape[2]
    used = min(n_sp, pl.cdiv(MAX_MEM_LEN, mrows))
    n_kv = cross_k.shape[2] // HEAD_DIM
    pairs, tiles = width // PAIR, 2 * rows // TILE
    combos = pairs * tiles
    wide = 2 * (rows - HANDED)
    dma = pltpu.SemaphoreType.DMA
    return pl.pallas_call(
        functools.partial(layer_kernel, n_sp, layers),
        out_shape=jax.ShapeDtypeStruct((rows, d_model), BF16),
        in_specs=[SMEM, ANY, ANY, VMEM, VMEM, VMEM] + [ANY] * 11,
        out_specs=VMEM,
        scratch_shapes=[
            pltpu.VMEM((rows, d_model), BF16),
            pltpu.VMEM((layers, 2 * rows, d_model), BF16),
            pltpu.VMEM((layers, 6, 2, rows // 2, d_model), BF16),
            pltpu.VMEM((mrows, d_model), BF16),
            *[pltpu.VMEM(cross_k.shape, BF16)] * 2,
            pltpu.VMEM((layers, mrows, mcols), BF16),
            pltpu.VMEM((used, layers, mrows, mcols), BF16),
            *[pltpu.VMEM((d_model, width), BF16)] * 3,
            *[pltpu.VMEM((width, d_model), BF16)] * 2,
            *[pltpu.VMEM((d_model, d_model), BF16)] * 3,
            *[pltpu.VMEM((d_model, ff), BF16)] * 2,
            pltpu.VMEM((ff, d_model), BF16),
            pltpu.VMEM((combos, PAIR, 2 * TILE), BF16),
            pltpu.VMEM((2 * pairs, PAIR, wide), BF16),
            pltpu.VMEM((pairs, CHUNK, PAIR), BF16),
            pltpu.VMEM((pairs, PAIR, CHUNK), BF16),
            pltpu.VMEM((n_kv, used * mrows, PAIR), BF16),
            pltpu.VMEM((n_kv, HEAD_DIM, used * mrows), BF16),
            *[pltpu.VMEM((combos, 1, wide), F32)] * 2,
            pltpu.VMEM((combos, HEAD_DIM, wide), F32),
            *[pltpu.VMEM((CHUNK, wide), F32)] * 2,
            *[pltpu.VMEM((1, wide), F32)] * 2,
            pltpu.VMEM((layers, rows, width), BF16),
            pltpu.VMEM((layers, 2, rows, width), BF16),
            pltpu.VMEM((rows, ff), BF16),
            pltpu.VMEM((3, layers, 1, d_model), F32),
            *[pltpu.VMEM((layers, HANDED, d_model), BF16)] * 2,
            pltpu.VMEM((layers, 2, HANDED, width), BF16),
            *[pltpu.VMEM((layers, HANDED, d_model), BF16)] * 2,
            pltpu.VMEM((2, HANDED, width), BF16),
            dma((13,)), dma((layers, 2)), *[dma((layers, 6))] * 4,
            *[dma((2,))] * 2, dma((4,)), dma((2,)), *[dma((5,))] * 2, dma((layers, 2)), *[dma((layers, 4))] * 2,
        ],
        compiler_params=pltpu.CompilerParams(collective_id=0, has_side_effects=True, vmem_limit_bytes=VMEM_LIMIT),
        name="layers",
    )(mem_len, hidden, memory, gain_self, gain_cross, gain_mlp, self_q, self_k, self_v, self_o, cross_q, cross_k, cross_v,
      cross_o, gate, up, down)


def solution(mesh):
    n_sp = mesh.shape["sp"]
    row_spec = P(("dp", "sp"), None)

    def device_fn(dec_hidden, memory, mem_len, *weights):
        return layers_call(n_sp, mem_len, dec_hidden, memory, *weights)

    return jax.shard_map(device_fn, mesh=mesh, in_specs=(row_spec, row_spec, P("dp")) + (P(),) * 14,
                         out_specs=row_spec, check_vma=False)
```

```python
import functools

import jax
import jax.numpy as jnp
from jax import lax
from jax.experimental import pallas as pl
from jax.experimental.pallas import tpu as pltpu
from jax.sharding import PartitionSpec as P

HEAD_DIM = 64
NORM_EPS = 1e-6
MASK_VALUE = -1e30
ATT_SCALE = HEAD_DIM ** -0.5
MAX_MEM_LEN = 1536
HANDED = 128
GROUP = 1
PAIR = 2 * HEAD_DIM
TILE = 256
CHUNK = 512
NN = (((1,), (0,)), ((), ()))
NT = (((1,), (1,)), ((), ()))
F32 = jnp.float32
BF16 = jnp.bfloat16
MESH = pl.DeviceIdType.MESH
VMEM_LIMIT = 52 * 1024 * 1024
ANY = pl.BlockSpec(memory_space=pl.ANY)
VMEM = pl.BlockSpec(memory_space=pltpu.VMEM)
SMEM = pl.BlockSpec(memory_space=pltpu.SMEM)


def rms_norm(val32, gain_row):
    inv_rms = lax.rsqrt(jnp.mean(val32 * val32, axis=-1, keepdims=True) + NORM_EPS)
    return (val32 * inv_rms * gain_row).astype(BF16)


def dot(lhs, rhs, dims=NN):
    return lax.dot_general(lhs, rhs, dims, preferred_element_type=F32)


def col_scores(k_val, q_val, buf, size, mask, n, m_ref, mc):
    width = q_val.shape[1]
    s = dot(k_val, q_val)
    if mask is not None:
        s = jnp.where(mask, s, MASK_VALUE)
    buf[:size, :width] = s
    mc[:, :width] = jnp.maximum(m_ref[n, :, :width], jnp.max(s, axis=0, keepdims=True))


def col_softmax(buf, size, width, mc, n, m_ref, l_ref):
    m_new = mc[:, :width]
    alpha = jnp.exp(m_ref[n, :, :width] - m_new)
    e = jnp.exp(buf[:size, :width] - m_new)
    l_ref[n, :, :width] = l_ref[n, :, :width] * alpha + jnp.sum(e, axis=0, keepdims=True)
    m_ref[n, :, :width] = m_new
    return e.astype(BF16), alpha


def layer_kernel(n_sp, n_layers, len_ref, hid_hbm, mem_hbm, gain_s, gain_c, gain_m, wq_hbm, wk_hbm, wv_hbm, wo_hbm, cq_hbm,
                 ck_hbm, cv_hbm, co_hbm, wg_hbm, wu_hbm, wd_hbm, out_ref,
                 y, h_own, h_rem, mem, ck, cv, mkv, mall, wq, wk, wv, wqt, wvt, wo, cq, co, wg, wu, wd,
                 qm, qc, k_s, vt_s, k_c, vt_c, m_ref, l_ref, acc, b0, b1, mc0, mc1, o_stage, o_full, act, gains,
                 y_give, y_take, o_take, y_back, y_done, o_part,
                 w_sem, own_sem, ici_s, ici_r, d2d_s, d2d_r, mi_s, mi_r, mo_s, mo_r, md_s, md_r, o_sem,
                 give_s, give_r):
    rows, d_model = y.shape
    half = rows // 2
    width = d_model // 2
    pairs = width // PAIR
    tiles = 2 * rows // TILE
    row_tiles = rows // TILE
    all_pairs = d_model // PAIR
    used, _, mrows, mcols = mall.shape
    mh = mrows // 2
    kv_dim = mcols // 2
    n_kv = kv_dim // HEAD_DIM
    group = all_pairs // n_kv
    ff = act.shape[1]
    n_chip = n_sp // 2
    me = lax.axis_index("sp")
    chip, core = me // 2, lax.rem(me, 2)
    other = 1 - core
    right, left = lax.rem(chip + 1, n_chip), lax.rem(chip + n_chip - 1, n_chip)
    opp = lax.rem(chip + 2, n_chip)
    partner = 2 * chip + other
    dev_r, dev_l = 2 * right + core, 2 * left + core
    last = n_chip - 1
    gives, takes = chip == last, chip == 0
    mate = 2 * (n_chip - 1 - chip) + core
    mate_other = 2 * (n_chip - 1 - chip) + other
    keep = rows - HANDED
    wide = 2 * keep

    def remote(src, dst, send, recv, dev):
        return pltpu.make_async_remote_copy(
            src_ref=src, dst_ref=dst, send_sem=send, recv_sem=recv, device_id={"sp": dev}, device_id_type=MESH)

    cols = pl.ds(pl.multiple_of(core * width, 128), width)
    own_rows = pl.ds(pl.multiple_of(core * rows, rows), rows)
    other_rows = pl.ds(pl.multiple_of(other * rows, rows), rows)

    def loads(layer):
        specs = [(wq_hbm.at[layer, :, cols], wq), (wk_hbm.at[layer, :, cols], wk), (wv_hbm.at[layer, :, cols], wv),
                 (wo_hbm.at[layer], wo), (cq_hbm.at[layer], cq), (co_hbm.at[layer], co), (wg_hbm.at[layer], wg),
                 (wu_hbm.at[layer], wu), (wd_hbm.at[layer], wd)]
        return [pltpu.make_async_copy(src, dst, w_sem.at[i]) for i, (src, dst) in enumerate(specs)]

    first = [pltpu.make_async_copy(src, dst, w_sem.at[9 + i])
             for i, (src, dst) in enumerate(((hid_hbm, y), (mem_hbm, mem), (ck_hbm, ck), (cv_hbm, cv)))]
    first[0].start()
    w_first = loads(0)
    for copy in (*w_first[:3], *first[1:], *w_first[3:]):
        copy.start()

    barrier = pltpu.get_barrier_semaphore()
    for dev in (dev_r, dev_l, partner, mate_other):
        pl.semaphore_signal(barrier, inc=1, device_id={"sp": dev}, device_id_type=MESH)

    for i, ref in enumerate((gain_s, gain_c, gain_m)):
        for j in range(n_layers):
            gains[i, j] = ref[j:j + 1].astype(F32)

    first[0].wait()
    h_own[0, own_rows] = rms_norm(y[...].astype(F32), gains[0, 0])
    pl.semaphore_wait(barrier, 4)

    to_r, to_l = chip < right, chip < left
    b_to_l = to_l | (chip < opp)
    relay_a, relay_b = left < right, right < left
    need_l, need_r, need_o = left < chip, right < chip, opp < chip
    got_rb = need_r | relay_b
    need = (need_l, need_r, need_l, need_r, need_o, need_o)
    got = (need_l, got_rb, need_l, need_r, need_o, need_o)
    sent = (to_r, b_to_l, to_r, to_l)

    def row_copies(layer):
        own_a = h_own.at[layer, pl.ds(pl.multiple_of(core * rows, half), half)]
        own_b = h_own.at[layer, pl.ds(pl.multiple_of(core * rows + half, half), half)]
        slot = [h_rem.at[layer, i, core] for i in range(6)]
        srcs = (own_a, own_b, own_b, own_a, slot[0], slot[1])
        ring = [remote(srcs[i], slot[i], ici_s.at[layer, i], ici_r.at[layer, i], dev_l if i % 2 else dev_r)
                for i in (0, 1)]
        ring += [remote(srcs[2], slot[2], ici_s.at[layer, 2], ici_r.at[layer, 2], dev_r),
                 remote(srcs[3], slot[3], ici_s.at[layer, 3], ici_r.at[layer, 3], dev_l),
                 remote(srcs[4], slot[4], ici_s.at[layer, 4], ici_r.at[layer, 4], dev_r),
                 remote(srcs[5], slot[5], ici_s.at[layer, 5], ici_r.at[layer, 5], dev_l)]
        fwd = [remote(slot[i], slot[i], d2d_s.at[layer, i], d2d_r.at[layer, i], partner) for i in range(6)]
        own = remote(h_own.at[layer, own_rows], h_own.at[layer, own_rows], own_sem.at[layer, 0], own_sem.at[layer, 1],
                     partner)
        return ring, fwd, own

    def give_copies(layer):
        handed_rows = pl.ds(keep, HANDED)
        return [remote(y_give.at[layer], y_take.at[layer], give_s.at[layer, 0], give_r.at[layer, 0], mate),
                remote(y_back.at[layer], y_done.at[layer], give_s.at[layer, 1], give_r.at[layer, 1], mate),
                remote(o_full.at[layer, core, handed_rows], o_take.at[layer, core], give_s.at[layer, 2],
                       give_r.at[layer, 2 + core], mate),
                remote(o_stage.at[layer, handed_rows], o_take.at[layer, core], give_s.at[layer, 3],
                       give_r.at[layer, 2 + core], mate_other)]

    def take_copies(layer):
        rows_of = o_full.at[layer, core, pl.ds(keep, HANDED)]
        return [remote(rows_of, o_take.at[layer, j], give_s.at[layer, 2], give_r.at[layer, 2 + j], mate)
                for j in range(2)]

    def give_y(layer):
        @pl.when(gives)
        def _():
            give_copies(layer)[0].start()

    def when_start(cond, copy):
        @pl.when(cond)
        def _():
            copy.start()

    def when_sent(cond, copy):
        @pl.when(cond)
        def _():
            copy.wait_send()

    def when_recv(cond, copy):
        @pl.when(cond)
        def _():
            copy.wait_recv()

    has_m = 2 * chip < used
    has_l, has_r, has_o = 2 * left < used, 2 * right < used, 2 * opp < used

    def blk(who, core_of):
        return jnp.minimum(2 * who + core_of, used - 1)

    b_me, b_l, b_r, b_o = blk(chip, core), blk(left, core), blk(right, core), blk(opp, core)
    top, low = pl.ds(0, mh), pl.ds(mh, mh)
    m_own = [
        remote(mkv, mall.at[b_me], mi_s.at[0], mi_r.at[0], dev_r),
        remote(mkv, mall.at[b_me], mi_s.at[1], mi_r.at[1], dev_l),
        remote(mkv, mall.at[b_me], md_s.at[0], md_r.at[0], partner),
    ]
    m_relay_l = [
        (remote(mall.at[b_l, :, top], mall.at[b_l, :, top], mo_s.at[0], mo_r.at[0], dev_r), has_l & (chip < last)),
        (remote(mall.at[b_l, :, low], mall.at[b_l, :, low], mo_s.at[1], mo_r.at[1], dev_r),
         has_l & (chip < last) & (right < last)),
    ]
    m_relay_r = [
        (remote(mall.at[b_r, :, top], mall.at[b_r, :, top], mo_s.at[2], mo_r.at[0], dev_l),
         has_r & (chip < last) & (left < last)),
        (remote(mall.at[b_r, :, low], mall.at[b_r, :, low], mo_s.at[3], mo_r.at[1], dev_l), has_r & (chip < last)),
    ]
    m_halves = [
        remote(mall.at[b_o, :, top], mall.at[b_o, :, top], mo_s.at[0], mo_r.at[0], dev_r),
        remote(mall.at[b_o, :, low], mall.at[b_o, :, low], mo_s.at[1], mo_r.at[1], dev_r),
    ]
    m_fwd = [
        remote(mall.at[b_l], mall.at[b_l], md_s.at[1], md_r.at[1], partner),
        remote(mall.at[b_r], mall.at[b_r], md_s.at[2], md_r.at[2], partner),
        remote(mall.at[b_o, :, top], mall.at[b_o, :, top], md_s.at[3], md_r.at[3], partner),
        remote(mall.at[b_o, :, low], mall.at[b_o, :, low], md_s.at[4], md_r.at[4], partner),
    ]
    m_has = (has_l, has_r, has_o, has_o)

    def start_rows(layer):
        ring, _, own = row_copies(layer)
        own.start()
        when_start(sent[0], ring[0])
        when_start(sent[1], ring[1])

    y_give[0] = y[keep:]
    start_rows(0)
    give_y(0)
    for copy in first[1:]:
        copy.wait()

    @pl.when(has_m)
    def _():
        for i in range(n_layers):
            mkv[i, :, :kv_dim] = dot(mem[...], ck[i]).astype(BF16)
            mkv[i, :, kv_dim:] = dot(mem[...], cv[i]).astype(BF16)
        mall[b_me] = mkv[...]
    def from_left():
        when_recv(has_l, m_own[0])
        when_start(has_l, m_fwd[0])
        for copy, cond in m_relay_l:
            when_start(cond, copy)

    def from_right():
        when_recv(has_r, m_own[1])
        when_start(has_r, m_fwd[1])
        for copy, cond in m_relay_r:
            when_start(cond, copy)

    qm[...] = jnp.zeros_like(qm)
    ones_row = (lax.broadcasted_iota(jnp.int32, (PAIR - HEAD_DIM, qc.shape[2]), 0) == 0).astype(F32).astype(BF16)
    for n in range(qc.shape[0]):
        qc[n, HEAD_DIM:] = ones_row
    when_start(has_m, m_own[2])
    when_start(has_m & (left < chip), m_own[1])

    def reset():
        m_ref[...] = jnp.full_like(m_ref, MASK_VALUE)
        l_ref[...] = jnp.zeros_like(l_ref)
        acc[...] = jnp.zeros_like(acc)

    def pipelined(count, item, scores, softmax, together=1):
        def place(i):
            k, v = (i // together) % 2, i % together
            return (b0, b1)[k].at[v], (mc0, mc1)[k].at[v]

        for i in range(-together, count, together):
            for j in range(i + together, min(i + 2 * together, count)):
                scores(item(j), *place(j))
            for j in range(max(i, 0), i + together):
                softmax(item(j), *place(j))

    def finish(n, m, first=0):
        span = slice(first, first + 2 * m)
        val = acc[n, :, span] * (1.0 / l_ref[n, :, span])
        return jnp.concatenate([val[:, :m], val[:, m:]], axis=0).astype(BF16).T

    def project_kv(pieces):
        size = CHUNK // len(pieces)
        for i, piece in enumerate(pieces):
            span = slice(i * size, (i + 1) * size)
            k_val = dot(piece, wk[...]).astype(BF16)
            v_val = dot(wvt[...], piece, NT).astype(BF16)
            for p in range(pairs):
                k_s[p, span] = k_val[:, p * PAIR:(p + 1) * PAIR]
                vt_s[p, :, span] = v_val[p * PAIR:(p + 1) * PAIR]

    def self_scores(pn, buf, mc, size=CHUNK, mask=None):
        p, n = pn
        col_scores(k_s[p, :size], qm[n], buf, size, mask, n, m_ref, mc)

    def self_softmax(pn, buf, mc, size=CHUNK):
        p, n = pn
        w = 2 * TILE
        e, alpha = col_softmax(buf, size, w, mc, n, m_ref, l_ref)
        acc[n, :, :TILE] = acc[n, :, :TILE] * alpha[:, :TILE] + dot(vt_s[p, :HEAD_DIM, :size], e[:, :TILE])
        acc[n, :, TILE:w] = acc[n, :, TILE:w] * alpha[:, TILE:] + dot(vt_s[p, HEAD_DIM:, :size], e[:, TILE:])

    def attend(first_tile, n_tiles):
        def item(i):
            p = i // n_tiles
            return p, p * tiles + first_tile + i % n_tiles

        pipelined(pairs * n_tiles, item, self_scores, self_softmax, GROUP)

    def rest_of_layer(layer, y_rows, o_rows, m):
        per = wide // (2 * m)
        w = 2 * m * per
        sets = all_pairs // per
        per_group = group // per
        m_ref[:sets, :, :w] = jnp.full((sets, 1, w), MASK_VALUE, F32)
        l_ref[:sets, :, :w] = jnp.zeros((sets, 1, w), F32)
        acc[:sets, :, :w] = jnp.zeros((sets, HEAD_DIM, w), F32)
        upd = dot(o_rows[0], wo[:width]) + dot(o_rows[1], wo[width:])
        y1 = (y_rows[...].astype(F32) + upd).astype(BF16)
        y_rows[...] = y1
        h = rms_norm(y1.astype(F32), gains[1, layer])
        q_val = (dot(h, cq[...]).astype(BF16) * ATT_SCALE).astype(BF16)
        for p in range(all_pairs):
            qt = q_val[:, p * PAIR:(p + 1) * PAIR].T
            n, at = p // per, (p % per) * 2 * m
            qc[n, :HEAD_DIM, at:at + m] = qt[:HEAD_DIM]
            qc[n, :HEAD_DIM, at + m:at + 2 * m] = qt[HEAD_DIM:]

        def item(i):
            c, n = i // sets, i % sets
            return pl.ds(c * CHUNK, CHUNK), n // per_group, n

        def scores(cgn, buf, mc):
            keys, g, n = cgn
            col_scores(k_c[g, keys], qc[n, :, :w], buf, CHUNK, None, n, m_ref, mc)

        def softmax(cgn, buf, mc):
            keys, g, n = cgn
            e, alpha = col_softmax(buf, CHUNK, w, mc, n, m_ref, l_ref)
            acc[n, :, :w] = acc[n, :, :w] * alpha + dot(vt_c[g, :, keys], e)

        count = sets * (used * mrows // CHUNK)
        pipelined(count, item, scores, softmax)
        o2 = act.at[:m, :d_model]
        for p in range(all_pairs):
            o2[:, p * PAIR:(p + 1) * PAIR] = finish(p // per, m, (p % per) * 2 * m)
        y2 = (y_rows[...].astype(F32) + dot(o2[...], co[...])).astype(BF16)
        y_rows[...] = y2
        h = rms_norm(y2.astype(F32), gains[2, layer])
        for c in range(0, ff, CHUNK):
            gate = dot(h, wg[:, c:c + CHUNK])
            act[:m, c:c + CHUNK] = (jax.nn.silu(gate) * dot(h, wu[:, c:c + CHUNK])).astype(BF16)
        y_rows[...] = (y_rows[...].astype(F32) + dot(act[:m], wd[...])).astype(BF16)

    def prepare(layer):
        for copy in loads(layer)[:3]:
            copy.wait()
        wqt[...] = wq[...].T
        wvt[...] = wv[...].T
        reset()

    def layer_body(layer, carry):
        ring, fwd, own = row_copies(layer)
        weights = loads(layer)
        def own_block(i, inner):
            block = jnp.where(i == 0, core, other)

            @pl.when(i == 1)
            def _():
                own.wait_recv()

            h_blk = h_own[layer, pl.ds(pl.multiple_of(block * rows, rows), rows)]
            q_val = (dot(wqt[...], h_blk, NT).astype(BF16) * ATT_SCALE).astype(BF16)
            for p in range(pairs):
                for t in range(row_tiles):
                    n = p * tiles + block * row_tiles + t
                    span = slice(t * TILE, (t + 1) * TILE)
                    qm[n, :HEAD_DIM, :TILE] = q_val[p * PAIR:p * PAIR + HEAD_DIM, span]
                    qm[n, HEAD_DIM:, TILE:] = q_val[p * PAIR + HEAD_DIM:(p + 1) * PAIR, span]
            return inner

        lax.fori_loop(0, 2, own_block, 0)

        def own_keys(block, inner):
            project_kv([h_own[layer, pl.ds(pl.multiple_of(block * rows, rows), rows)]])
            key = lax.broadcasted_iota(jnp.int32, (CHUNK, 2 * TILE), 0)
            query = lax.broadcasted_iota(jnp.int32, (CHUNK, 2 * TILE), 1) % TILE

            order = [(p, t) for p in range(pairs) for t in range(row_tiles)]
            masks = (key[:TILE] <= query[:TILE], key <= query + TILE)

            def diagonal(j, step):
                p, t = order[j]
                step((p, p * tiles + block * row_tiles + t), (b0, b1)[j % 2].at[0], (mc0, mc1)[j % 2].at[0], t)

            def diagonal_scores(pn, buf, mc, t):
                self_scores(pn, buf, mc, (t + 1) * TILE, masks[t])

            def diagonal_softmax(pn, buf, mc, t):
                self_softmax(pn, buf, mc, (t + 1) * TILE)

            diagonal(0, diagonal_scores)
            for j in range(len(order)):
                if j + 1 < len(order):
                    diagonal(j + 1, diagonal_scores)
                diagonal(j, diagonal_softmax)

            @pl.when(block == 0)
            def _():
                attend(tiles // 2, tiles // 2)
                when_start(sent[2], ring[2])
                when_start(sent[3], ring[3])

            return inner

        lax.fori_loop(0, 2, own_keys, 0)

        def take(i):
            when_recv(got[i], ring[i])
            if i == 0:
                when_start(relay_a, ring[4])
            if i == 1:
                when_start(relay_b, ring[5])
            when_start(need[i], fwd[i])

        def attend_two(stage, inner):
            @pl.when(stage == 0)
            def _():
                take(0)
                take(1)

                @pl.when(layer == 0)
                def _():
                    when_start(has_m, m_own[0])
                    when_start(has_m & (left > chip), m_own[1])

                    @pl.when(chip < last)
                    def _():
                        from_right()


            @pl.when(stage == 1)
            def _():
                take(2)
                take(3)

            @pl.when(stage == 2)
            def _():
                take(4)
                take(5)

            any_need = jnp.where(stage == 2, opp, left) < chip
            both = jnp.where(stage == 2, opp, right) < chip

            def one(i, deep):
                @pl.when(i == 1)
                def _():
                    for j in range(3):
                        @pl.when(stage == j)
                        def _(j=j):
                            when_recv(need[2 * j], fwd[2 * j])
                            when_recv(need[2 * j + 1], fwd[2 * j + 1])

                @pl.when((stage == 2) & (i == 1) & (layer == 0))
                def _():
                    from_left()

                    @pl.when(chip == last)
                    def _():
                        from_right()

                @pl.when(any_need & ((i == 1) | both))
                def _():
                    from_a = jnp.where((i == 1) & both, other, core)
                    from_b = jnp.where(i == 1, other, core)
                    slot_b = jnp.where(both, 2 * stage + 1, 2 * stage)
                    project_kv([h_rem[layer, 2 * stage, from_a], h_rem[layer, slot_b, from_b]])
                    attend(0, tiles)

                return deep

            return lax.fori_loop(0, 2, one, inner)

        lax.fori_loop(0, 3, attend_two, 0)

        for t in reversed(range(row_tiles)):
            span = slice(t * TILE, (t + 1) * TILE)
            for p in range(pairs):
                o_stage[layer, span, p * PAIR:(p + 1) * PAIR] = finish(p * tiles + other * row_tiles + t, TILE)
            for p in range(pairs):
                if t == 0 and p == 1:
                    for copy in give_copies(layer)[2:]:
                        when_start(gives, copy)
                o_full[layer, core, span, p * PAIR:(p + 1) * PAIR] = finish(p * tiles + core * row_tiles + t, TILE)
        o_send = remote(o_stage.at[layer], o_full.at[layer, core], o_sem.at[layer, 0], o_sem.at[layer, 1], partner)
        o_send.start()

        @pl.when(layer + 1 < n_layers)
        def _():
            for copy in loads(layer + 1)[:3]:
                copy.start()

        @pl.when(layer == 0)
        def _():
            when_recv(has_o, m_halves[0])
            when_start(has_o, m_fwd[2])
            when_recv(has_o, m_halves[1])
            when_start(has_o, m_fwd[3])
            when_recv(has_m, m_own[2])
            for cond, copy in zip(m_has, m_fwd):
                when_recv(cond, copy)

        mem_len = len_ref[0]
        for b in range(used):
            span = slice(b * mrows, (b + 1) * mrows)
            vt = mall[b, layer, :, kv_dim:].T
            pos = lax.broadcasted_iota(jnp.int32, (mrows, HEAD_DIM), 0) + b * mrows
            lane = lax.broadcasted_iota(jnp.int32, (mrows, HEAD_DIM), 1)
            bias = jnp.where((pos >= mem_len) & (lane == 0), MASK_VALUE, 0.0).astype(BF16)
            for g in range(n_kv):
                k_c[g, span, :HEAD_DIM] = mall[b, layer, :, g * HEAD_DIM:(g + 1) * HEAD_DIM]
                k_c[g, span, HEAD_DIM:] = bias
                vt_c[g, :, span] = vt[g * HEAD_DIM:(g + 1) * HEAD_DIM]

        o_send.wait_recv()
        y_copy, back_copy = give_copies(layer)[:2]
        for copy in weights[3:]:
            copy.wait()
        rest_of_layer(layer, y.at[:keep], o_full.at[layer, :, pl.ds(0, keep)], keep)

        def next_rows(span):
            h_own[layer + 1, pl.ds(core * rows + span.start, span.stop - span.start)] = rms_norm(
                y[span].astype(F32), gains[0, layer + 1])

        @pl.when(layer + 1 < n_layers)
        def _():
            next_rows(slice(0, keep))

        def next_start():
            @pl.when(layer + 1 < n_layers)
            def _():
                next_rows(slice(keep, rows))
                y_give[layer + 1] = y[keep:]
                start_rows(layer + 1)
                give_y(layer + 1)

        def handed(i, inner):
            @pl.when(i == 0)
            def _():
                y_back[layer] = y[keep:]
                o_part[...] = o_full[layer, :, keep:]

            @pl.when(i == 1)
            def _():
                y_copy.wait_recv()
                for copy in take_copies(layer):
                    copy.wait_recv()
                y_back[layer] = y_take[layer]
                o_part[...] = o_take[layer]

            rest_of_layer(layer, y_back.at[layer], o_part, HANDED)

            @pl.when(i == 0)
            def _():
                y[keep:] = y_back[layer]
                next_start()

            return inner

        @pl.when(jnp.logical_not(gives))
        def _():
            lax.fori_loop(0, jnp.where(takes, 2, 1), handed, 0)

        @pl.when(takes)
        def _():
            back_copy.start()

        @pl.when(layer + 1 < n_layers)
        def _():
            prepare(layer + 1)

        @pl.when(gives)
        def _():
            back_copy.wait_recv()
            y[keep:] = y_done[layer]
            next_start()

        @pl.when(layer + 1 < n_layers)
        def _():
            for copy in loads(layer + 1)[3:]:
                copy.start()

        return carry

    prepare(0)
    lax.fori_loop(0, n_layers, layer_body, 0)
    out_ref[...] = y[...]

    for copy in m_own:
        when_sent(has_m, copy)
    for copy, cond in (*m_relay_l, *m_relay_r):
        when_sent(cond, copy)
    for cond, copy in zip(m_has, m_fwd):
        when_sent(cond, copy)

    def sent_all(layer, carry):
        ring, fwd, own = row_copies(layer)
        y_copy, back_copy, *o_copies = give_copies(layer)
        own.wait_send()
        remote(o_stage.at[layer], o_full.at[layer, core], o_sem.at[layer, 0], o_sem.at[layer, 1], partner).wait_send()
        for cond, copy in zip((*sent, relay_a, relay_b), ring):
            when_sent(cond, copy)
        for cond, copy in zip(need, fwd):
            when_sent(cond, copy)
        when_sent(gives, y_copy)
        for copy in o_copies:
            when_sent(gives, copy)
        when_sent(takes, back_copy)
        return carry

    lax.fori_loop(0, n_layers, sent_all, 0)


def layers_call(n_sp, mem_len, hidden, memory, gain_self, gain_cross, gain_mlp, self_q, self_k, self_v, self_o, cross_q,
                cross_k, cross_v, cross_o, gate, up, down):
    rows, d_model = hidden.shape
    layers = gain_self.shape[0]
    width = d_model // 2
    ff = gate.shape[2]
    mrows, mcols = memory.shape[0], 2 * cross_k.shape[2]
    used = min(n_sp, pl.cdiv(MAX_MEM_LEN, mrows))
    n_kv = cross_k.shape[2] // HEAD_DIM
    pairs, tiles = width // PAIR, 2 * rows // TILE
    combos = pairs * tiles
    wide = 2 * (rows - HANDED)
    dma = pltpu.SemaphoreType.DMA
    return pl.pallas_call(
        functools.partial(layer_kernel, n_sp, layers),
        out_shape=jax.ShapeDtypeStruct((rows, d_model), BF16),
        in_specs=[SMEM, ANY, ANY, VMEM, VMEM, VMEM] + [ANY] * 11,
        out_specs=VMEM,
        scratch_shapes=[
            pltpu.VMEM((rows, d_model), BF16),
            pltpu.VMEM((layers, 2 * rows, d_model), BF16),
            pltpu.VMEM((layers, 6, 2, rows // 2, d_model), BF16),
            pltpu.VMEM((mrows, d_model), BF16),
            *[pltpu.VMEM(cross_k.shape, BF16)] * 2,
            pltpu.VMEM((layers, mrows, mcols), BF16),
            pltpu.VMEM((used, layers, mrows, mcols), BF16),
            *[pltpu.VMEM((d_model, width), BF16)] * 3,
            *[pltpu.VMEM((width, d_model), BF16)] * 2,
            *[pltpu.VMEM((d_model, d_model), BF16)] * 3,
            *[pltpu.VMEM((d_model, ff), BF16)] * 2,
            pltpu.VMEM((ff, d_model), BF16),
            pltpu.VMEM((combos, PAIR, 2 * TILE), BF16),
            pltpu.VMEM((2 * pairs, PAIR, wide), BF16),
            pltpu.VMEM((pairs, CHUNK, PAIR), BF16),
            pltpu.VMEM((pairs, PAIR, CHUNK), BF16),
            pltpu.VMEM((n_kv, used * mrows, PAIR), BF16),
            pltpu.VMEM((n_kv, HEAD_DIM, used * mrows), BF16),
            *[pltpu.VMEM((combos, 1, wide), F32)] * 2,
            pltpu.VMEM((combos, HEAD_DIM, wide), F32),
            *[pltpu.VMEM((GROUP, CHUNK, wide), F32)] * 2,
            *[pltpu.VMEM((GROUP, 1, wide), F32)] * 2,
            pltpu.VMEM((layers, rows, width), BF16),
            pltpu.VMEM((layers, 2, rows, width), BF16),
            pltpu.VMEM((rows, ff), BF16),
            pltpu.VMEM((3, layers, 1, d_model), F32),
            *[pltpu.VMEM((layers, HANDED, d_model), BF16)] * 2,
            pltpu.VMEM((layers, 2, HANDED, width), BF16),
            *[pltpu.VMEM((layers, HANDED, d_model), BF16)] * 2,
            pltpu.VMEM((2, HANDED, width), BF16),
            dma((13,)), dma((layers, 2)), *[dma((layers, 6))] * 4,
            *[dma((2,))] * 2, dma((4,)), dma((2,)), *[dma((5,))] * 2, dma((layers, 2)), *[dma((layers, 4))] * 2,
        ],
        compiler_params=pltpu.CompilerParams(collective_id=0, has_side_effects=True, vmem_limit_bytes=VMEM_LIMIT),
        name="layers",
    )(mem_len, hidden, memory, gain_self, gain_cross, gain_mlp, self_q, self_k, self_v, self_o, cross_q, cross_k, cross_v,
      cross_o, gate, up, down)


def solution(mesh):
    n_sp = mesh.shape["sp"]
    row_spec = P(("dp", "sp"), None)

    def device_fn(dec_hidden, memory, mem_len, *weights):
        return layers_call(n_sp, mem_len, dec_hidden, memory, *weights)

    return jax.shard_map(device_fn, mesh=mesh, in_specs=(row_spec, row_spec, P("dp")) + (P(),) * 14,
                         out_specs=row_spec, check_vma=False)
```

```python
import functools

import jax
import jax.numpy as jnp
from jax import lax
from jax.experimental import pallas as pl
from jax.experimental.pallas import tpu as pltpu
from jax.sharding import PartitionSpec as P

HEAD_DIM = 64
NORM_EPS = 1e-6
MASK_VALUE = -1e30
ATT_SCALE = HEAD_DIM ** -0.5
MAX_MEM_LEN = 1536
HANDED = 128
GROUP = 1
PAIR = 2 * HEAD_DIM
TILE = 256
CHUNK = 512
NN = (((1,), (0,)), ((), ()))
NT = (((1,), (1,)), ((), ()))
F32 = jnp.float32
BF16 = jnp.bfloat16
MESH = pl.DeviceIdType.MESH
VMEM_LIMIT = 52 * 1024 * 1024
HBM = pl.BlockSpec(memory_space=pltpu.HBM)
VMEM = pl.BlockSpec(memory_space=pltpu.VMEM)
SMEM = pl.BlockSpec(memory_space=pltpu.SMEM)


def rms_norm(val32, gain_row):
    inv_rms = lax.rsqrt(jnp.mean(val32 * val32, axis=-1, keepdims=True) + NORM_EPS)
    return (val32 * inv_rms * gain_row).astype(BF16)


def dot(lhs, rhs, dims=NN):
    return lax.dot_general(lhs, rhs, dims, preferred_element_type=F32)


def col_scores(k_val, q_val, buf, size, mask, n, m_ref, mc):
    width = q_val.shape[1]
    s = dot(k_val, q_val)
    if mask is not None:
        s = jnp.where(mask, s, MASK_VALUE)
    buf[:size, :width] = s
    mc[:, :width] = jnp.maximum(m_ref[n, :, :width], jnp.max(s, axis=0, keepdims=True))


def col_softmax(buf, size, width, mc, n, m_ref, l_ref):
    m_new = mc[:, :width]
    alpha = jnp.exp(m_ref[n, :, :width] - m_new)
    e = jnp.exp(buf[:size, :width] - m_new)
    l_ref[n, :, :width] = l_ref[n, :, :width] * alpha + jnp.sum(e, axis=0, keepdims=True)
    m_ref[n, :, :width] = m_new
    return e.astype(BF16), alpha


def layer_kernel(n_sp, n_layers, len_ref, hid_hbm, mem_hbm, gain_s, gain_c, gain_m, wq_hbm, wk_hbm, wv_hbm, wo_hbm, cq_hbm,
                 ck_hbm, cv_hbm, co_hbm, wg_hbm, wu_hbm, wd_hbm, out_ref,
                 y, h_own, h_rem, mem, ck, cv, mkv, mall, wq, wk, wv, wqt, wvt, wo, cq, co, wg, wu, wd,
                 qm, qc, k_s, vt_s, k_c, vt_c, m_ref, l_ref, acc, b0, b1, mc0, mc1, o_stage, o_full, act, gains, gain_in,
                 y_give, y_take, o_take, y_back, y_done, o_part,
                 w_sem, own_sem, ici_s, ici_r, d2d_s, d2d_r, mi_s, mi_r, mo_s, mo_r, md_s, md_r, o_sem,
                 give_s, give_r):
    rows, d_model = y.shape
    half = rows // 2
    width = d_model // 2
    pairs = width // PAIR
    tiles = 2 * rows // TILE
    row_tiles = rows // TILE
    all_pairs = d_model // PAIR
    used, _, mrows, mcols = mall.shape
    mh = mrows // 2
    kv_dim = mcols // 2
    n_kv = kv_dim // HEAD_DIM
    group = all_pairs // n_kv
    ff = act.shape[1]
    n_chip = n_sp // 2
    me = lax.axis_index("sp")
    chip, core = me // 2, lax.rem(me, 2)
    other = 1 - core
    right, left = lax.rem(chip + 1, n_chip), lax.rem(chip + n_chip - 1, n_chip)
    opp = lax.rem(chip + 2, n_chip)
    partner = 2 * chip + other
    dev_r, dev_l = 2 * right + core, 2 * left + core
    last = n_chip - 1
    gives, takes = chip == last, chip == 0
    mate = 2 * (n_chip - 1 - chip) + core
    mate_other = 2 * (n_chip - 1 - chip) + other
    keep = rows - HANDED
    wide = 2 * keep

    def remote(src, dst, send, recv, dev):
        return pltpu.make_async_remote_copy(
            src_ref=src, dst_ref=dst, send_sem=send, recv_sem=recv, device_id={"sp": dev}, device_id_type=MESH)

    cols = pl.ds(pl.multiple_of(core * width, 128), width)
    own_rows = pl.ds(pl.multiple_of(core * rows, rows), rows)
    other_rows = pl.ds(pl.multiple_of(other * rows, rows), rows)

    def loads(layer):
        specs = [(wq_hbm.at[layer, :, cols], wq), (wk_hbm.at[layer, :, cols], wk), (wv_hbm.at[layer, :, cols], wv),
                 (wo_hbm.at[layer], wo), (cq_hbm.at[layer], cq), (co_hbm.at[layer], co), (wg_hbm.at[layer], wg),
                 (wu_hbm.at[layer], wu), (wd_hbm.at[layer], wd)]
        return [pltpu.make_async_copy(src, dst, w_sem.at[i]) for i, (src, dst) in enumerate(specs)]

    first = [pltpu.make_async_copy(src, dst, w_sem.at[9 + i])
             for i, (src, dst) in enumerate(((hid_hbm, y), (mem_hbm, mem), (ck_hbm, ck), (cv_hbm, cv)))]
    first[0].start()
    gain_loads = [pltpu.make_async_copy(src, gain_in.at[i], w_sem.at[13 + i]) for i, src in enumerate((gain_s, gain_c, gain_m))]
    for copy in gain_loads:
        copy.start()
    w_first = loads(0)
    for copy in (*w_first[:3], *first[1:], *w_first[3:]):
        copy.start()

    barrier = pltpu.get_barrier_semaphore()
    for dev in (dev_r, dev_l, partner, mate_other):
        pl.semaphore_signal(barrier, inc=1, device_id={"sp": dev}, device_id_type=MESH)

    for copy in gain_loads:
        copy.wait()
    for i in range(3):
        for j in range(n_layers):
            gains[i, j] = gain_in[i, j:j + 1].astype(F32)

    first[0].wait()
    h_own[0, own_rows] = rms_norm(y[...].astype(F32), gains[0, 0])
    pl.semaphore_wait(barrier, 4)

    to_r, to_l = chip < right, chip < left
    b_to_l = to_l | (chip < opp)
    relay_a, relay_b = left < right, right < left
    need_l, need_r, need_o = left < chip, right < chip, opp < chip
    got_rb = need_r | relay_b
    need = (need_l, need_r, need_l, need_r, need_o, need_o)
    got = (need_l, got_rb, need_l, need_r, need_o, need_o)
    sent = (to_r, b_to_l, to_r, to_l)

    def row_copies(layer):
        own_a = h_own.at[layer, pl.ds(pl.multiple_of(core * rows, half), half)]
        own_b = h_own.at[layer, pl.ds(pl.multiple_of(core * rows + half, half), half)]
        slot = [h_rem.at[layer, i, core] for i in range(6)]
        srcs = (own_a, own_b, own_b, own_a, slot[0], slot[1])
        ring = [remote(srcs[i], slot[i], ici_s.at[layer, i], ici_r.at[layer, i], dev_l if i % 2 else dev_r)
                for i in (0, 1)]
        ring += [remote(srcs[2], slot[2], ici_s.at[layer, 2], ici_r.at[layer, 2], dev_r),
                 remote(srcs[3], slot[3], ici_s.at[layer, 3], ici_r.at[layer, 3], dev_l),
                 remote(srcs[4], slot[4], ici_s.at[layer, 4], ici_r.at[layer, 4], dev_r),
                 remote(srcs[5], slot[5], ici_s.at[layer, 5], ici_r.at[layer, 5], dev_l)]
        fwd = [remote(slot[i], slot[i], d2d_s.at[layer, i], d2d_r.at[layer, i], partner) for i in range(6)]
        own = remote(h_own.at[layer, own_rows], h_own.at[layer, own_rows], own_sem.at[layer, 0], own_sem.at[layer, 1],
                     partner)
        return ring, fwd, own

    def give_copies(layer):
        handed_rows = pl.ds(keep, HANDED)
        return [remote(y_give.at[layer], y_take.at[layer], give_s.at[layer, 0], give_r.at[layer, 0], mate),
                remote(y_back.at[layer], y_done.at[layer], give_s.at[layer, 1], give_r.at[layer, 1], mate),
                remote(o_full.at[layer, core, handed_rows], o_take.at[layer, core], give_s.at[layer, 2],
                       give_r.at[layer, 2 + core], mate),
                remote(o_stage.at[layer, handed_rows], o_take.at[layer, core], give_s.at[layer, 3],
                       give_r.at[layer, 2 + core], mate_other)]

    def take_copies(layer):
        rows_of = o_full.at[layer, core, pl.ds(keep, HANDED)]
        return [remote(rows_of, o_take.at[layer, j], give_s.at[layer, 2], give_r.at[layer, 2 + j], mate)
                for j in range(2)]

    def give_y(layer):
        @pl.when(gives)
        def _():
            give_copies(layer)[0].start()

    def when_start(cond, copy):
        @pl.when(cond)
        def _():
            copy.start()

    def when_sent(cond, copy):
        @pl.when(cond)
        def _():
            copy.wait_send()

    def when_recv(cond, copy):
        @pl.when(cond)
        def _():
            copy.wait_recv()

    has_m = 2 * chip < used
    has_l, has_r, has_o = 2 * left < used, 2 * right < used, 2 * opp < used

    def blk(who, core_of):
        return jnp.minimum(2 * who + core_of, used - 1)

    b_me, b_l, b_r, b_o = blk(chip, core), blk(left, core), blk(right, core), blk(opp, core)
    top, low = pl.ds(0, mh), pl.ds(mh, mh)
    m_own = [
        remote(mkv, mall.at[b_me], mi_s.at[0], mi_r.at[0], dev_r),
        remote(mkv, mall.at[b_me], mi_s.at[1], mi_r.at[1], dev_l),
        remote(mkv, mall.at[b_me], md_s.at[0], md_r.at[0], partner),
    ]
    m_relay_l = [
        (remote(mall.at[b_l, :, top], mall.at[b_l, :, top], mo_s.at[0], mo_r.at[0], dev_r), has_l & (chip < last)),
        (remote(mall.at[b_l, :, low], mall.at[b_l, :, low], mo_s.at[1], mo_r.at[1], dev_r),
         has_l & (chip < last) & (right < last)),
    ]
    m_relay_r = [
        (remote(mall.at[b_r, :, top], mall.at[b_r, :, top], mo_s.at[2], mo_r.at[0], dev_l),
         has_r & (chip < last) & (left < last)),
        (remote(mall.at[b_r, :, low], mall.at[b_r, :, low], mo_s.at[3], mo_r.at[1], dev_l), has_r & (chip < last)),
    ]
    m_halves = [
        remote(mall.at[b_o, :, top], mall.at[b_o, :, top], mo_s.at[0], mo_r.at[0], dev_r),
        remote(mall.at[b_o, :, low], mall.at[b_o, :, low], mo_s.at[1], mo_r.at[1], dev_r),
    ]
    m_fwd = [
        remote(mall.at[b_l], mall.at[b_l], md_s.at[1], md_r.at[1], partner),
        remote(mall.at[b_r], mall.at[b_r], md_s.at[2], md_r.at[2], partner),
        remote(mall.at[b_o, :, top], mall.at[b_o, :, top], md_s.at[3], md_r.at[3], partner),
        remote(mall.at[b_o, :, low], mall.at[b_o, :, low], md_s.at[4], md_r.at[4], partner),
    ]
    m_has = (has_l, has_r, has_o, has_o)

    def start_rows(layer):
        ring, _, own = row_copies(layer)
        own.start()
        when_start(sent[0], ring[0])
        when_start(sent[1], ring[1])

    y_give[0] = y[keep:]
    start_rows(0)
    give_y(0)
    for copy in first[1:]:
        copy.wait()

    @pl.when(has_m)
    def _():
        for i in range(n_layers):
            mkv[i, :, :kv_dim] = dot(mem[...], ck[i]).astype(BF16)
            mkv[i, :, kv_dim:] = dot(mem[...], cv[i]).astype(BF16)
        mall[b_me] = mkv[...]
    def from_left():
        when_recv(has_l, m_own[0])
        when_start(has_l, m_fwd[0])
        for copy, cond in m_relay_l:
            when_start(cond, copy)

    def from_right():
        when_recv(has_r, m_own[1])
        when_start(has_r, m_fwd[1])
        for copy, cond in m_relay_r:
            when_start(cond, copy)

    qm[...] = jnp.zeros_like(qm)
    ones_row = (lax.broadcasted_iota(jnp.int32, (PAIR - HEAD_DIM, qc.shape[2]), 0) == 0).astype(F32).astype(BF16)
    for n in range(qc.shape[0]):
        qc[n, HEAD_DIM:] = ones_row
    when_start(has_m, m_own[2])
    when_start(has_m & (left < chip), m_own[1])

    def reset():
        m_ref[...] = jnp.full_like(m_ref, MASK_VALUE)
        l_ref[...] = jnp.zeros_like(l_ref)
        acc[...] = jnp.zeros_like(acc)

    def pipelined(count, item, scores, softmax, together=1):
        def place(i):
            k, v = (i // together) % 2, i % together
            return (b0, b1)[k].at[v], (mc0, mc1)[k].at[v]

        for i in range(-together, count, together):
            for j in range(i + together, min(i + 2 * together, count)):
                scores(item(j), *place(j))
            for j in range(max(i, 0), i + together):
                softmax(item(j), *place(j))

    def finish(n, m, first=0):
        span = slice(first, first + 2 * m)
        val = acc[n, :, span] * (1.0 / l_ref[n, :, span])
        return jnp.concatenate([val[:, :m], val[:, m:]], axis=0).astype(BF16).T

    def project_kv(pieces):
        size = CHUNK // len(pieces)
        for i, piece in enumerate(pieces):
            span = slice(i * size, (i + 1) * size)
            k_val = dot(piece, wk[...]).astype(BF16)
            v_val = dot(wvt[...], piece, NT).astype(BF16)
            for p in range(pairs):
                k_s[p, span] = k_val[:, p * PAIR:(p + 1) * PAIR]
                vt_s[p, :, span] = v_val[p * PAIR:(p + 1) * PAIR]

    def self_scores(pn, buf, mc, size=CHUNK, mask=None):
        p, n = pn
        col_scores(k_s[p, :size], qm[n], buf, size, mask, n, m_ref, mc)

    def self_softmax(pn, buf, mc, size=CHUNK):
        p, n = pn
        w = 2 * TILE
        e, alpha = col_softmax(buf, size, w, mc, n, m_ref, l_ref)
        acc[n, :, :TILE] = acc[n, :, :TILE] * alpha[:, :TILE] + dot(vt_s[p, :HEAD_DIM, :size], e[:, :TILE])
        acc[n, :, TILE:w] = acc[n, :, TILE:w] * alpha[:, TILE:] + dot(vt_s[p, HEAD_DIM:, :size], e[:, TILE:])

    def attend(first_tile, n_tiles):
        def item(i):
            p = i // n_tiles
            return p, p * tiles + first_tile + i % n_tiles

        pipelined(pairs * n_tiles, item, self_scores, self_softmax, GROUP)

    def rest_of_layer(layer, y_rows, o_rows, m):
        per = wide // (2 * m)
        w = 2 * m * per
        sets = all_pairs // per
        per_group = group // per
        m_ref[:sets, :, :w] = jnp.full((sets, 1, w), MASK_VALUE, F32)
        l_ref[:sets, :, :w] = jnp.zeros((sets, 1, w), F32)
        acc[:sets, :, :w] = jnp.zeros((sets, HEAD_DIM, w), F32)
        upd = dot(o_rows[0], wo[:width]) + dot(o_rows[1], wo[width:])
        y1 = (y_rows[...].astype(F32) + upd).astype(BF16)
        y_rows[...] = y1
        h = rms_norm(y1.astype(F32), gains[1, layer])
        q_val = (dot(h, cq[...]).astype(BF16) * ATT_SCALE).astype(BF16)
        for p in range(all_pairs):
            qt = q_val[:, p * PAIR:(p + 1) * PAIR].T
            n, at = p // per, (p % per) * 2 * m
            qc[n, :HEAD_DIM, at:at + m] = qt[:HEAD_DIM]
            qc[n, :HEAD_DIM, at + m:at + 2 * m] = qt[HEAD_DIM:]

        def item(i):
            c, n = i // sets, i % sets
            return pl.ds(c * CHUNK, CHUNK), n // per_group, n

        def scores(cgn, buf, mc):
            keys, g, n = cgn
            col_scores(k_c[g, keys], qc[n, :, :w], buf, CHUNK, None, n, m_ref, mc)

        def softmax(cgn, buf, mc):
            keys, g, n = cgn
            e, alpha = col_softmax(buf, CHUNK, w, mc, n, m_ref, l_ref)
            acc[n, :, :w] = acc[n, :, :w] * alpha + dot(vt_c[g, :, keys], e)

        count = sets * (used * mrows // CHUNK)
        pipelined(count, item, scores, softmax)
        o2 = act.at[:m, :d_model]
        for p in range(all_pairs):
            o2[:, p * PAIR:(p + 1) * PAIR] = finish(p // per, m, (p % per) * 2 * m)
        y2 = (y_rows[...].astype(F32) + dot(o2[...], co[...])).astype(BF16)
        y_rows[...] = y2
        h = rms_norm(y2.astype(F32), gains[2, layer])
        for c in range(0, ff, CHUNK):
            gate = dot(h, wg[:, c:c + CHUNK])
            act[:m, c:c + CHUNK] = (jax.nn.silu(gate) * dot(h, wu[:, c:c + CHUNK])).astype(BF16)
        y_rows[...] = (y_rows[...].astype(F32) + dot(act[:m], wd[...])).astype(BF16)

    def prepare(layer):
        for copy in loads(layer)[:3]:
            copy.wait()
        wqt[...] = wq[...].T
        wvt[...] = wv[...].T
        reset()

    def layer_body(layer, carry):
        ring, fwd, own = row_copies(layer)
        weights = loads(layer)
        def own_block(i, inner):
            block = jnp.where(i == 0, core, other)

            @pl.when(i == 1)
            def _():
                own.wait_recv()

            h_blk = h_own[layer, pl.ds(pl.multiple_of(block * rows, rows), rows)]
            q_val = (dot(wqt[...], h_blk, NT).astype(BF16) * ATT_SCALE).astype(BF16)
            for p in range(pairs):
                for t in range(row_tiles):
                    n = p * tiles + block * row_tiles + t
                    span = slice(t * TILE, (t + 1) * TILE)
                    qm[n, :HEAD_DIM, :TILE] = q_val[p * PAIR:p * PAIR + HEAD_DIM, span]
                    qm[n, HEAD_DIM:, TILE:] = q_val[p * PAIR + HEAD_DIM:(p + 1) * PAIR, span]
            return inner

        lax.fori_loop(0, 2, own_block, 0)

        def own_keys(block, inner):
            project_kv([h_own[layer, pl.ds(pl.multiple_of(block * rows, rows), rows)]])
            key = lax.broadcasted_iota(jnp.int32, (CHUNK, 2 * TILE), 0)
            query = lax.broadcasted_iota(jnp.int32, (CHUNK, 2 * TILE), 1) % TILE

            order = [(p, t) for p in range(pairs) for t in range(row_tiles)]
            masks = (key[:TILE] <= query[:TILE], key <= query + TILE)

            def diagonal(j, step):
                p, t = order[j]
                step((p, p * tiles + block * row_tiles + t), (b0, b1)[j % 2].at[0], (mc0, mc1)[j % 2].at[0], t)

            def diagonal_scores(pn, buf, mc, t):
                self_scores(pn, buf, mc, (t + 1) * TILE, masks[t])

            def diagonal_softmax(pn, buf, mc, t):
                self_softmax(pn, buf, mc, (t + 1) * TILE)

            diagonal(0, diagonal_scores)
            for j in range(len(order)):
                if j + 1 < len(order):
                    diagonal(j + 1, diagonal_scores)
                diagonal(j, diagonal_softmax)

            @pl.when(block == 0)
            def _():
                attend(tiles // 2, tiles // 2)
                when_start(sent[2], ring[2])
                when_start(sent[3], ring[3])

            return inner

        lax.fori_loop(0, 2, own_keys, 0)

        def take(i):
            when_recv(got[i], ring[i])
            if i == 0:
                when_start(relay_a, ring[4])
            if i == 1:
                when_start(relay_b, ring[5])
            when_start(need[i], fwd[i])

        def attend_two(stage, inner):
            @pl.when(stage == 0)
            def _():
                take(0)
                take(1)

                @pl.when(layer == 0)
                def _():
                    when_start(has_m, m_own[0])
                    when_start(has_m & (left > chip), m_own[1])

                    @pl.when(chip < last)
                    def _():
                        from_right()


            @pl.when(stage == 1)
            def _():
                take(2)
                take(3)

            @pl.when(stage == 2)
            def _():
                take(4)
                take(5)

            any_need = jnp.where(stage == 2, opp, left) < chip
            both = jnp.where(stage == 2, opp, right) < chip

            def one(i, deep):
                @pl.when(i == 1)
                def _():
                    for j in range(3):
                        @pl.when(stage == j)
                        def _(j=j):
                            when_recv(need[2 * j], fwd[2 * j])
                            when_recv(need[2 * j + 1], fwd[2 * j + 1])

                @pl.when((stage == 2) & (i == 1) & (layer == 0))
                def _():
                    from_left()

                    @pl.when(chip == last)
                    def _():
                        from_right()

                @pl.when(any_need & ((i == 1) | both))
                def _():
                    from_a = jnp.where((i == 1) & both, other, core)
                    from_b = jnp.where(i == 1, other, core)
                    slot_b = jnp.where(both, 2 * stage + 1, 2 * stage)
                    project_kv([h_rem[layer, 2 * stage, from_a], h_rem[layer, slot_b, from_b]])
                    attend(0, tiles)

                return deep

            return lax.fori_loop(0, 2, one, inner)

        lax.fori_loop(0, 3, attend_two, 0)

        for t in reversed(range(row_tiles)):
            span = slice(t * TILE, (t + 1) * TILE)
            for p in range(pairs):
                o_stage[layer, span, p * PAIR:(p + 1) * PAIR] = finish(p * tiles + other * row_tiles + t, TILE)
            for p in range(pairs):
                if t == 0 and p == 1:
                    for copy in give_copies(layer)[2:]:
                        when_start(gives, copy)
                o_full[layer, core, span, p * PAIR:(p + 1) * PAIR] = finish(p * tiles + core * row_tiles + t, TILE)
        o_send = remote(o_stage.at[layer], o_full.at[layer, core], o_sem.at[layer, 0], o_sem.at[layer, 1], partner)
        o_send.start()

        @pl.when(layer + 1 < n_layers)
        def _():
            for copy in loads(layer + 1)[:3]:
                copy.start()

        @pl.when(layer == 0)
        def _():
            when_recv(has_o, m_halves[0])
            when_start(has_o, m_fwd[2])
            when_recv(has_o, m_halves[1])
            when_start(has_o, m_fwd[3])
            when_recv(has_m, m_own[2])
            for cond, copy in zip(m_has, m_fwd):
                when_recv(cond, copy)

        mem_len = len_ref[0]
        for b in range(used):
            span = slice(b * mrows, (b + 1) * mrows)
            vt = mall[b, layer, :, kv_dim:].T
            pos = lax.broadcasted_iota(jnp.int32, (mrows, HEAD_DIM), 0) + b * mrows
            lane = lax.broadcasted_iota(jnp.int32, (mrows, HEAD_DIM), 1)
            bias = jnp.where((pos >= mem_len) & (lane == 0), MASK_VALUE, 0.0).astype(BF16)
            for g in range(n_kv):
                k_c[g, span, :HEAD_DIM] = mall[b, layer, :, g * HEAD_DIM:(g + 1) * HEAD_DIM]
                k_c[g, span, HEAD_DIM:] = bias
                vt_c[g, :, span] = vt[g * HEAD_DIM:(g + 1) * HEAD_DIM]

        o_send.wait_recv()
        y_copy, back_copy = give_copies(layer)[:2]
        for copy in weights[3:]:
            copy.wait()
        rest_of_layer(layer, y.at[:keep], o_full.at[layer, :, pl.ds(0, keep)], keep)

        def next_rows(span):
            h_own[layer + 1, pl.ds(core * rows + span.start, span.stop - span.start)] = rms_norm(
                y[span].astype(F32), gains[0, layer + 1])

        @pl.when(layer + 1 < n_layers)
        def _():
            next_rows(slice(0, keep))

        def next_start():
            @pl.when(layer + 1 < n_layers)
            def _():
                next_rows(slice(keep, rows))
                y_give[layer + 1] = y[keep:]
                start_rows(layer + 1)
                give_y(layer + 1)

        def handed(i, inner):
            @pl.when(i == 0)
            def _():
                y_back[layer] = y[keep:]
                o_part[...] = o_full[layer, :, keep:]

            @pl.when(i == 1)
            def _():
                y_copy.wait_recv()
                for copy in take_copies(layer):
                    copy.wait_recv()
                y_back[layer] = y_take[layer]
                o_part[...] = o_take[layer]

            rest_of_layer(layer, y_back.at[layer], o_part, HANDED)

            @pl.when(i == 0)
            def _():
                y[keep:] = y_back[layer]
                next_start()

            return inner

        @pl.when(jnp.logical_not(gives))
        def _():
            lax.fori_loop(0, jnp.where(takes, 2, 1), handed, 0)

        @pl.when(takes)
        def _():
            back_copy.start()

        @pl.when(layer + 1 < n_layers)
        def _():
            prepare(layer + 1)

        @pl.when(gives)
        def _():
            back_copy.wait_recv()
            y[keep:] = y_done[layer]
            next_start()

        @pl.when(layer + 1 < n_layers)
        def _():
            for copy in loads(layer + 1)[3:]:
                copy.start()

        return carry

    prepare(0)
    lax.fori_loop(0, n_layers, layer_body, 0)
    out_ref[...] = y[...]

    for copy in m_own:
        when_sent(has_m, copy)
    for copy, cond in (*m_relay_l, *m_relay_r):
        when_sent(cond, copy)
    for cond, copy in zip(m_has, m_fwd):
        when_sent(cond, copy)

    def sent_all(layer, carry):
        ring, fwd, own = row_copies(layer)
        y_copy, back_copy, *o_copies = give_copies(layer)
        own.wait_send()
        remote(o_stage.at[layer], o_full.at[layer, core], o_sem.at[layer, 0], o_sem.at[layer, 1], partner).wait_send()
        for cond, copy in zip((*sent, relay_a, relay_b), ring):
            when_sent(cond, copy)
        for cond, copy in zip(need, fwd):
            when_sent(cond, copy)
        when_sent(gives, y_copy)
        for copy in o_copies:
            when_sent(gives, copy)
        when_sent(takes, back_copy)
        return carry

    lax.fori_loop(0, n_layers, sent_all, 0)


def layers_call(n_sp, mem_len, hidden, memory, gain_self, gain_cross, gain_mlp, self_q, self_k, self_v, self_o, cross_q,
                cross_k, cross_v, cross_o, gate, up, down):
    rows, d_model = hidden.shape
    layers = gain_self.shape[0]
    width = d_model // 2
    ff = gate.shape[2]
    mrows, mcols = memory.shape[0], 2 * cross_k.shape[2]
    used = min(n_sp, pl.cdiv(MAX_MEM_LEN, mrows))
    n_kv = cross_k.shape[2] // HEAD_DIM
    pairs, tiles = width // PAIR, 2 * rows // TILE
    combos = pairs * tiles
    wide = 2 * (rows - HANDED)
    dma = pltpu.SemaphoreType.DMA
    return pl.pallas_call(
        functools.partial(layer_kernel, n_sp, layers),
        out_shape=jax.ShapeDtypeStruct((rows, d_model), BF16),
        in_specs=[SMEM] + [HBM] * 16,
        out_specs=VMEM,
        scratch_shapes=[
            pltpu.VMEM((rows, d_model), BF16),
            pltpu.VMEM((layers, 2 * rows, d_model), BF16),
            pltpu.VMEM((layers, 6, 2, rows // 2, d_model), BF16),
            pltpu.VMEM((mrows, d_model), BF16),
            *[pltpu.VMEM(cross_k.shape, BF16)] * 2,
            pltpu.VMEM((layers, mrows, mcols), BF16),
            pltpu.VMEM((used, layers, mrows, mcols), BF16),
            *[pltpu.VMEM((d_model, width), BF16)] * 3,
            *[pltpu.VMEM((width, d_model), BF16)] * 2,
            *[pltpu.VMEM((d_model, d_model), BF16)] * 3,
            *[pltpu.VMEM((d_model, ff), BF16)] * 2,
            pltpu.VMEM((ff, d_model), BF16),
            pltpu.VMEM((combos, PAIR, 2 * TILE), BF16),
            pltpu.VMEM((2 * pairs, PAIR, wide), BF16),
            pltpu.VMEM((pairs, CHUNK, PAIR), BF16),
            pltpu.VMEM((pairs, PAIR, CHUNK), BF16),
            pltpu.VMEM((n_kv, used * mrows, PAIR), BF16),
            pltpu.VMEM((n_kv, HEAD_DIM, used * mrows), BF16),
            *[pltpu.VMEM((combos, 1, wide), F32)] * 2,
            pltpu.VMEM((combos, HEAD_DIM, wide), F32),
            *[pltpu.VMEM((GROUP, CHUNK, wide), F32)] * 2,
            *[pltpu.VMEM((GROUP, 1, wide), F32)] * 2,
            pltpu.VMEM((layers, rows, width), BF16),
            pltpu.VMEM((layers, 2, rows, width), BF16),
            pltpu.VMEM((rows, ff), BF16),
            pltpu.VMEM((3, layers, 1, d_model), F32),
            pltpu.VMEM((3, layers, d_model), BF16),
            *[pltpu.VMEM((layers, HANDED, d_model), BF16)] * 2,
            pltpu.VMEM((layers, 2, HANDED, width), BF16),
            *[pltpu.VMEM((layers, HANDED, d_model), BF16)] * 2,
            pltpu.VMEM((2, HANDED, width), BF16),
            dma((16,)), dma((layers, 2)), *[dma((layers, 6))] * 4,
            *[dma((2,))] * 2, dma((4,)), dma((2,)), *[dma((5,))] * 2, dma((layers, 2)), *[dma((layers, 4))] * 2,
        ],
        compiler_params=pltpu.CompilerParams(collective_id=0, has_side_effects=True, vmem_limit_bytes=VMEM_LIMIT),
        name="layers",
    )(mem_len, *[pltpu.with_memory_space_constraint(x, pltpu.HBM) for x in (
        hidden, memory, gain_self, gain_cross, gain_mlp, self_q, self_k, self_v, self_o, cross_q, cross_k, cross_v, cross_o,
        gate, up, down)])


def solution(mesh):
    n_sp = mesh.shape["sp"]
    row_spec = P(("dp", "sp"), None)

    def device_fn(dec_hidden, memory, mem_len, *weights):
        return layers_call(n_sp, mem_len, dec_hidden, memory, *weights)

    return jax.shard_map(device_fn, mesh=mesh, in_specs=(row_spec, row_spec, P("dp")) + (P(),) * 14,
                         out_specs=row_spec, check_vma=False)
```
